32 devices in a mesh: grp: 2 (over y), gx: 4 (over z), gy: 2 (over x), gz: 2 (over core).
Axes of the slice: x: 2, y: 2, z: 4, core: 2. Of those that a mesh axis runs over, the one named last changes fastest.
Arguments:
- design: int32 [16, 16, 256], P(('grp', 'gx'), 'gy', 'gz'), parts along dimension 0, may hold values from 0 to 15
- supports: int32 [16, 16, 256], P(('grp', 'gx'), 'gy', 'gz'), parts along dimension 0, may hold values 0 or 1
- body_load: float32 [12, 3, 8, 16, 256], P('grp', None, 'gx', 'gy', 'gz'), parts along dimension 0, may hold values from -6 to 6
- start: float32 [12, 3, 8, 16, 256], P('grp', None, 'gx', 'gy', 'gz'), parts along dimension 0, may hold values from -1.8 to 1.8
- load_nodes: int32 [12, 16], P('grp'), parts along dimension 0, may hold values from 0 to 32767
- load_values: float32 [12, 16, 3], P('grp'), parts along dimension 0, may hold values from -24 to 24
Outputs:
- solution: float32 [12, 3, 8, 16, 256], P('grp', None, 'gx', 'gy', 'gz'), parts along dimension 0
- residual: float32 [12, 3, 8, 16, 256], P('grp', None, 'gx', 'gy', 'gz'), parts along dimension 0
The draws below stay inside these ranges and needn't reach their ends.
There are 2 independent parts, one for each index of `grp`. The reference program is written for one: setup_inputs(seed, part) draws one part's arguments, and reference() takes and returns one part's arrays. A program takes and returns all parts, laid end to end along the dimension named above; each array names one. Nothing has to cross between parts.
Inputs may be any that keep to these rules, and one draw needn't show every extreme that they name: `supports`: 1 where all three displacements of the node are held fixed. `load_nodes`: flat index (i * 16 + j) * 256 + k of a loaded node; a node may be named several times.
All inputs are finite; a program needn't handle non-finite values. No bound on the sum of `supports` on one device may be relied on, other than what follows from the above.
Results may differ from the reference program's by a relative error of at most 0.0003.
Values sent between devices are 32-bit elements; how exact they have to be, the bound alone decides.
No kernel may reach another device: no remote copies, remote signals or barrier semaphores. Data moves between devices by JAX's collectives and lax.ppermute only.
A program may use at most 64 MiB of HBM per device.

```python
import jax
import jax.numpy as jnp
import numpy as np
from jax import lax

CASES = 6
LOADS = 16
LEVELS = 16
ITERS = 2
NX = 8
NY = 16
NZ = 256


def plant(values, key, low, largest):
    place = [jax.random.randint(jax.random.fold_in(key, axis), (), 0, length) for axis, length in enumerate(values.shape)]
    main_axis = values.shape.index(max(values.shape))
    neighbour = place[:main_axis] + [(place[main_axis] + 1) % values.shape[main_axis]] + place[main_axis + 1:]
    return values.at[tuple(place)].set(low).at[tuple(neighbour)].set(largest)


def block_scale(own_key, shape, shards, smallest, top_value):
    gain = 1.0
    for dim, parts in shards:
        heights = jax.random.uniform(jax.random.fold_in(jax.random.fold_in(own_key, 6), dim), (parts,), jnp.float32, smallest / len(shards), top_value / len(shards))
        gain = gain * jnp.repeat(jnp.exp(heights), shape[dim] // parts).reshape((-1,) + (1,) * (len(shape) - 1 - dim))
    return gain


def centred(rng, shape, scale, reach, pieces=(), kind=jnp.bfloat16):
    result = jax.random.normal(rng, shape, jnp.float32) * scale
    if len(pieces) > 0:
        result = block_scale(rng, shape, pieces, -0.22, 0.18) * result
    return jnp.clip(result, min=-reach, max=reach).astype(kind)


def setup_inputs(seed: int = 0, part: int = 0) -> dict:
    key_of = jax.random.split(jax.random.key(seed), 7)
    part_keys = jax.random.split(jax.random.fold_in(key_of[6], part), 7)
    return {
        "design": plant(jax.random.randint(part_keys[0], (NX, NY, NZ), 0, LEVELS), jax.random.fold_in(part_keys[0], 1), 0, LEVELS - 1).astype(jnp.int32),
        "supports": plant((jax.random.randint(part_keys[1], (NX, NY, NZ), 0, 16) < 1).astype(jnp.int32), jax.random.fold_in(part_keys[1], 1), 0, 1),
        "body_load": centred(part_keys[2], (CASES, 3, NX, NY, NZ), 1.0, 6.0, ((2, 4), (3, 2), (4, 2)), jnp.float32),
        "start": centred(part_keys[3], (CASES, 3, NX, NY, NZ), 0.3, 1.8, ((2, 4), (3, 2), (4, 2)), jnp.float32),
        "load_nodes": plant(jax.random.randint(part_keys[4], (CASES, LOADS), 0, NX * NY * NZ), jax.random.fold_in(part_keys[4], 1), 0, (NX * NY * NZ) - 1).astype(jnp.int32),
        "load_values": centred(part_keys[5], (CASES, LOADS, 3), 4.0, 24.0, (), jnp.float32),
    }


soft_modulus = 0.05
poisson_ratio = 0.3
highest = lax.Precision.HIGHEST

def corner_list():
    return [(first, second, third) for first in (0, 1) for second in (0, 1) for third in (0, 1)]

def element_matrix():
    ratio = poisson_ratio
    lame_first = ratio / ((1.0 + ratio) * (1.0 - 2.0 * ratio))
    shear_modulus = 1.0 / (2.0 * (1.0 + ratio))
    elastic = np.zeros((6, 6))
    elastic[:3, :3] = lame_first
    for axis_dim in range(3):
        elastic[axis_dim, axis_dim] += 2.0 * shear_modulus
        elastic[3 + axis_dim, 3 + axis_dim] = shear_modulus
    gauss_points = [0.5 - 0.5 / np.sqrt(3.0), 0.5 + 0.5 / np.sqrt(3.0)]
    corners = corner_list()
    matrix_total = np.zeros((24, 24))
    for first_point in gauss_points:
        for second_point in gauss_points:
            for third_point in gauss_points:
                points = (first_point, second_point, third_point)
                strain = np.zeros((6, 24))
                for number, corner in enumerate(corners):
                    values = [points[axis_dim] if corner[axis_dim] else 1.0 - points[axis_dim] for axis_dim in range(3)]
                    slopes = [1.0 if corner[axis_dim] else -1.0 for axis_dim in range(3)]
                    grad_first = slopes[0] * values[1] * values[2]
                    grad_second = values[0] * slopes[1] * values[2]
                    grad_third = values[0] * values[1] * slopes[2]
                    column = 3 * number
                    strain[0, column] = grad_first
                    strain[1, column + 1] = grad_second
                    strain[2, column + 2] = grad_third
                    strain[3, column] = grad_second
                    strain[3, column + 1] = grad_first
                    strain[4, column + 1] = grad_third
                    strain[4, column + 2] = grad_second
                    strain[5, column] = grad_third
                    strain[5, column + 2] = grad_first
                matrix_total = matrix_total + strain.T @ elastic @ strain / 8.0
    return jnp.asarray(matrix_total, dtype=jnp.float32)

def stiffness_of(design):
    density = (design.astype(jnp.float32) + 1.0) / LEVELS
    return soft_modulus + (1.0 - soft_modulus) * density * density * density

def crop(array, width):
    return array[..., width:array.shape[-3] - width, width:array.shape[-2] - width, width:array.shape[-1] - width]

def pad_grid(array):
    widths = [(0, 0)] * (array.ndim - 3) + [(1, 1)] * 3
    return jnp.pad(array, widths)

def stiff_apply(padded, moduli, element_stiffness):
    span_first, span_second, span_third = padded.shape[-3:]
    corners = corner_list()
    results = []
    for member in range(padded.shape[0]):
        single = padded[member]
        stacked = jnp.concatenate([single[:, corner[0]:span_first - 1 + corner[0], corner[1]:span_second - 1 + corner[1], corner[2]:span_third - 1 + corner[2]] for corner in corners], axis=0)
        forces = jnp.einsum('ij,jxyz->ixyz', element_stiffness, stacked, precision=highest)
        forces = forces * moduli[None, :span_first - 1, :span_second - 1, :span_third - 1]
        accumulated = jnp.zeros((3, span_first - 2, span_second - 2, span_third - 2), jnp.float32)
        for number, corner in enumerate(corners):
            accumulated = accumulated + forces[3 * number:3 * number + 3, 1 - corner[0]:span_first - 1 - corner[0], 1 - corner[1]:span_second - 1 - corner[1], 1 - corner[2]:span_third - 1 - corner[2]]
        results.append(accumulated)
    return jnp.stack(results)

def operate(padded, moduli, movable_pad, element_stiffness):
    forces = stiff_apply(padded * movable_pad, moduli, element_stiffness)
    inner = crop(movable_pad, 1)
    return inner * forces + (1.0 - inner) * crop(padded, 1)

def inverse_diagonal(moduli, movable_inner, element_stiffness):
    span_first, span_second, span_third = moduli.shape
    adjacent = jnp.zeros((span_first - 2, span_second - 2, span_third - 2), jnp.float32)
    for corner in corner_list():
        adjacent = adjacent + moduli[1 - corner[0]:span_first - 1 - corner[0], 1 - corner[1]:span_second - 1 - corner[1], 1 - corner[2]:span_third - 1 - corner[2]]
    guarded = jnp.where(movable_inner > 0, adjacent, 1.0)
    return movable_inner / (element_stiffness[0, 0] * guarded) + (1.0 - movable_inner)

def gram_matrix(first, second):
    return jnp.einsum('iaxyz,jaxyz->ij', first, second, precision=highest)

def combine(fields, coeffs):
    return jnp.einsum('jaxyz,ji->iaxyz', fields, coeffs, precision=highest)

def small_solve(matrix, right):
    factor = jnp.linalg.cholesky(matrix)
    middle = lax.linalg.triangular_solve(factor, right, left_side=True, lower=True)
    return lax.linalg.triangular_solve(factor, middle, left_side=True, lower=True, transpose_a=True)

def add_points(plane, nodes, values):
    return plane.at[:, nodes].add(values.T)

def reference(design, supports, body_load, start, load_nodes, load_values):
    element_stiffness = element_matrix()
    stiffness = stiffness_of(design)
    movable = 1.0 - supports.astype(jnp.float32)
    moduli = pad_grid(stiffness)
    movable_pad = pad_grid(movable)
    flat = body_load.reshape(body_load.shape[0], 3, -1)
    loaded = jax.vmap(add_points)(flat, load_nodes, load_values).reshape(body_load.shape)
    loading = movable * loaded
    residual = loading - operate(pad_grid(start), moduli, movable_pad, element_stiffness)
    scaling = inverse_diagonal(moduli, movable, element_stiffness)
    direction = scaling * residual
    solution = start
    for turn_index in range(ITERS):
        applied = operate(pad_grid(direction), moduli, movable_pad, element_stiffness)
        curvature = gram_matrix(direction, applied)
        projection = gram_matrix(direction, residual)
        step_size = small_solve(curvature, projection)
        solution = solution + combine(direction, step_size)
        updated = residual - combine(applied, step_size)
        if turn_index + 1 < ITERS:
            scaled = scaling * updated
            coupling = gram_matrix(applied, scaled)
            direction = scaled + combine(direction, -small_solve(curvature, coupling))
        residual = updated
    return (solution, residual)
```

```python
import jax
import jax.numpy as jnp
import numpy as np
from jax import lax
from jax.experimental import pallas as pl
from jax.experimental.pallas import tpu as pltpu
from jax.sharding import PartitionSpec as P

LEVELS = 16

soft_modulus = 0.05
poisson_ratio = 0.3
lame = poisson_ratio / ((1.0 + poisson_ratio) * (1.0 - 2.0 * poisson_ratio))
shear = 1.0 / (2.0 * (1.0 + poisson_ratio))
THREE, TWO, ONE = 1.0 / 16.0, 1.0 / 48.0, 1.0 / 144.0
CORNER = THREE * (lame + 4.0 * shear) + 2.0 * TWO * (lame + 4.0 * shear) + ONE * (lame + 4.0 * shear)

VMEM, SMEM = pltpu.VMEM, pltpu.SMEM
F32 = jnp.float32


def up8(n):
    return -(-n // 8) * 8


def call(body, outs, ins, scratch=(), flops=0, final=False, smem=()):
    make = jax.ShapeDtypeStruct if final else VMEM
    specs = [pl.BlockSpec(memory_space=SMEM if i in smem else VMEM) for i in range(len(ins))]
    ins = [x if i in smem else pltpu.with_memory_space_constraint(x, VMEM) for i, x in enumerate(ins)]
    return pl.pallas_call(
        body,
        out_shape=[make(s, F32) for s in outs],
        in_specs=specs,
        out_specs=[pl.BlockSpec(memory_space=VMEM)] * len(outs),
        scratch_shapes=[VMEM(s, F32) for s in scratch],
        cost_estimate=pl.CostEstimate(flops=flops, bytes_accessed=0, transcendentals=0),
    )(*ins)


class Plan:
    def __init__(self, block, mesh):
        self.cases, self.comps, self.planes, self.rows, self.width = block
        self.fields = self.cases * self.comps
        self.ngx, self.ngy, self.tiles = mesh["gx"], mesh["gy"], mesh["gz"]
        if not (self.planes == self.tiles == 2 and self.rows % 8 == 0 and self.comps == 3):
            raise ValueError("block shape")
        self.depth = (self.tiles * self.width, self.ngy * self.rows)
        self.r0 = self.rows + 6
        self.per0 = up8(self.fields * self.r0 + 2 * self.r0)
        self.sta = self.fields * self.r0

    def per(self, count):
        return up8(self.fields * count)

    def tile(self, ref, base, count, comp, row):
        return ref[pl.ds(base + comp * count + row, self.cases, stride=self.comps * count), :]

    def put(self, ref, base, count, comp, row, value):
        ref[pl.ds(base + comp * count + row, self.cases, stride=self.comps * count), :] = value

    def raw(self, ref, base, comp, plane, row):
        start = base + (comp * self.planes + plane) * self.rows + row
        return ref[pl.ds(start, self.cases, stride=self.comps * self.planes * self.rows), :]

    def lanes(self, count=None):
        return lax.broadcasted_iota(jnp.int32, (count or self.cases, self.width), 1)

    def ahead(self, tiles, lane):
        moved = [pltpu.roll(v, self.width - 1, 1) for v in tiles]
        moved.append(jnp.zeros_like(tiles[0]))
        return [jnp.where(lane == self.width - 1, moved[t + 1], moved[t]) for t in range(self.tiles)]

    def behind(self, tiles, lane):
        moved = [pltpu.roll(v, 1, 1) for v in tiles]
        moved = [jnp.zeros_like(tiles[0])] + moved
        return [jnp.where(lane == 0, moved[t], moved[t + 1]) for t in range(self.tiles)]

    def wide(self, row):
        return jnp.broadcast_to(row, (self.cases, self.width))


def modes_z(p, load, mask, count, sign, out):
    lane = p.lanes()
    for r in range(count):
        m = [p.wide(mask(t, r)) for t in range(p.tiles)]
        ms = [x * sign for x in m]
        for comp in range(3):
            v = [load(t, comp, r) * (ms[t] if comp == 0 else m[t]) for t in range(p.tiles)]
            n = p.ahead(v, lane)
            for t in range(p.tiles):
                out[((comp * 2) * count + r) * p.tiles + t, 0 : p.cases, :] = v[t] + n[t]
                out[((comp * 2 + 1) * count + r) * p.tiles + t, 0 : p.cases, :] = n[t] - v[t]


def layer(p, own, other, flip, modulus, count, sign, emit):
    lane = p.lanes()

    def modes_y(ref, e, t):
        found = {}
        for comp in range(3):
            for c in (0, 1):
                at = ((comp * 2 + c) * count + e) * p.tiles + t
                a = ref[at, 0 : p.cases, :]
                b = ref[at + p.tiles, 0 : p.cases, :]
                found[comp, 0, c] = a + b
                found[comp, 1, c] = b - a
        return found

    carry = {}
    for e in range(count - 1):
        done = {}
        for t in range(p.tiles):
            near, far = modes_y(own, e, t), modes_y(other, e, t)
            u = [{}, {}, {}]
            for (comp, b, c), x in near.items():
                y = far[comp, b, c]
                plus, minus = (y - x, y + x) if flip and comp == 0 else (y + x, y - x)
                u[comp][0, b, c], u[comp][1, b, c] = plus, minus
            ux, uy, uz = u
            mod = p.wide(modulus(t, e))
            ea, eb, es = mod * (THREE * lame), mod * (2.0 * THREE * shear), mod * (THREE * shear)
            ed, ee, ef = mod * (TWO * (lame + 3.0 * shear)), mod * (TWO * lame), mod * (TWO * shear)
            eg = mod * (ONE * (lame + 4.0 * shear))
            q = ea * (ux[1, 0, 0] + uy[0, 1, 0] + uz[0, 0, 1])
            sxy = es * (uy[1, 0, 0] + ux[0, 1, 0])
            syz = es * (uz[0, 1, 0] + uy[0, 0, 1])
            sxz = es * (uz[1, 0, 0] + ux[0, 0, 1])
            s = ux[0, 1, 1] + uy[1, 0, 1] + uz[1, 1, 0]
            gx = {
                (1, 0, 0): q + eb * ux[1, 0, 0],
                (0, 1, 0): sxy,
                (0, 0, 1): sxz,
                (1, 0, 1): ed * ux[1, 0, 1] + ee * uy[0, 1, 1],
                (1, 1, 0): ed * ux[1, 1, 0] + ee * uz[0, 1, 1],
                (0, 1, 1): ef * (s + ux[0, 1, 1]),
                (1, 1, 1): eg * ux[1, 1, 1],
            }
            gy = {
                (0, 1, 0): q + eb * uy[0, 1, 0],
                (1, 0, 0): sxy,
                (0, 0, 1): syz,
                (0, 1, 1): ed * uy[0, 1, 1] + ee * ux[1, 0, 1],
                (1, 1, 0): ed * uy[1, 1, 0] + ee * uz[1, 0, 1],
                (1, 0, 1): ef * (s + uy[1, 0, 1]),
                (1, 1, 1): eg * uy[1, 1, 1],
            }
            gz = {
                (0, 0, 1): q + eb * uz[0, 0, 1],
                (1, 0, 0): sxz,
                (0, 1, 0): syz,
                (0, 1, 1): ed * uz[0, 1, 1] + ee * ux[1, 1, 0],
                (1, 0, 1): ed * uz[1, 0, 1] + ee * uy[1, 1, 0],
                (1, 1, 0): ef * (s + uz[1, 1, 0]),
                (1, 1, 1): eg * uz[1, 1, 1],
            }
            for comp, g in enumerate((gx, gy, gz)):
                h = {bc: g[(0,) + bc] - g[(1,) + bc] for bc in ((0, 1), (1, 0), (1, 1))}
                h[0, 0] = -g[1, 0, 0]
                for c in (0, 1):
                    if e:
                        done[comp, c, t] = carry[comp, c, t] + (h[0, c] - h[1, c])
                    carry[comp, c, t] = h[0, c] + h[1, c]
        if e:
            for comp in range(3):
                low = [done[comp, 0, t] - done[comp, 1, t] for t in range(p.tiles)]
                high = [done[comp, 0, t] + done[comp, 1, t] for t in range(p.tiles)]
                back = p.behind(high, lane)
                for t in range(p.tiles):
                    total = low[t] + back[t]
                    emit(t, comp, e - 1, total * sign if comp == 0 else total)


OWN, PARTNER, RECEIVED, NEAR, FAR, SCALE = range(6)


def static(p, ref, kind, t, row):
    at = (kind * p.tiles + t) * up8(p.r0) + row
    return ref[at : at + 1, :]


def place():
    core = lax.axis_index("gz")
    return core, 1.0 - 2.0 * core.astype(F32)


def shards(mesh, design, supports, body_load, start, load_nodes, load_values):
    p = Plan(body_load.shape, mesh)
    C, D, Y, W, T, FL = p.cases, p.comps, p.rows, p.width, p.tiles, p.fields
    Q = p.planes
    n_raw = FL * Q * Y
    z_load = n_raw
    z_stat = z_load + FL * Y
    z_rows = z_stat + 2 * Q * Y
    y_load = Q * FL * 3
    y_stat = y_load + Q * FL * 2
    y_rows = up8(y_stat + Q * 6)
    R0, R1, R2 = Y + 6, Y + 4, Y + 2
    N0, N1, N2, N3 = p.per0, p.per(R1), p.per(R2), p.per(Y)
    both = p.ngy == 2

    x0 = start.reshape(n_raw, W)
    bl = body_load.reshape(n_raw, W)
    de = design.reshape(Q * Y, W)
    su = supports.reshape(Q * Y, W)

    def gather_body(x_ref, b_ref, d_ref, s_ref, z_ref, *y_refs):
        core = lax.axis_index("gz")
        density = (d_ref[...].astype(F32) + 1.0) / LEVELS
        z_ref[z_stat : z_stat + Q * Y, :] = (
            soft_modulus + (1.0 - soft_modulus) * density * density * density
        )
        z_ref[z_stat + Q * Y : z_rows, :] = 1.0 - s_ref[...].astype(F32)
        if both:
            first = lax.axis_index("gy") == 0
            froms = [(jnp.where(first, Y - 3, 0), jnp.where(first, Y - 2, 0))]
        else:
            froms = [(Y - 3, Y - 2), (0, 0)]
        for y_ref, (three, two) in zip(y_refs, froms):
            if y_rows > y_stat + Q * 6:
                y_ref[y_stat + Q * 6 : y_rows, :] = jnp.zeros((y_rows - y_stat - Q * 6, W), F32)
            for q in range(Q):
                for comp in range(D):
                    for r in range(3):
                        p.put(y_ref, q * FL * 3, 3, comp, r, p.raw(x_ref, 0, comp, q, three + r))
                    for r in range(2):
                        p.put(y_ref, y_load + q * FL * 2, 2, comp, r, p.raw(b_ref, 0, comp, q, two + r))
                for kind in range(2):
                    for r in range(3):
                        at = y_stat + q * 6 + kind * 3 + r
                        y_ref[at : at + 1, :] = z_ref[pl.ds(z_stat + (kind * Q + q) * Y + three + r, 1), :]
        z_ref[0:n_raw, :] = x_ref[...]
        for f in range(FL):
            z_ref[z_load + f * Y : z_load + (f + 1) * Y, :] = b_ref[
                pl.ds(pl.multiple_of((f * Q + 1 - core) * Y, 8), Y), :
            ]

    z_msg, *y_msgs = call(
        gather_body, [(z_rows, W)] + [(y_rows, W)] * (1 if both else 2), [x0, bl, de, su], flops=10**5
    )

    def cores(x):
        return lax.ppermute(x, "gz", [(i, 1 - i) for i in range(T)])

    def rows_along(x, step):
        return lax.ppermute(x, "gy", [(i, (i + step) % p.ngy) for i in range(p.ngy)])

    def planes_along(x):
        pairs = []
        for i in range(p.ngx):
            for j in range(p.ngy):
                for k in range(T):
                    to = i + 2 * k - 1
                    mine = (i * p.ngy + j) * T + k
                    if 0 <= to < p.ngx:
                        pairs.append((mine, (to * p.ngy + j) * T + 1 - k))
                    elif p.ngy % 2 == 0:
                        pairs.append((mine, (i * p.ngy + (j ^ 1)) * T + k))
                    else:
                        pairs.append((mine, mine))
        return lax.ppermute(x, ("gx", "gy", "gz"), pairs)

    if both:
        y_got = [rows_along(y_msgs[0], 1)]
    else:
        y_got = [rows_along(y_msgs[0], 1), rows_along(y_msgs[1], -1)]
    z_got = cores(z_msg)
    zy_got = [cores(y) for y in y_got]
    halos = len(y_got)

    def assemble_body(x_ref, s_ref, z_ref, *refs):
        y_refs, zy_refs = refs[:halos], refs[halos : 2 * halos]
        own_ref, par_ref = refs[2 * halos :]
        core = lax.axis_index("gz")
        row = lax.axis_index("gy")
        below = jnp.where(row > 0, 1.0, 0.0)
        above = jnp.where(row < p.ngy - 1, 1.0, 0.0)
        for out, plane in ((own_ref, core), (par_ref, 1 - core)):
            for half in range(2):
                base = (core if half == 0 else 1 - core) * N0
                x_src, s_src = (x_ref, s_ref) if half == 0 else (z_ref, z_ref)
                ys = y_refs if half == 0 else zy_refs
                low, high = ys[0], ys[-1]
                for comp in range(D):
                    for r in range(R0):
                        if r < 3:
                            v = p.tile(low, plane * (FL * 3), 3, comp, r)
                        elif r < Y + 3:
                            v = p.raw(x_src, 0, comp, plane, r - 3)
                        else:
                            v = p.tile(high, plane * (FL * 3), 3, comp, r - Y - 3)
                        p.put(out, base, R0, comp, r, v)
                for kind in range(2):
                    for r in range(R0):
                        if r < 3:
                            v = low[pl.ds(y_stat + plane * 6 + kind * 3 + r, 1), :] * below
                        elif r < Y + 3:
                            v = s_src[pl.ds(z_stat + (kind * Q + plane) * Y + r - 3, 1), :]
                        else:
                            v = high[pl.ds(y_stat + plane * 6 + kind * 3 + r - Y - 3, 1), :] * above
                        out[pl.ds(base + p.sta + kind * R0 + r, 1), :] = v

    own, par = call(assemble_body, [(T * N0, W)] * 2, [x0, z_msg, z_got] + y_got + zy_got, flops=10**5)
    far = planes_along(own)

    def modulus_at(ref, t, r):
        at = t * N0 + p.sta + r
        return ref[at : at + 1, :]

    def movable_at(ref, t, r):
        at = t * N0 + p.sta + R0 + r
        return ref[at : at + 1, :]

    def loads_body(node_ref, value_ref, b_ref, z_ref, *refs):
        y_refs, zy_refs = refs[:halos], refs[halos : 2 * halos]
        out = refs[2 * halos]
        core = lax.axis_index("gz")
        for half in range(2):
            t = core if half == 0 else 1 - core
            ys = y_refs if half == 0 else zy_refs
            for comp in range(D):
                for r in range(R1):
                    if r < 2:
                        v = p.tile(ys[0], y_load + core * (FL * 2), 2, comp, r)
                    elif r < Y + 2:
                        if half == 0:
                            v = p.raw(b_ref, 0, comp, core, r - 2)
                        else:
                            v = p.tile(z_ref, z_load, Y, comp, r - 2)
                    else:
                        v = p.tile(ys[-1], y_load + core * (FL * 2), 2, comp, r - Y - 2)
                    out[t * (D * R1) + comp * R1 + r, 0:C, :] = v
        deep, across = p.depth
        base = ((lax.axis_index("gx") * Q + core) * across + lax.axis_index("gy") * Y - 2) * deep
        case_of = lax.broadcasted_iota(jnp.int32, (C, W), 0)
        lane = p.lanes()
        n_loads = load_nodes.shape[1]

        def one(number, _):
            case = number // n_loads
            which = number - case * n_loads
            spot = node_ref[case, which] - base

            @pl.when((spot >= 0) & (spot < R1 * deep))
            def _():
                r = spot // deep
                k = spot - r * deep
                t = k // W
                here = (case_of == case) & (lane == k - t * W)
                for comp in range(D):
                    at = t * (D * R1) + comp * R1 + r
                    out[at, 0:C, :] += jnp.where(here, value_ref[case, which * D + comp], 0.0)

            return 0

        lax.fori_loop(0, C * n_loads, one, 0)

    (loaded,) = call(
        loads_body,
        [(T * D * R1, 8, W)],
        [load_nodes, load_values.reshape(C, -1), bl, z_got] + y_got + zy_got,
        flops=2 * 10**5,
        smem=(0, 1),
    )

    def near_start_body(own_ref, par_ref, modes_ref, part_ref, other_ref):
        core, sign = place()
        modes_z(p, lambda t, k, r: p.tile(own_ref, t * N0, R0, k, r), lambda t, r: movable_at(own_ref, t, r), R0, sign, modes_ref)
        modes_z(p, lambda t, k, r: p.tile(par_ref, t * N0, R0, k, r), lambda t, r: movable_at(par_ref, t, r), R0, sign, other_ref)

        def modulus(t, e):
            return jnp.where(core == 0, modulus_at(own_ref, t, e), modulus_at(par_ref, t, e))

        def emit(t, comp, r, v):
            part_ref[(comp * R1 + r) * T + t, 0:C, :] = v

        layer(p, modes_ref, other_ref, False, modulus, R0, sign, emit)

    def field_shapes(count):
        return (6 * count * T, 8, W)

    modes, part = call(
        near_start_body,
        [field_shapes(R0), (D * R1 * T, 8, W)],
        [own, par],
        [field_shapes(R0)],
        flops=10**6,
    )

    def far_start_body(far_ref, own_ref, par_ref, modes_ref, part_ref, load_ref, r_ref, d_ref, st_ref, other_ref):
        core, sign = place()
        column = lax.axis_index("gx")
        inside = jnp.where(core == 0, column > 0, column < p.ngx - 1)
        valid = jnp.where(inside, 1.0, 0.0)
        lane_rows = lax.broadcasted_iota(jnp.int32, (R1, W), 1)
        pad = up8(R0)
        sums = []
        for t in range(T):
            at = t * N0 + p.sta
            own_e, par_e, far_e = (x[at : at + R0, :] for x in (own_ref, par_ref, far_ref))
            near = jnp.where(core == 0, own_e, par_e)
            rest = jnp.where(core == 0, far_e * valid, own_e)
            at += R0
            for kind, v in (
                (OWN, own_ref[at : at + R0, :]),
                (PARTNER, par_ref[at : at + R0, :]),
                (RECEIVED, far_ref[at : at + R0, :] * valid),
                (NEAR, near),
                (FAR, rest),
            ):
                to = (kind * T + t) * pad
                st_ref[to : to + R0, :] = v
            total = near + rest
            sums.append(total[0:R1, :] + total[1 : R1 + 1, :])
        back = p.behind(sums, lane_rows)
        for t in range(T):
            around = sums[t] + back[t]
            at = t * N0 + p.sta + R0 + 1
            mov = own_ref[at : at + R1, :]
            guarded = jnp.where(mov > 0, around, 1.0)
            to = (SCALE * T + t) * pad + 1
            st_ref[to : to + R1, :] = mov / (CORNER * guarded) + (1.0 - mov)
        modes_z(
            p,
            lambda t, k, r: p.tile(far_ref, t * N0, R0, k, r),
            lambda t, r: static(p, st_ref, RECEIVED, t, r),
            R0,
            -sign,
            other_ref,
        )

        def emit(t, comp, r, v):
            force = v + part_ref[(comp * R1 + r) * T + t, 0:C, :]
            mov = p.wide(static(p, st_ref, OWN, t, r + 1))
            here = p.tile(own_ref, t * N0, R0, comp, r + 1)
            load = load_ref[t * (D * R1) + comp * R1 + r, 0:C, :]
            res = mov * (load - force) - (1.0 - mov) * here
            p.put(d_ref, t * N1, R1, comp, r, p.wide(static(p, st_ref, SCALE, t, r + 1)) * res)
            if 2 <= r < Y + 2:
                p.put(r_ref, t * N3, Y, comp, r - 2, res)

        layer(p, modes_ref, other_ref, True, lambda t, e: static(p, st_ref, FAR, t, e), R0, -sign, emit)

    res0, dir0, consts = call(
        far_start_body,
        [(T * N3, W), (T * N1, W), (6 * T * up8(R0), W)],
        [far, own, par, modes, part, loaded],
        [field_shapes(R0)],
        flops=10**6,
    )

    def near_apply(own_ref, par_ref, st_ref, modes_ref, part_ref, other_ref, per, count, shift):
        _, sign = place()
        modes_z(p, lambda t, k, r: p.tile(own_ref, t * per, count, k, r), lambda t, r: static(p, st_ref, OWN, t, r + shift), count, sign, modes_ref)
        modes_z(p, lambda t, k, r: p.tile(par_ref, t * per, count, k, r), lambda t, r: static(p, st_ref, PARTNER, t, r + shift), count, sign, other_ref)

        def emit(t, comp, r, v):
            part_ref[(comp * (count - 2) + r) * T + t, 0:C, :] = v

        layer(p, modes_ref, other_ref, False, lambda t, e: static(p, st_ref, NEAR, t, e + shift), count, sign, emit)

    def far_apply(far_ref, own_ref, st_ref, modes_ref, part_ref, other_ref, per, count, shift, emit):
        _, sign = place()
        modes_z(p, lambda t, k, r: p.tile(far_ref, t * per, count, k, r), lambda t, r: static(p, st_ref, RECEIVED, t, r + shift), count, -sign, other_ref)

        def finish(t, comp, r, v):
            force = v + part_ref[(comp * (count - 2) + r) * T + t, 0:C, :]
            mov = p.wide(static(p, st_ref, OWN, t, r + 1 + shift))
            here = p.tile(own_ref, t * per, count, comp, r + 1)
            emit(t, comp, r, mov * force + (1.0 - mov) * here, here)

        layer(p, modes_ref, other_ref, True, lambda t, e: static(p, st_ref, FAR, t, e + shift), count, -sign, finish)

    far_d = planes_along(dir0)
    par_d = cores(dir0)

    def near_one_body(own_ref, par_ref, st_ref, modes_ref, part_ref, other_ref):
        near_apply(own_ref, par_ref, st_ref, modes_ref, part_ref, other_ref, N1, R1, 1)

    modes1, part1 = call(
        near_one_body, [field_shapes(R1), (D * R2 * T, 8, W)], [dir0, par_d, consts], [field_shapes(R1)], flops=10**6
    )

    def far_one_body(far_ref, own_ref, st_ref, modes_ref, part_ref, q_ref, w_ref, other_ref):
        if N2 > FL * R2:
            for t in range(T):
                w_ref[t * N2 + FL * R2 : (t + 1) * N2, :] = jnp.zeros((N2 - FL * R2, W), F32)

        def emit(t, comp, r, image, here):
            scale = p.wide(static(p, st_ref, SCALE, t, r + 2))
            p.put(w_ref, t * N2, R2, comp, r, scale * image - here)
            if 1 <= r < Y + 1:
                p.put(q_ref, t * N3, Y, comp, r - 1, image)

        far_apply(far_ref, own_ref, st_ref, modes_ref, part_ref, other_ref, N1, R1, 1, emit)

    image0, second = call(
        far_one_body,
        [(T * N3, W), (T * N2, W)],
        [far_d, dir0, consts, modes1, part1],
        [field_shapes(R1)],
        flops=10**6,
    )

    far_w = planes_along(second)
    par_w = cores(second)

    def columns(number, sums, lane):
        table = jnp.zeros((C, W), F32)
        for j in range(C):
            column = jnp.sum(sums[j], axis=1, keepdims=True)
            table = jnp.where(lane == number * C + j, column, table)
        return table

    def gram_body(d_ref, q_ref, r_ref, w_ref, g_ref, mine_ref, send_ref):
        core = lax.axis_index("gz")
        lane = p.lanes()
        sums = [[jnp.zeros((C, W), F32) for _ in range(C)] for _ in range(3)]
        for t in range(T):
            for comp in range(D):
                for r in range(Y):
                    d = p.tile(d_ref, t * N1, R1, comp, r + 2)
                    w = p.tile(w_ref, t * N2, R2, comp, r + 1)
                    for j in range(C):
                        at = t * N3 + (j * D + comp) * Y + r
                        q = q_ref[at : at + 1, :]
                        sums[0][j] = sums[0][j] + d * q
                        sums[1][j] = sums[1][j] + d * r_ref[at : at + 1, :]
                        sums[2][j] = sums[2][j] + w * q
        table = columns(0, sums[0], lane) + columns(1, sums[1], lane) + columns(2, sums[2], lane)
        g_ref[...] = jnp.zeros((8, W), F32)
        g_ref[0:C, :] = table
        for out, t in ((mine_ref, core), (send_ref, 1 - core)):
            for number, src in enumerate((r_ref, q_ref)):
                out[number * N3 : (number + 1) * N3, :] = src[pl.ds(pl.multiple_of(t * N3, 8), N3), :]
            for comp in range(D):
                for r in range(Y):
                    p.put(out, 2 * N3, Y, comp, r, p.tile(d_ref, t * N1, R1, comp, r + 2))
                    p.put(out, 3 * N3, Y, comp, r, p.tile(w_ref, t * N2, R2, comp, r + 1))

    gram3, mine, send = call(
        gram_body,
        [(8, W), (4 * N3, W), (4 * N3, W)],
        [dir0, image0, res0, second],
        flops=10**6,
    )

    def near_two_body(own_ref, par_ref, st_ref, modes_ref, part_ref, other_ref):
        near_apply(own_ref, par_ref, st_ref, modes_ref, part_ref, other_ref, N2, R2, 2)

    modes2, part2 = call(
        near_two_body, [field_shapes(R2), (D * Y * T, 8, W)], [second, par_w, consts], [field_shapes(R2)], flops=10**6
    )
    kept = cores(send)

    def far_two_body(far_ref, own_ref, st_ref, modes_ref, part_ref, gram_ref, g_ref, mine_ref, send_ref, other_ref, u_ref):
        core = lax.axis_index("gz")

        def emit(t, comp, r, image, here):
            p.put(u_ref, t * N3, Y, comp, r, image)
            sums_in.append((image, t, comp, r))

        sums_in = []
        far_apply(far_ref, own_ref, st_ref, modes_ref, part_ref, other_ref, N2, R2, 2, emit)
        sums = [jnp.zeros((C, W), F32) for _ in range(C)]
        for _, t, comp, r in sums_in:
            u = p.tile(u_ref, t * N3, Y, comp, r)
            for j in range(C):
                at = t * N2 + (j * D + comp) * R2 + r + 1
                sums[j] = sums[j] + u * own_ref[at : at + 1, :]
        g_ref[...] = gram_ref[...]
        g_ref[0:C, :] = gram_ref[0:C, :] + columns(3, sums, p.lanes())
        mine_ref[...] = u_ref[pl.ds(pl.multiple_of(core * N3, 8), N3), :]
        send_ref[...] = u_ref[pl.ds(pl.multiple_of((1 - core) * N3, 8), N3), :]

    table, mine_u, send_u = call(
        far_two_body,
        [(8, W), (N3, W), (N3, W)],
        [far_w, second, consts, modes2, part2, gram3],
        [field_shapes(R2), (T * N3, W)],
        flops=10**6,
    )
    kept_u = cores(send_u)

    table = table + cores(table)
    for axis, size in (("gy", p.ngy), ("gx", p.ngx)):
        if size & (size - 1):
            table = lax.psum(table, axis)
            continue
        step = 1
        while step < size:
            pairs = [(i * T + k, (i ^ step) * T + 1 - k) for i in range(size) for k in range(T)]
            table = table + lax.ppermute(table, (axis, "gz"), pairs)
            step *= 2

    def final_body(g_ref, x_ref, mine_ref, mine_u_ref, kept_ref, kept_u_ref, out_ref, res_ref, a_ref):
        core = lax.axis_index("gz")
        lane = lax.broadcasted_iota(jnp.int32, (1, W), 1)

        def splat(row, at):
            return jnp.broadcast_to(row[:, at : at + 1], (1, W))

        def factor(rows, first):
            a = {(i, j): splat(rows[i], first + j) for i in range(C) for j in range(i + 1)}
            low, inv = {}, []
            for k in range(C):
                inv.append(1.0 / a[k, k])
                for i in range(k + 1, C):
                    low[i, k] = a[i, k] * inv[k]
                for i in range(k + 1, C):
                    for j in range(k + 1, i + 1):
                        a[i, j] = a[i, j] - low[i, k] * a[j, k]
            return low, inv

        def solve(factors, right):
            low, inv = factors
            y = []
            for i in range(C):
                v = right[i]
                for k in range(i):
                    v = v - low[i, k] * y[k]
                y.append(v)
            x = [None] * C
            for i in reversed(range(C)):
                v = y[i] * inv[i]
                for k in range(i + 1, C):
                    v = v - low[k, i] * x[k]
                x[i] = v
            return x

        rows = [g_ref[i : i + 1, :] for i in range(C)]
        first = solve(factor(rows, 0), rows)
        reduced = []
        for i in range(C):
            v = jnp.where(
                lane < 2 * C, pltpu.roll(rows[i], C, 1) - rows[i], pltpu.roll(rows[i], W - C, 1)
            )
            for k in range(C):
                v = v - splat(rows[i], 2 * C + k) * first[k]
            reduced.append(v)
        on_second = solve(factor(reduced, 2 * C), reduced)
        for i in range(C):
            v = first[i]
            for k in range(C):
                v = v - splat(first[i], 2 * C + k) * on_second[k]
            for k in range(C):
                a_ref[i * C + k] = jnp.broadcast_to(v[:, C + k : C + k + 1], (Y, W))
                a_ref[C * C + i * C + k] = jnp.broadcast_to(on_second[i][:, C + k : C + k + 1], (Y, W))
        for src, src_u, plane in ((mine_ref, mine_u_ref, core), (kept_ref, kept_u_ref, 1 - core)):
            for comp in range(D):
                fs = [(j * D + comp) * Y for j in range(C)]
                q = [src[N3 + f : N3 + f + Y, :] for f in fs]
                d = [src[2 * N3 + f : 2 * N3 + f + Y, :] for f in fs]
                w = [src[3 * N3 + f : 3 * N3 + f + Y, :] for f in fs]
                u = [src_u[f : f + Y, :] for f in fs]
                for i in range(C):
                    at = pl.ds(pl.multiple_of(((i * D + comp) * Q + plane) * Y, 8), Y)
                    sol = x_ref[at, :]
                    res = src[fs[i] : fs[i] + Y, :]
                    for j in range(C):
                        a, b = a_ref[j * C + i], a_ref[C * C + j * C + i]
                        sol = sol + (d[j] * a + w[j] * b)
                        res = res - (q[j] * a + u[j] * b)
                    out_ref[at, :] = sol
                    res_ref[at, :] = res

    out, res = call(
        final_body,
        [(n_raw, W)] * 2,
        [table, x0, mine, mine_u, kept, kept_u],
        [(2 * C * C, Y, W)],
        flops=10**5,
        final=True,
    )
    return out.reshape(start.shape), res.reshape(start.shape)


def solution(mesh):
    in_specs = (
        P(("grp", "gx"), "gy", "gz"),
        P(("grp", "gx"), "gy", "gz"),
        P("grp", None, "gx", "gy", "gz"),
        P("grp", None, "gx", "gy", "gz"),
        P("grp", None),
        P("grp", None, None),
    )
    out_specs = (P("grp", None, "gx", "gy", "gz"), P("grp", None, "gx", "gy", "gz"))

    def body(*args):
        return shards(dict(mesh.shape), *args)

    return jax.shard_map(body, mesh=mesh, in_specs=in_specs, out_specs=out_specs, check_vma=False)
```

```python
import jax
import jax.numpy as jnp
from jax import lax
from jax.experimental import pallas as pl
from jax.experimental.pallas import tpu as pltpu
from jax.sharding import PartitionSpec as P


LEVELS = 16

soft_modulus = 0.05
poisson_ratio = 0.3
lame = poisson_ratio / ((1.0 + poisson_ratio) * (1.0 - 2.0 * poisson_ratio))
shear = 1.0 / (2.0 * (1.0 + poisson_ratio))
THREE, TWO, ONE = 1.0 / 16.0, 1.0 / 48.0, 1.0 / 144.0
CORNER = THREE * (lame + 4.0 * shear) + 2.0 * TWO * (lame + 4.0 * shear) + ONE * (lame + 4.0 * shear)

VMEM, SMEM = pltpu.VMEM, pltpu.SMEM
F32 = jnp.float32


def up8(n):
    return -(-n // 8) * 8


def call(body, outs, ins, scratch=(), flops=0, smem=(), hbm=(), far_out=False):
    kinds = [SMEM if i in smem else pltpu.HBM if i in hbm else VMEM for i in range(len(ins))]
    ins = [x if k is SMEM else pltpu.with_memory_space_constraint(x, k) for x, k in zip(ins, kinds)]
    return pl.pallas_call(
        body,
        out_shape=[jax.ShapeDtypeStruct(s, F32) if far_out else VMEM(s, F32) for s in outs],
        in_specs=[pl.BlockSpec(memory_space=k) for k in kinds],
        out_specs=[pl.BlockSpec(memory_space=pl.ANY if far_out else VMEM)] * len(outs),
        scratch_shapes=[VMEM(s, F32) if isinstance(s, tuple) else s for s in scratch],
        compiler_params=pltpu.CompilerParams(vmem_limit_bytes=16 * 2**20),
        cost_estimate=pl.CostEstimate(flops=flops, bytes_accessed=0, transcendentals=0),
    )(*ins)


class Plan:
    def __init__(self, block, mesh):
        self.cases, self.comps, self.planes, self.rows, self.width = block
        self.fields = self.cases * self.comps
        self.ngx, self.ngy, self.tiles = mesh["gx"], mesh["gy"], mesh["gz"]
        if not (self.planes == self.tiles == 2 and self.rows % 8 == 0 and self.comps == 3):
            raise ValueError("block shape")
        self.depth = (self.tiles * self.width, self.ngy * self.rows)
        self.r0 = self.rows + 6
        self.main = up8((self.fields + 2) * self.rows)
        self.halo = up8((self.fields + 2) * 6)

    def per(self, count):
        return up8(self.fields * count)

    def tile(self, ref, base, count, comp, row):
        return ref[pl.ds(base + comp * count + row, self.cases, stride=self.comps * count), :]

    def put(self, ref, base, count, comp, row, value):
        ref[pl.ds(base + comp * count + row, self.cases, stride=self.comps * count), :] = value

    def raw(self, ref, base, comp, plane, row):
        start = base + (comp * self.planes + plane) * self.rows + row
        return ref[pl.ds(start, self.cases, stride=self.comps * self.planes * self.rows), :]

    def lanes(self, count=None):
        return lax.broadcasted_iota(jnp.int32, (count or self.cases, self.width), 1)

    def ahead(self, tiles, lane):
        moved = [pltpu.roll(v, self.width - 1, 1) for v in tiles]
        moved.append(jnp.zeros_like(tiles[0]))
        return [jnp.where(lane == self.width - 1, moved[t + 1], moved[t]) for t in range(self.tiles)]

    def behind(self, tiles, lane):
        moved = [pltpu.roll(v, 1, 1) for v in tiles]
        moved = [jnp.zeros_like(tiles[0])] + moved
        return [jnp.where(lane == 0, moved[t], moved[t + 1]) for t in range(self.tiles)]

    def wide(self, row):
        return jnp.broadcast_to(row, (self.cases, self.width))


def modes_z(p, load, mask, count, sign, out):
    lane = p.lanes()
    for r in range(count):
        m = [p.wide(mask(t, r)) for t in range(p.tiles)]
        ms = [x * sign for x in m]
        for comp in range(3):
            v = [load(t, comp, r) * (ms[t] if comp == 0 else m[t]) for t in range(p.tiles)]
            n = p.ahead(v, lane)
            for t in range(p.tiles):
                out[((comp * 2) * count + r) * p.tiles + t, 0 : p.cases, :] = v[t] + n[t]
                out[((comp * 2 + 1) * count + r) * p.tiles + t, 0 : p.cases, :] = n[t] - v[t]


def layer(p, own, other, flip, modulus, count, sign, emit):
    lane = p.lanes()

    def modes_y(ref, e, t):
        found = {}
        for comp in range(3):
            for c in (0, 1):
                at = ((comp * 2 + c) * count + e) * p.tiles + t
                a = ref[at, 0 : p.cases, :]
                b = ref[at + p.tiles, 0 : p.cases, :]
                found[comp, 0, c] = a + b
                found[comp, 1, c] = b - a
        return found

    carry = {}
    for e in range(count - 1):
        done = {}
        for t in range(p.tiles):
            near, far = modes_y(own, e, t), modes_y(other, e, t)
            u = [{}, {}, {}]
            for (comp, b, c), x in near.items():
                y = far[comp, b, c]
                plus, minus = (y - x, y + x) if flip and comp == 0 else (y + x, y - x)
                u[comp][0, b, c], u[comp][1, b, c] = plus, minus
            ux, uy, uz = u
            mod = p.wide(modulus(t, e))
            ea, eb, es = mod * (THREE * lame), mod * (2.0 * THREE * shear), mod * (THREE * shear)
            ed, ee, ef = mod * (TWO * (lame + 3.0 * shear)), mod * (TWO * lame), mod * (TWO * shear)
            eg = mod * (ONE * (lame + 4.0 * shear))
            q = ea * (ux[1, 0, 0] + uy[0, 1, 0] + uz[0, 0, 1])
            sxy = es * (uy[1, 0, 0] + ux[0, 1, 0])
            syz = es * (uz[0, 1, 0] + uy[0, 0, 1])
            sxz = es * (uz[1, 0, 0] + ux[0, 0, 1])
            s = ux[0, 1, 1] + uy[1, 0, 1] + uz[1, 1, 0]
            gx = {
                (1, 0, 0): q + eb * ux[1, 0, 0],
                (0, 1, 0): sxy,
                (0, 0, 1): sxz,
                (1, 0, 1): ed * ux[1, 0, 1] + ee * uy[0, 1, 1],
                (1, 1, 0): ed * ux[1, 1, 0] + ee * uz[0, 1, 1],
                (0, 1, 1): ef * (s + ux[0, 1, 1]),
                (1, 1, 1): eg * ux[1, 1, 1],
            }
            gy = {
                (0, 1, 0): q + eb * uy[0, 1, 0],
                (1, 0, 0): sxy,
                (0, 0, 1): syz,
                (0, 1, 1): ed * uy[0, 1, 1] + ee * ux[1, 0, 1],
                (1, 1, 0): ed * uy[1, 1, 0] + ee * uz[1, 0, 1],
                (1, 0, 1): ef * (s + uy[1, 0, 1]),
                (1, 1, 1): eg * uy[1, 1, 1],
            }
            gz = {
                (0, 0, 1): q + eb * uz[0, 0, 1],
                (1, 0, 0): sxz,
                (0, 1, 0): syz,
                (0, 1, 1): ed * uz[0, 1, 1] + ee * ux[1, 1, 0],
                (1, 0, 1): ed * uz[1, 0, 1] + ee * uy[1, 1, 0],
                (1, 1, 0): ef * (s + uz[1, 1, 0]),
                (1, 1, 1): eg * uz[1, 1, 1],
            }
            for comp, g in enumerate((gx, gy, gz)):
                h = {bc: g[(0,) + bc] - g[(1,) + bc] for bc in ((0, 1), (1, 0), (1, 1))}
                h[0, 0] = -g[1, 0, 0]
                for c in (0, 1):
                    if e:
                        done[comp, c, t] = carry[comp, c, t] + (h[0, c] - h[1, c])
                    carry[comp, c, t] = h[0, c] + h[1, c]
        if e:
            for comp in range(3):
                low = [done[comp, 0, t] - done[comp, 1, t] for t in range(p.tiles)]
                high = [done[comp, 0, t] + done[comp, 1, t] for t in range(p.tiles)]
                back = p.behind(high, lane)
                for t in range(p.tiles):
                    total = low[t] + back[t]
                    emit(t, comp, e - 1, total * sign if comp == 0 else total)


def single(p, ref, modulus, count, sign, way, emit):
    lane = p.lanes()
    cq, cb, cs = THREE * lame, 2.0 * THREE * shear, THREE * shear
    cd, ce, cf = TWO * (lame + 3.0 * shear), TWO * lame, TWO * shear
    cg = ONE * (lame + 4.0 * shear)
    carry = {}
    for e in range(count - 1):
        done = {}
        for t in range(p.tiles):
            m = [{}, {}, {}]
            for comp in range(3):
                for c in (0, 1):
                    at = ((comp * 2 + c) * count + e) * p.tiles + t
                    a = ref[at, 0 : p.cases, :]
                    b = ref[at + p.tiles, 0 : p.cases, :]
                    m[comp][0, c], m[comp][1, c] = a + b, b - a
            x, y, z = m
            mod = p.wide(modulus(t, e))
            q = cq * (x[0, 0] + y[1, 0] + z[0, 1])
            sxy = cs * (y[0, 0] + x[1, 0])
            sxz = cs * (z[0, 0] + x[0, 1])
            pair = z[1, 0] + y[0, 1]
            syz = cs * pair
            s = x[1, 1] + pair
            if way > 0:
                sh = {
                    (0, 1, 0): sxy - (cd * x[1, 0] + ce * z[1, 1]),
                    (0, 0, 1): sxz - (cd * x[0, 1] + ce * y[1, 1]),
                    (0, 1, 1): (2.0 * cf - cg) * x[1, 1] + cf * pair,
                    (1, 0, 0): -sxy,
                    (1, 1, 0): q + ((cb - cd) * y[1, 0] - ce * z[0, 1]),
                    (1, 0, 1): syz - cf * (s + y[0, 1]),
                    (1, 1, 1): (cd - cg) * y[1, 1] + ce * x[0, 1],
                    (2, 0, 0): -sxz,
                    (2, 0, 1): q + ((cb - cd) * z[0, 1] - ce * y[1, 0]),
                    (2, 1, 0): syz - cf * (s + z[1, 0]),
                    (2, 1, 1): (cd - cg) * z[1, 1] + ce * x[1, 0],
                }
            else:
                sh = {
                    (0, 1, 0): -sxy - (cd * x[1, 0] + ce * z[1, 1]),
                    (0, 0, 1): -sxz - (cd * x[0, 1] + ce * y[1, 1]),
                    (0, 1, 1): (-2.0 * cf - cg) * x[1, 1] - cf * pair,
                    (1, 0, 0): sxy,
                    (1, 1, 0): q + ((cb + cd) * y[1, 0] + ce * z[0, 1]),
                    (1, 0, 1): syz + cf * (s + y[0, 1]),
                    (1, 1, 1): (cd + cg) * y[1, 1] + ce * x[0, 1],
                    (2, 0, 0): sxz,
                    (2, 0, 1): q + ((cb + cd) * z[0, 1] + ce * y[1, 0]),
                    (2, 1, 0): syz + cf * (s + z[1, 0]),
                    (2, 1, 1): (cd + cg) * z[1, 1] + ce * x[1, 0],
                }
            sh[0, 0, 0] = -(q + cb * x[0, 0])
            for comp in range(3):
                h = {bc: mod * sh[(comp,) + bc] for bc in ((0, 0), (0, 1), (1, 0), (1, 1))}
                for c in (0, 1):
                    if e:
                        done[comp, c, t] = carry[comp, c, t] + (h[0, c] - h[1, c])
                    carry[comp, c, t] = h[0, c] + h[1, c]
        if e:
            for comp in range(3):
                low = [done[comp, 0, t] - done[comp, 1, t] for t in range(p.tiles)]
                high = [done[comp, 0, t] + done[comp, 1, t] for t in range(p.tiles)]
                back = p.behind(high, lane)
                for t in range(p.tiles):
                    total = low[t] + back[t]
                    emit(t, comp, e - 1, total * sign if comp == 0 else total)


OWN, PARTNER, RECEIVED, NEAR, FAR, SCALE = range(6)


def static(p, ref, kind, t, row):
    at = (kind * p.tiles + t) * up8(p.r0) + row
    return ref[at : at + 1, :]


def place():
    core = lax.axis_index("gz")
    return core, 1.0 - 2.0 * core.astype(F32)


def shards(mesh, design, supports, body_load, start, load_nodes, load_values):
    p = Plan(body_load.shape, mesh)
    C, D, Y, W, T, FL = p.cases, p.comps, p.rows, p.width, p.tiles, p.fields
    Q = p.planes
    n_raw = FL * Q * Y
    z_load = n_raw
    z_stat = z_load + FL * Y
    z_rows = z_stat + 2 * Q * Y
    y_load = Q * FL * 3
    y_stat = y_load + Q * FL * 2
    y_rows = up8(y_stat + Q * 6)
    R0, R1, R2 = Y + 6, Y + 4, Y + 2
    N1, N2, N3 = p.per(R1), p.per(R2), p.per(Y)
    M, H = p.main, p.halo
    both = p.ngy == 2

    x0 = start.reshape(n_raw, W)
    bl = body_load.reshape(n_raw, W)
    de = design.reshape(Q * Y, W)
    su = supports.reshape(Q * Y, W)

    def gather_body(x_hbm, b_hbm, d_hbm, s_hbm, z_ref, b_ref, *refs):
        y_refs, (d_ref, s_ref, sems) = refs[:-3], refs[-3:]
        core = lax.axis_index("gz")
        moves = [
            pltpu.make_async_copy(src, dst, sems.at[i])
            for i, (src, dst) in enumerate(
                ((x_hbm, z_ref.at[pl.ds(0, n_raw)]), (b_hbm, b_ref), (d_hbm, d_ref), (s_hbm, s_ref))
            )
        ]
        for move in moves:
            move.start()
        moves[2].wait()
        density = (d_ref[...].astype(F32) + 1.0) / LEVELS
        z_ref[z_stat : z_stat + Q * Y, :] = (
            soft_modulus + (1.0 - soft_modulus) * density * density * density
        )
        moves[3].wait()
        z_ref[z_stat + Q * Y : z_rows, :] = 1.0 - s_ref[...].astype(F32)
        if both:
            first = lax.axis_index("gy") == 0
            froms = [(jnp.where(first, Y - 3, 0), jnp.where(first, Y - 2, 0))]
        else:
            froms = [(Y - 3, Y - 2), (0, 0)]
        for y_ref, (three, _) in zip(y_refs, froms):
            if y_rows > y_stat + Q * 6:
                y_ref[y_stat + Q * 6 : y_rows, :] = jnp.zeros((y_rows - y_stat - Q * 6, W), F32)
            for q in range(Q):
                for kind in range(2):
                    for r in range(3):
                        at = y_stat + q * 6 + kind * 3 + r
                        y_ref[at : at + 1, :] = z_ref[pl.ds(z_stat + (kind * Q + q) * Y + three + r, 1), :]
        moves[0].wait()
        for y_ref, (three, _) in zip(y_refs, froms):
            for q in range(Q):
                for comp in range(D):
                    for r in range(3):
                        p.put(y_ref, q * FL * 3, 3, comp, r, p.raw(z_ref, 0, comp, q, three + r))
        moves[1].wait()
        for y_ref, (_, two) in zip(y_refs, froms):
            for q in range(Q):
                for comp in range(D):
                    for r in range(2):
                        p.put(y_ref, y_load + q * FL * 2, 2, comp, r, p.raw(b_ref, 0, comp, q, two + r))
        for f in range(FL):
            z_ref[z_load + f * Y : z_load + (f + 1) * Y, :] = b_ref[
                pl.ds(pl.multiple_of((f * Q + 1 - core) * Y, 8), Y), :
            ]

    z_msg, b_near, *y_msgs = call(
        gather_body,
        [(z_rows, W), (n_raw, W)] + [(y_rows, W)] * (1 if both else 2),
        [x0, bl, de, su],
        [VMEM((Q * Y, W), jnp.int32), VMEM((Q * Y, W), jnp.int32), pltpu.SemaphoreType.DMA((4,))],
        flops=10**5,
        hbm=(0, 1, 2, 3),
    )

    def cores(x):
        return lax.ppermute(x, "gz", [(i, 1 - i) for i in range(T)])

    def rows_along(x, step):
        return lax.ppermute(x, "gy", [(i, (i + step) % p.ngy) for i in range(p.ngy)])

    def planes_along(x):
        pairs = []
        for i in range(p.ngx):
            for j in range(p.ngy):
                for k in range(T):
                    to = i + 2 * k - 1
                    mine = (i * p.ngy + j) * T + k
                    if 0 <= to < p.ngx:
                        pairs.append((mine, (to * p.ngy + j) * T + 1 - k))
                    elif p.ngy % 2 == 0:
                        pairs.append((mine, (i * p.ngy + (j ^ 1)) * T + k))
                    else:
                        pairs.append((mine, mine))
        return lax.ppermute(x, ("gx", "gy", "gz"), pairs)

    if both:
        y_got = [rows_along(y_msgs[0], 1)]
    else:
        y_got = [rows_along(y_msgs[0], 1), rows_along(y_msgs[1], -1)]
    z_got = cores(z_msg)
    zy_got = [cores(y) for y in y_got]
    halos = len(y_got)

    def main_body(s_ref, z_ref, own_ref, par_ref):
        core = lax.axis_index("gz")
        for out, plane in ((own_ref, core), (par_ref, 1 - core)):
            for src, half in ((s_ref, core), (z_ref, 1 - core)):
                base = half * M
                for comp in range(D):
                    for r in range(Y):
                        p.put(out, base, Y, comp, r, p.raw(src, 0, comp, plane, r))
                for kind in range(2):
                    out[pl.ds(pl.multiple_of(base + (FL + kind) * Y, 8), Y), :] = src[
                        pl.ds(pl.multiple_of(z_stat + (kind * Q + plane) * Y, 8), Y), :
                    ]

    own_m, par_m = call(main_body, [(T * M, W)] * 2, [z_msg, z_got], flops=10**5)
    far_m = planes_along(own_m)

    def halo_body(*refs):
        y_refs, zy_refs = refs[:halos], refs[halos : 2 * halos]
        own_ref, par_ref = refs[2 * halos :]
        core = lax.axis_index("gz")
        row = lax.axis_index("gy")
        below = jnp.where(row > 0, 1.0, 0.0)
        above = jnp.where(row < p.ngy - 1, 1.0, 0.0)
        for out, plane in ((own_ref, core), (par_ref, 1 - core)):
            for ys, half in ((y_refs, core), (zy_refs, 1 - core)):
                base = half * H
                for r in range(6):
                    src, flag = (ys[0], below) if r < 3 else (ys[-1], above)
                    for comp in range(D):
                        p.put(out, base, 6, comp, r, p.tile(src, plane * (FL * 3), 3, comp, r % 3))
                    for kind in range(2):
                        v = src[pl.ds(y_stat + plane * 6 + kind * 3 + r % 3, 1), :]
                        out[pl.ds(base + (FL + kind) * 6 + r, 1), :] = v * flag

    own_h, par_h = call(halo_body, [(T * H, W)] * 2, y_got + zy_got, flops=10**5)
    far_h = planes_along(own_h)

    def field_at(refs, t, comp, r):
        main, halo = refs
        if 3 <= r < Y + 3:
            return p.tile(main, t * M, Y, comp, r - 3)
        return p.tile(halo, t * H, 6, comp, r if r < 3 else r - Y)

    def const_at(refs, kind, t, r):
        main, halo = refs
        if 3 <= r < Y + 3:
            at = t * M + (FL + kind) * Y + r - 3
            return main[at : at + 1, :]
        at = t * H + (FL + kind) * 6 + (r if r < 3 else r - Y)
        return halo[at : at + 1, :]

    def const_parts(refs, kind, t):
        main, halo = refs
        at = t * H + (FL + kind) * 6
        to = t * M + (FL + kind) * Y
        return halo[at : at + 3, :], main[to : to + Y, :], halo[at + 3 : at + 6, :]

    def points_body(node_ref, value_ref, out):
        core = lax.axis_index("gz")
        deep, across = p.depth
        base = ((lax.axis_index("gx") * Q + core) * across + lax.axis_index("gy") * Y - 2) * deep
        spots = jnp.concatenate([node_ref[c : c + 1, :] for c in range(C)], axis=1) - base
        total = C * n_loads
        if W & (W - 1):
            row = spots // W
            lane = spots - row * W
        else:
            row, lane = spots >> (W.bit_length() - 1), spots & (W - 1)
        hot = jnp.where(lax.broadcasted_iota(jnp.int32, (W, total), 0) == lane, 1.0, 0.0)
        rows8 = jnp.broadcast_to(row, (8, total))
        mine = lax.broadcasted_iota(jnp.int32, (8, total), 0)
        column = lax.broadcasted_iota(jnp.int32, (8, total), 1)
        mine = (column >= mine * n_loads) & (column < (mine + 1) * n_loads)
        values = []
        for comp in range(D):
            v = jnp.concatenate([value_ref[c, comp : comp + 1, :] for c in range(C)], axis=1)
            values.append(jnp.where(mine, jnp.broadcast_to(v, (8, total)), 0.0))
        left = [
            jnp.where(rows8 == r * T + t, values[comp], 0.0)
            for t in range(T)
            for comp in range(D)
            for r in range(R1)
        ]
        out[...] = lax.dot_general(
            jnp.concatenate(left, axis=0),
            hot,
            (((1,), (1,)), ((), ())),
            precision=lax.Precision.HIGHEST,
            preferred_element_type=F32,
        )

    n_loads = load_nodes.shape[1]
    (points,) = call(
        points_body,
        [(T * D * R1 * 8, W)],
        [load_nodes, jnp.swapaxes(load_values, 1, 2)],
        flops=10**6,
    )

    def loads_body(p_ref, b_ref, z_ref, *refs):
        y_refs, zy_refs = refs[:halos], refs[halos : 2 * halos]
        out = refs[2 * halos]
        core = lax.axis_index("gz")
        for half in range(2):
            t = core if half == 0 else 1 - core
            ys = y_refs if half == 0 else zy_refs
            for comp in range(D):
                for r in range(R1):
                    if r < 2:
                        v = p.tile(ys[0], y_load + core * (FL * 2), 2, comp, r)
                    elif r < Y + 2:
                        if half == 0:
                            v = p.raw(b_ref, 0, comp, core, r - 2)
                        else:
                            v = p.tile(z_ref, z_load, Y, comp, r - 2)
                    else:
                        v = p.tile(ys[-1], y_load + core * (FL * 2), 2, comp, r - Y - 2)
                    at = t * (D * R1) + comp * R1 + r
                    out[at, 0:C, :] = v + p_ref[pl.ds(pl.multiple_of(at * 8, 8), C), :]

    (loaded,) = call(
        loads_body,
        [(T * D * R1, 8, W)],
        [points, b_near, z_got] + y_got + zy_got,
        flops=10**6,
    )

    def near_start_body(own_m_ref, own_h_ref, par_m_ref, par_h_ref, modes_ref, part_ref, other_ref):
        core, sign = place()
        own, par = (own_m_ref, own_h_ref), (par_m_ref, par_h_ref)
        for refs, out in ((own, modes_ref), (par, other_ref)):
            modes_z(
                p,
                lambda t, k, r, refs=refs: field_at(refs, t, k, r),
                lambda t, r, refs=refs: const_at(refs, 1, t, r),
                R0,
                sign,
                out,
            )

        def modulus(t, e):
            return jnp.where(core == 0, const_at(own, 0, t, e), const_at(par, 0, t, e))

        def emit(t, comp, r, v):
            part_ref[(comp * R1 + r) * T + t, 0:C, :] = v

        layer(p, modes_ref, other_ref, False, modulus, R0, sign, emit)

    def field_shapes(count):
        return (6 * count * T, 8, W)

    modes, part = call(
        near_start_body,
        [field_shapes(R0), (D * R1 * T, 8, W)],
        [own_m, own_h, par_m, par_h],
        [field_shapes(R0)],
        flops=10**6,
    )

    def far_start_body(
        far_m_ref, far_h_ref, own_m_ref, own_h_ref, par_m_ref, par_h_ref, modes_ref, part_ref, load_ref,
        r_ref, d_ref, st_ref, other_ref,
    ):
        core, sign = place()
        far, own, par = (far_m_ref, far_h_ref), (own_m_ref, own_h_ref), (par_m_ref, par_h_ref)
        column = lax.axis_index("gx")
        inside = jnp.where(core == 0, column > 0, column < p.ngx - 1)
        valid = jnp.where(inside, 1.0, 0.0)
        lane_rows = lax.broadcasted_iota(jnp.int32, (R1, W), 1)
        pad = up8(R0)
        sums = []
        for t in range(T):
            spans = ((0, 3), (3, Y), (Y + 3, 3))
            own_e, par_e, far_e = (const_parts(x, 0, t) for x in (own, par, far))
            own_m, par_m, far_m = (const_parts(x, 1, t) for x in (own, par, far))
            for n, (first, count) in enumerate(spans):
                for kind, v in (
                    (OWN, own_m[n]),
                    (PARTNER, par_m[n]),
                    (RECEIVED, far_m[n] * valid),
                    (NEAR, jnp.where(core == 0, own_e[n], par_e[n])),
                    (FAR, jnp.where(core == 0, far_e[n] * valid, own_e[n])),
                ):
                    to = (kind * T + t) * pad + first
                    st_ref[to : to + count, :] = v
            near, rest = (NEAR * T + t) * pad, (FAR * T + t) * pad
            sums.append(
                (st_ref[near : near + R1, :] + st_ref[rest : rest + R1, :])
                + (st_ref[near + 1 : near + 1 + R1, :] + st_ref[rest + 1 : rest + 1 + R1, :])
            )
        back = p.behind(sums, lane_rows)
        for t in range(T):
            around = sums[t] + back[t]
            at = (OWN * T + t) * pad + 1
            mov = st_ref[at : at + R1, :]
            guarded = jnp.where(mov > 0, around, 1.0)
            to = (SCALE * T + t) * pad + 1
            st_ref[to : to + R1, :] = mov / (CORNER * guarded) + (1.0 - mov)
        modes_z(
            p,
            lambda t, k, r: field_at(far, t, k, r),
            lambda t, r: static(p, st_ref, RECEIVED, t, r),
            R0,
            -sign,
            other_ref,
        )

        def emit(t, comp, r, v):
            force = v + part_ref[(comp * R1 + r) * T + t, 0:C, :]
            mov = p.wide(static(p, st_ref, OWN, t, r + 1))
            here = field_at(own, t, comp, r + 1)
            load = load_ref[t * (D * R1) + comp * R1 + r, 0:C, :]
            res = mov * (load - force) - (1.0 - mov) * here
            p.put(d_ref, t * N1, R1, comp, r, p.wide(static(p, st_ref, SCALE, t, r + 1)) * res)
            if 2 <= r < Y + 2:
                p.put(r_ref, t * N3, Y, comp, r - 2, res)

        layer(p, modes_ref, other_ref, True, lambda t, e: static(p, st_ref, FAR, t, e), R0, -sign, emit)

    res0, dir0, consts = call(
        far_start_body,
        [(T * N3, W), (T * N1, W), (6 * T * up8(R0), W)],
        [far_m, far_h, own_m, own_h, par_m, par_h, modes, part, loaded],
        [field_shapes(R0)],
        flops=10**6,
    )

    def near_apply(own_ref, par_ref, st_ref, part_ref, modes_ref, other_ref, per, count, shift):
        _, sign = place()
        modes_z(p, lambda t, k, r: p.tile(own_ref, t * per, count, k, r), lambda t, r: static(p, st_ref, OWN, t, r + shift), count, sign, modes_ref)
        modes_z(p, lambda t, k, r: p.tile(par_ref, t * per, count, k, r), lambda t, r: static(p, st_ref, PARTNER, t, r + shift), count, sign, other_ref)

        def emit(t, comp, r, v):
            part_ref[(comp * (count - 2) + r) * T + t, 0:C, :] = v

        def more(t, comp, r, v):
            at = (comp * (count - 2) + r) * T + t
            part_ref[at, 0:C, :] = part_ref[at, 0:C, :] + v

        layer(p, modes_ref, other_ref, False, lambda t, e: static(p, st_ref, NEAR, t, e + shift), count, sign, emit)
        single(p, modes_ref, lambda t, e: static(p, st_ref, FAR, t, e + shift), count, -sign, -1, more)

    def far_apply(far_ref, own_ref, st_ref, part_ref, other_ref, per, count, shift, emit):
        _, sign = place()
        modes_z(p, lambda t, k, r: p.tile(far_ref, t * per, count, k, r), lambda t, r: static(p, st_ref, RECEIVED, t, r + shift), count, -sign, other_ref)

        def finish(t, comp, r, v):
            force = v + part_ref[(comp * (count - 2) + r) * T + t, 0:C, :]
            mov = p.wide(static(p, st_ref, OWN, t, r + 1 + shift))
            here = p.tile(own_ref, t * per, count, comp, r + 1)
            emit(t, comp, r, mov * force + (1.0 - mov) * here, here)

        single(p, other_ref, lambda t, e: static(p, st_ref, FAR, t, e + shift), count, -sign, 1, finish)

    far_d = planes_along(dir0)
    par_d = cores(dir0)

    def near_one_body(own_ref, par_ref, st_ref, part_ref, modes_ref, other_ref):
        near_apply(own_ref, par_ref, st_ref, part_ref, modes_ref, other_ref, N1, R1, 1)

    (part1,) = call(
        near_one_body, [(D * R2 * T, 8, W)], [dir0, par_d, consts], [field_shapes(R1)] * 2, flops=10**6
    )

    def far_one_body(far_ref, own_ref, st_ref, part_ref, q_ref, w_ref, other_ref):
        if N2 > FL * R2:
            for t in range(T):
                w_ref[t * N2 + FL * R2 : (t + 1) * N2, :] = jnp.zeros((N2 - FL * R2, W), F32)

        def emit(t, comp, r, image, here):
            scale = p.wide(static(p, st_ref, SCALE, t, r + 2))
            p.put(w_ref, t * N2, R2, comp, r, scale * image - here)
            if 1 <= r < Y + 1:
                p.put(q_ref, t * N3, Y, comp, r - 1, image)

        far_apply(far_ref, own_ref, st_ref, part_ref, other_ref, N1, R1, 1, emit)

    image0, second = call(
        far_one_body,
        [(T * N3, W), (T * N2, W)],
        [far_d, dir0, consts, part1],
        [field_shapes(R1)],
        flops=10**6,
    )

    far_w = planes_along(second)
    par_w = cores(second)

    def columns(number, sums, lane):
        table = jnp.zeros((C, W), F32)
        for j in range(C):
            column = jnp.sum(sums[j], axis=1, keepdims=True)
            table = jnp.where(lane == number * C + j, column, table)
        return table

    def gram_body(d_ref, q_ref, r_ref, w_ref, g_ref, mine_ref, send_ref):
        core = lax.axis_index("gz")
        lane = p.lanes()
        sums = [[jnp.zeros((C, W), F32) for _ in range(C)] for _ in range(3)]
        for t in range(T):
            for comp in range(D):
                for r in range(Y):
                    d = p.tile(d_ref, t * N1, R1, comp, r + 2)
                    w = p.tile(w_ref, t * N2, R2, comp, r + 1)
                    for j in range(C):
                        at = t * N3 + (j * D + comp) * Y + r
                        q = q_ref[at : at + 1, :]
                        sums[0][j] = sums[0][j] + d * q
                        sums[1][j] = sums[1][j] + d * r_ref[at : at + 1, :]
                        sums[2][j] = sums[2][j] + w * q
        table = columns(0, sums[0], lane) + columns(1, sums[1], lane) + columns(2, sums[2], lane)
        g_ref[...] = jnp.zeros((8, W), F32)
        g_ref[0:C, :] = table
        for out, t in ((mine_ref, core), (send_ref, 1 - core)):
            for number, src in enumerate((r_ref, q_ref)):
                out[number * N3 : (number + 1) * N3, :] = src[pl.ds(pl.multiple_of(t * N3, 8), N3), :]
            for comp in range(D):
                for r in range(Y):
                    p.put(out, 2 * N3, Y, comp, r, p.tile(d_ref, t * N1, R1, comp, r + 2))
                    p.put(out, 3 * N3, Y, comp, r, p.tile(w_ref, t * N2, R2, comp, r + 1))

    gram3, mine, send = call(gram_body, [(8, W), (4 * N3, W), (4 * N3, W)], [dir0, image0, res0, second], flops=10**6)

    def near_two_body(own_ref, par_ref, st_ref, part_ref, modes_ref, other_ref):
        near_apply(own_ref, par_ref, st_ref, part_ref, modes_ref, other_ref, N2, R2, 2)

    (part2,) = call(
        near_two_body, [(D * Y * T, 8, W)], [second, par_w, consts], [field_shapes(R2)] * 2, flops=10**6
    )
    kept = cores(send)

    def far_two_body(far_ref, own_ref, st_ref, part_ref, gram_ref, mine_ref, send_ref, other_ref, u_ref):
        core = lax.axis_index("gz")

        def emit(t, comp, r, image, here):
            p.put(u_ref, t * N3, Y, comp, r, image)
            sums_in.append((image, t, comp, r))

        sums_in = []
        far_apply(far_ref, own_ref, st_ref, part_ref, other_ref, N2, R2, 2, emit)
        sums = [jnp.zeros((C, W), F32) for _ in range(C)]
        for _, t, comp, r in sums_in:
            u = p.tile(u_ref, t * N3, Y, comp, r)
            for j in range(C):
                at = t * N2 + (j * D + comp) * R2 + r + 1
                sums[j] = sums[j] + u * own_ref[at : at + 1, :]
        table = gram_ref[0:C, :] + columns(3, sums, p.lanes())
        for out, t in ((mine_ref, core), (send_ref, 1 - core)):
            out[0:N3, :] = u_ref[pl.ds(pl.multiple_of(t * N3, 8), N3), :]
            out[N3 : N3 + 8, :] = jnp.zeros((8, W), F32)
            out[N3 : N3 + C, :] = table

    mine_u, send_u = call(
        far_two_body,
        [(N3 + 8, W), (N3 + 8, W)],
        [far_w, second, consts, part2, gram3],
        [field_shapes(R2), (T * N3, W)],
        flops=10**6,
    )
    kept_u = cores(send_u)

    table = mine_u[N3 : N3 + 8, :] + kept_u[N3 : N3 + 8, :]
    for axis, size in (("gy", p.ngy), ("gx", p.ngx)):
        if size & (size - 1):
            table = lax.psum(table, axis)
            continue
        step = 1
        while step < size:
            pairs = [(i * T + k, (i ^ step) * T + 1 - k) for i in range(size) for k in range(T)]
            table = table + lax.ppermute(table, (axis, "gz"), pairs)
            step *= 2

    def final_body(
        g_ref, x_ref, mine_ref, mine_u_ref, kept_ref, kept_u_ref, out_hbm, res_hbm, a_ref, out_ref, res_ref, sems
    ):
        core = lax.axis_index("gz")
        lane = lax.broadcasted_iota(jnp.int32, (1, W), 1)

        def splat(row, at):
            return jnp.broadcast_to(row[:, at : at + 1], (1, W))

        def factor(rows, first):
            a = {(i, j): splat(rows[i], first + j) for i in range(C) for j in range(i + 1)}
            low, inv = {}, []
            for k in range(C):
                inv.append(1.0 / a[k, k])
                for i in range(k + 1, C):
                    low[i, k] = a[i, k] * inv[k]
                for i in range(k + 1, C):
                    for j in range(k + 1, i + 1):
                        a[i, j] = a[i, j] - low[i, k] * a[j, k]
            return low, inv

        def solve(factors, right):
            low, inv = factors
            y = []
            for i in range(C):
                v = right[i]
                for k in range(i):
                    v = v - low[i, k] * y[k]
                y.append(v)
            x = [None] * C
            for i in reversed(range(C)):
                v = y[i] * inv[i]
                for k in range(i + 1, C):
                    v = v - low[k, i] * x[k]
                x[i] = v
            return x

        rows = [g_ref[i : i + 1, :] for i in range(C)]
        first = solve(factor(rows, 0), rows)
        reduced = []
        for i in range(C):
            v = jnp.where(
                lane < 2 * C, pltpu.roll(rows[i], C, 1) - rows[i], pltpu.roll(rows[i], W - C, 1)
            )
            for k in range(C):
                v = v - splat(rows[i], 2 * C + k) * first[k]
            reduced.append(v)
        on_second = solve(factor(reduced, 2 * C), reduced)
        for i in range(C):
            v = first[i]
            for k in range(C):
                v = v - splat(first[i], 2 * C + k) * on_second[k]
            for k in range(C):
                a_ref[i * C + k] = jnp.broadcast_to(v[:, C + k : C + k + 1], (Y, W))
                a_ref[C * C + i * C + k] = jnp.broadcast_to(on_second[i][:, C + k : C + k + 1], (Y, W))
        halves = ((mine_ref, mine_u_ref, core), (kept_ref, kept_u_ref, 1 - core))
        moves = []
        for number in range(2):
            target = (out_ref, res_ref)[number]
            for src, src_u, plane in halves:
                for comp in range(D):
                    fs = [(j * D + comp) * Y for j in range(C)]
                    at = N3 if number else 2 * N3
                    v = [src[at + f : at + f + Y, :] for f in fs]
                    u = [src_u[f : f + Y, :] if number else src[3 * N3 + f : 3 * N3 + f + Y, :] for f in fs]
                    for i in range(C):
                        at = pl.ds(pl.multiple_of(((i * D + comp) * Q + plane) * Y, 8), Y)
                        total = a_ref[i] * v[0] + a_ref[C * C + i] * u[0]
                        for j in range(1, C):
                            total = total + (a_ref[j * C + i] * v[j] + a_ref[C * C + j * C + i] * u[j])
                        if number:
                            target[at, :] = src[fs[i] : fs[i] + Y, :] - total
                        else:
                            target[at, :] = x_ref[at, :] + total
            moves.append(pltpu.make_async_copy(target, (out_hbm, res_hbm)[number], sems.at[number]))
            moves[-1].start()
        for move in moves:
            move.wait()

    out, res = call(
        final_body,
        [(n_raw, W)] * 2,
        [table, z_msg, mine, mine_u, kept, kept_u],
        [(2 * C * C, Y, W), (n_raw, W), (n_raw, W), pltpu.SemaphoreType.DMA((2,))],
        flops=10**5,
        far_out=True,
    )
    return out.reshape(start.shape), res.reshape(start.shape)


def solution(mesh):
    in_specs = (
        P(("grp", "gx"), "gy", "gz"),
        P(("grp", "gx"), "gy", "gz"),
        P("grp", None, "gx", "gy", "gz"),
        P("grp", None, "gx", "gy", "gz"),
        P("grp", None),
        P("grp", None, None),
    )
    out_specs = (P("grp", None, "gx", "gy", "gz"), P("grp", None, "gx", "gy", "gz"))

    def body(*args):
        return shards(dict(mesh.shape), *args)

    return jax.shard_map(body, mesh=mesh, in_specs=in_specs, out_specs=out_specs, check_vma=False)
```

```python
import jax
import jax.numpy as jnp
from jax import lax
from jax.experimental import pallas as pl
from jax.experimental.pallas import tpu as pltpu
from jax.sharding import PartitionSpec as P


LEVELS = 16

soft_modulus = 0.05
poisson_ratio = 0.3
lame = poisson_ratio / ((1.0 + poisson_ratio) * (1.0 - 2.0 * poisson_ratio))
shear = 1.0 / (2.0 * (1.0 + poisson_ratio))
THREE, TWO, ONE = 1.0 / 16.0, 1.0 / 48.0, 1.0 / 144.0
CORNER = THREE * (lame + 4.0 * shear) + 2.0 * TWO * (lame + 4.0 * shear) + ONE * (lame + 4.0 * shear)

VMEM, SMEM = pltpu.VMEM, pltpu.SMEM
F32 = jnp.float32


def up8(n):
    return -(-n // 8) * 8


def call(body, outs, ins, scratch=(), flops=0, smem=(), hbm=(), far_out=False):
    kinds = [SMEM if i in smem else pltpu.HBM if i in hbm else VMEM for i in range(len(ins))]
    ins = [x if k is SMEM else pltpu.with_memory_space_constraint(x, k) for x, k in zip(ins, kinds)]
    return pl.pallas_call(
        body,
        out_shape=[jax.ShapeDtypeStruct(s, F32) if far_out else VMEM(s, F32) for s in outs],
        in_specs=[pl.BlockSpec(memory_space=k) for k in kinds],
        out_specs=[pl.BlockSpec(memory_space=pl.ANY if far_out else VMEM)] * len(outs),
        scratch_shapes=[VMEM(s, F32) if isinstance(s, tuple) else s for s in scratch],
        compiler_params=pltpu.CompilerParams(vmem_limit_bytes=16 * 2**20),
        cost_estimate=pl.CostEstimate(flops=flops, bytes_accessed=0, transcendentals=0),
    )(*ins)


class Plan:
    def __init__(self, block, mesh):
        self.cases, self.comps, self.planes, self.rows, self.width = block
        self.fields = self.cases * self.comps
        self.ngx, self.ngy, self.tiles = mesh["gx"], mesh["gy"], mesh["gz"]
        if not (self.planes == self.tiles == 2 and self.rows % 8 == 0 and self.comps == 3):
            raise ValueError("block shape")
        self.depth = (self.tiles * self.width, self.ngy * self.rows)
        self.r0 = self.rows + 6
        self.main = up8((self.fields + 2) * self.rows)

    def per(self, count):
        return up8(self.fields * count)

    def tile(self, ref, base, count, comp, row):
        return ref[pl.ds(base + comp * count + row, self.cases, stride=self.comps * count), :]

    def put(self, ref, base, count, comp, row, value):
        ref[pl.ds(base + comp * count + row, self.cases, stride=self.comps * count), :] = value

    def raw(self, ref, base, comp, plane, row):
        start = base + (comp * self.planes + plane) * self.rows + row
        return ref[pl.ds(start, self.cases, stride=self.comps * self.planes * self.rows), :]

    def lanes(self, count=None):
        return lax.broadcasted_iota(jnp.int32, (count or self.cases, self.width), 1)

    def ahead(self, tiles, lane):
        moved = [pltpu.roll(v, self.width - 1, 1) for v in tiles]
        moved.append(jnp.zeros_like(tiles[0]))
        return [jnp.where(lane == self.width - 1, moved[t + 1], moved[t]) for t in range(self.tiles)]

    def behind(self, tiles, lane):
        moved = [pltpu.roll(v, 1, 1) for v in tiles]
        moved = [jnp.zeros_like(tiles[0])] + moved
        return [jnp.where(lane == 0, moved[t], moved[t + 1]) for t in range(self.tiles)]

    def wide(self, row):
        return jnp.broadcast_to(row, (self.cases, self.width))


def modes_z(p, load, mask, count, sign, out):
    lane = p.lanes()
    for r in range(count):
        m = [p.wide(mask(t, r)) for t in range(p.tiles)]
        ms = [x * sign for x in m]
        for comp in range(3):
            v = [load(t, comp, r) * (ms[t] if comp == 0 else m[t]) for t in range(p.tiles)]
            n = p.ahead(v, lane)
            for t in range(p.tiles):
                out[((comp * 2) * count + r) * p.tiles + t, 0 : p.cases, :] = v[t] + n[t]
                out[((comp * 2 + 1) * count + r) * p.tiles + t, 0 : p.cases, :] = n[t] - v[t]


def layer(p, own, other, flip, modulus, count, sign, emit):
    lane = p.lanes()

    def modes_y(ref, e, t):
        found = {}
        for comp in range(3):
            for c in (0, 1):
                at = ((comp * 2 + c) * count + e) * p.tiles + t
                a = ref[at, 0 : p.cases, :]
                b = ref[at + p.tiles, 0 : p.cases, :]
                found[comp, 0, c] = a + b
                found[comp, 1, c] = b - a
        return found

    carry = {}
    for e in range(count - 1):
        done = {}
        for t in range(p.tiles):
            near, far = modes_y(own, e, t), modes_y(other, e, t)
            u = [{}, {}, {}]
            for (comp, b, c), x in near.items():
                y = far[comp, b, c]
                plus, minus = (y - x, y + x) if flip and comp == 0 else (y + x, y - x)
                u[comp][0, b, c], u[comp][1, b, c] = plus, minus
            ux, uy, uz = u
            mod = p.wide(modulus(t, e))
            ea, eb, es = mod * (THREE * lame), mod * (2.0 * THREE * shear), mod * (THREE * shear)
            ed, ee, ef = mod * (TWO * (lame + 3.0 * shear)), mod * (TWO * lame), mod * (TWO * shear)
            eg = mod * (ONE * (lame + 4.0 * shear))
            q = ea * (ux[1, 0, 0] + uy[0, 1, 0] + uz[0, 0, 1])
            sxy = es * (uy[1, 0, 0] + ux[0, 1, 0])
            syz = es * (uz[0, 1, 0] + uy[0, 0, 1])
            sxz = es * (uz[1, 0, 0] + ux[0, 0, 1])
            s = ux[0, 1, 1] + uy[1, 0, 1] + uz[1, 1, 0]
            gx = {
                (1, 0, 0): q + eb * ux[1, 0, 0],
                (0, 1, 0): sxy,
                (0, 0, 1): sxz,
                (1, 0, 1): ed * ux[1, 0, 1] + ee * uy[0, 1, 1],
                (1, 1, 0): ed * ux[1, 1, 0] + ee * uz[0, 1, 1],
                (0, 1, 1): ef * (s + ux[0, 1, 1]),
                (1, 1, 1): eg * ux[1, 1, 1],
            }
            gy = {
                (0, 1, 0): q + eb * uy[0, 1, 0],
                (1, 0, 0): sxy,
                (0, 0, 1): syz,
                (0, 1, 1): ed * uy[0, 1, 1] + ee * ux[1, 0, 1],
                (1, 1, 0): ed * uy[1, 1, 0] + ee * uz[1, 0, 1],
                (1, 0, 1): ef * (s + uy[1, 0, 1]),
                (1, 1, 1): eg * uy[1, 1, 1],
            }
            gz = {
                (0, 0, 1): q + eb * uz[0, 0, 1],
                (1, 0, 0): sxz,
                (0, 1, 0): syz,
                (0, 1, 1): ed * uz[0, 1, 1] + ee * ux[1, 1, 0],
                (1, 0, 1): ed * uz[1, 0, 1] + ee * uy[1, 1, 0],
                (1, 1, 0): ef * (s + uz[1, 1, 0]),
                (1, 1, 1): eg * uz[1, 1, 1],
            }
            for comp, g in enumerate((gx, gy, gz)):
                h = {bc: g[(0,) + bc] - g[(1,) + bc] for bc in ((0, 1), (1, 0), (1, 1))}
                h[0, 0] = -g[1, 0, 0]
                for c in (0, 1):
                    if e:
                        done[comp, c, t] = carry[comp, c, t] + (h[0, c] - h[1, c])
                    carry[comp, c, t] = h[0, c] + h[1, c]
        if e:
            for comp in range(3):
                low = [done[comp, 0, t] - done[comp, 1, t] for t in range(p.tiles)]
                high = [done[comp, 0, t] + done[comp, 1, t] for t in range(p.tiles)]
                back = p.behind(high, lane)
                for t in range(p.tiles):
                    total = low[t] + back[t]
                    emit(t, comp, e - 1, total * sign if comp == 0 else total)


def single(p, ref, modulus, count, sign, way, emit):
    lane = p.lanes()
    cq, cb, cs = THREE * lame, 2.0 * THREE * shear, THREE * shear
    cd, ce, cf = TWO * (lame + 3.0 * shear), TWO * lame, TWO * shear
    cg = ONE * (lame + 4.0 * shear)
    carry = {}
    for e in range(count - 1):
        done = {}
        for t in range(p.tiles):
            m = [{}, {}, {}]
            for comp in range(3):
                for c in (0, 1):
                    at = ((comp * 2 + c) * count + e) * p.tiles + t
                    a = ref[at, 0 : p.cases, :]
                    b = ref[at + p.tiles, 0 : p.cases, :]
                    m[comp][0, c], m[comp][1, c] = a + b, b - a
            x, y, z = m
            mod = p.wide(modulus(t, e))
            q = cq * (x[0, 0] + y[1, 0] + z[0, 1])
            sxy = cs * (y[0, 0] + x[1, 0])
            sxz = cs * (z[0, 0] + x[0, 1])
            pair = z[1, 0] + y[0, 1]
            syz = cs * pair
            s = x[1, 1] + pair
            if way > 0:
                sh = {
                    (0, 1, 0): sxy - (cd * x[1, 0] + ce * z[1, 1]),
                    (0, 0, 1): sxz - (cd * x[0, 1] + ce * y[1, 1]),
                    (0, 1, 1): (2.0 * cf - cg) * x[1, 1] + cf * pair,
                    (1, 0, 0): -sxy,
                    (1, 1, 0): q + ((cb - cd) * y[1, 0] - ce * z[0, 1]),
                    (1, 0, 1): syz - cf * (s + y[0, 1]),
                    (1, 1, 1): (cd - cg) * y[1, 1] + ce * x[0, 1],
                    (2, 0, 0): -sxz,
                    (2, 0, 1): q + ((cb - cd) * z[0, 1] - ce * y[1, 0]),
                    (2, 1, 0): syz - cf * (s + z[1, 0]),
                    (2, 1, 1): (cd - cg) * z[1, 1] + ce * x[1, 0],
                }
            else:
                sh = {
                    (0, 1, 0): -sxy - (cd * x[1, 0] + ce * z[1, 1]),
                    (0, 0, 1): -sxz - (cd * x[0, 1] + ce * y[1, 1]),
                    (0, 1, 1): (-2.0 * cf - cg) * x[1, 1] - cf * pair,
                    (1, 0, 0): sxy,
                    (1, 1, 0): q + ((cb + cd) * y[1, 0] + ce * z[0, 1]),
                    (1, 0, 1): syz + cf * (s + y[0, 1]),
                    (1, 1, 1): (cd + cg) * y[1, 1] + ce * x[0, 1],
                    (2, 0, 0): sxz,
                    (2, 0, 1): q + ((cb + cd) * z[0, 1] + ce * y[1, 0]),
                    (2, 1, 0): syz + cf * (s + z[1, 0]),
                    (2, 1, 1): (cd + cg) * z[1, 1] + ce * x[1, 0],
                }
            sh[0, 0, 0] = -(q + cb * x[0, 0])
            for comp in range(3):
                h = {bc: mod * sh[(comp,) + bc] for bc in ((0, 0), (0, 1), (1, 0), (1, 1))}
                for c in (0, 1):
                    if e:
                        done[comp, c, t] = carry[comp, c, t] + (h[0, c] - h[1, c])
                    carry[comp, c, t] = h[0, c] + h[1, c]
        if e:
            for comp in range(3):
                low = [done[comp, 0, t] - done[comp, 1, t] for t in range(p.tiles)]
                high = [done[comp, 0, t] + done[comp, 1, t] for t in range(p.tiles)]
                back = p.behind(high, lane)
                for t in range(p.tiles):
                    total = low[t] + back[t]
                    emit(t, comp, e - 1, total * sign if comp == 0 else total)


OWN, PARTNER, RECEIVED, NEAR, FAR, SCALE = range(6)


def static(p, ref, kind, t, row):
    at = (kind * p.tiles + t) * up8(p.r0) + row
    return ref[at : at + 1, :]


def place():
    core = lax.axis_index("gz")
    return core, 1.0 - 2.0 * core.astype(F32)


def shards(mesh, design, supports, body_load, start, load_nodes, load_values):
    p = Plan(body_load.shape, mesh)
    C, D, Y, W, T, FL = p.cases, p.comps, p.rows, p.width, p.tiles, p.fields
    Q = p.planes
    n_raw = FL * Q * Y
    z_load = n_raw
    z_stat = z_load + FL * Y
    z_rows = z_stat + 2 * Q * Y
    y_stat = FL * 3
    y_load = y_stat + 6
    y_part = up8(y_load + FL * 2)
    d_part = up8(y_load)
    R0, R1, R2 = Y + 6, Y + 4, Y + 2
    N1, N2, N3 = p.per(R1), p.per(R2), p.per(Y)
    M = p.main
    both = p.ngy == 2

    x0 = start.reshape(n_raw, W)
    bl = body_load.reshape(n_raw, W)
    de = design.reshape(Q * Y, W)
    su = supports.reshape(Q * Y, W)

    def gather_body(x_hbm, b_hbm, d_hbm, s_hbm, z_ref, b_ref, *refs):
        d_ref, s_ref, sems = refs
        core = lax.axis_index("gz")
        moves = [
            pltpu.make_async_copy(src, dst, sems.at[i])
            for i, (src, dst) in enumerate(
                ((x_hbm, z_ref.at[pl.ds(0, n_raw)]), (b_hbm, b_ref), (d_hbm, d_ref), (s_hbm, s_ref))
            )
        ]
        for move in moves:
            move.start()
        moves[2].wait()
        density = (d_ref[...].astype(F32) + 1.0) / LEVELS
        z_ref[z_stat : z_stat + Q * Y, :] = (
            soft_modulus + (1.0 - soft_modulus) * density * density * density
        )
        moves[3].wait()
        z_ref[z_stat + Q * Y : z_rows, :] = 1.0 - s_ref[...].astype(F32)
        moves[1].wait()
        for f in range(FL):
            z_ref[z_load + f * Y : z_load + (f + 1) * Y, :] = b_ref[
                pl.ds(pl.multiple_of((f * Q + 1 - core) * Y, 8), Y), :
            ]
        moves[0].wait()

    z_msg, b_near = call(
        gather_body,
        [(z_rows, W), (n_raw, W)],
        [x0, bl, de, su],
        [VMEM((Q * Y, W), jnp.int32), VMEM((Q * Y, W), jnp.int32), pltpu.SemaphoreType.DMA((4,))],
        flops=10**5,
        hbm=(0, 1, 2, 3),
    )

    def cores(x):
        return lax.ppermute(x, "gz", [(i, 1 - i) for i in range(T)])

    def rows_along(x, step):
        return lax.ppermute(x, "gy", [(i, (i + step) % p.ngy) for i in range(p.ngy)])

    def planes_along(x, step=0):
        pairs = []
        for i in range(p.ngx):
            for j in range(p.ngy):
                for k in range(T):
                    to = i + 2 * k - 1
                    mine = (i * p.ngy + j) * T + k
                    row = (j + step) % p.ngy
                    if 0 <= to < p.ngx:
                        pairs.append((mine, (to * p.ngy + row) * T + 1 - k))
                    elif step:
                        pairs.append((mine, (i * p.ngy + row) * T + k))
                    elif p.ngy % 2 == 0:
                        pairs.append((mine, (i * p.ngy + (j ^ 1)) * T + k))
                    else:
                        pairs.append((mine, mine))
        return lax.ppermute(x, ("gx", "gy", "gz"), pairs)

    z_got = cores(z_msg)

    def main_body(s_ref, z_ref, b_ref, own_ref, par_ref, *y_refs):
        core = lax.axis_index("gz")
        if both:
            first = lax.axis_index("gy") == 0
            froms = [(jnp.where(first, Y - 3, 0), jnp.where(first, Y - 2, 0))]
        else:
            froms = [(Y - 3, Y - 2), (0, 0)]
        count = len(froms)
        for y_ref, d_ref, (three, two) in zip(y_refs[:count], y_refs[count:], froms):
            for src, half in ((s_ref, core), (z_ref, 1 - core)):
                at, to = half * y_part, half * d_part
                for comp in range(D):
                    for r in range(3):
                        v = p.raw(src, 0, comp, core, three + r)
                        p.put(y_ref, at, 3, comp, r, v)
                        p.put(d_ref, to, 3, comp, r, v)
                    for r in range(2):
                        if src is s_ref:
                            v = p.raw(b_ref, 0, comp, core, two + r)
                        else:
                            v = p.tile(src, z_load, Y, comp, two + r)
                        p.put(y_ref, at + y_load, 2, comp, r, v)
                for kind in range(2):
                    for r in range(3):
                        v = src[pl.ds(z_stat + (kind * Q + core) * Y + three + r, 1), :]
                        y_ref[pl.ds(at + y_stat + kind * 3 + r, 1), :] = v
                        d_ref[pl.ds(to + y_stat + kind * 3 + r, 1), :] = v
            for t in range(T):
                for ref, part, used in ((y_ref, y_part, y_load + FL * 2), (d_ref, d_part, y_load)):
                    if part > used:
                        ref[t * part + used : (t + 1) * part, :] = jnp.zeros((part - used, W), F32)
        for out, plane in ((own_ref, core), (par_ref, 1 - core)):
            for src, half in ((s_ref, core), (z_ref, 1 - core)):
                base = half * M
                for comp in range(D):
                    for r in range(Y):
                        p.put(out, base, Y, comp, r, p.raw(src, 0, comp, plane, r))
                for kind in range(2):
                    out[pl.ds(pl.multiple_of(base + (FL + kind) * Y, 8), Y), :] = src[
                        pl.ds(pl.multiple_of(z_stat + (kind * Q + plane) * Y, 8), Y), :
                    ]

    ways = (1,) if both else (1, -1)
    halos = len(ways)
    own_m, par_m, *sent = call(
        main_body,
        [(T * M, W)] * 2 + [(T * y_part, W)] * halos + [(T * d_part, W)] * halos,
        [z_msg, z_got, b_near],
        flops=10**5,
    )
    y_got = [rows_along(x, step) for x, step in zip(sent, ways)]
    far_m = planes_along(own_m)
    far_y = [planes_along(x, step) for x, step in zip(sent[halos:], ways)]
    par_y = [cores(x) for x in y_got]

    def halo(main, refs, part):
        row = lax.axis_index("gy")
        below = jnp.where(row > 0, 1.0, 0.0)
        above = jnp.where(row < p.ngy - 1, 1.0, 0.0)
        return main, refs[0], refs[-1], part, below, above

    def field_at(refs, t, comp, r):
        main, low, high, part, _, _ = refs
        if 3 <= r < Y + 3:
            return p.tile(main, t * M, Y, comp, r - 3)
        if r < 3:
            return p.tile(low, t * part, 3, comp, r)
        return p.tile(high, t * part, 3, comp, r - Y - 3)

    def const_at(refs, kind, t, r):
        main, low, high, part, below, above = refs
        if 3 <= r < Y + 3:
            at = t * M + (FL + kind) * Y + r - 3
            return main[at : at + 1, :]
        at = t * part + y_stat + kind * 3
        if r < 3:
            return low[at + r : at + r + 1, :] * below
        at += r - Y - 3
        return high[at : at + 1, :] * above

    def const_parts(refs, kind, t):
        main, low, high, part, below, above = refs
        at = t * part + y_stat + kind * 3
        to = t * M + (FL + kind) * Y
        return low[at : at + 3, :] * below, main[to : to + Y, :], high[at : at + 3, :] * above

    def points_body(node_ref, value_ref, out):
        core = lax.axis_index("gz")
        deep, across = p.depth
        base = ((lax.axis_index("gx") * Q + core) * across + lax.axis_index("gy") * Y - 2) * deep
        spots = jnp.concatenate([node_ref[c : c + 1, :] for c in range(C)], axis=1) - base
        total = C * n_loads
        if W & (W - 1):
            row = spots // W
            lane = spots - row * W
        else:
            row, lane = spots >> (W.bit_length() - 1), spots & (W - 1)
        hot = jnp.where(lax.broadcasted_iota(jnp.int32, (W, total), 0) == lane, 1.0, 0.0)
        rows8 = jnp.broadcast_to(row, (8, total))
        mine = lax.broadcasted_iota(jnp.int32, (8, total), 0)
        column = lax.broadcasted_iota(jnp.int32, (8, total), 1)
        mine = (column >= mine * n_loads) & (column < (mine + 1) * n_loads)
        values = []
        for comp in range(D):
            v = jnp.concatenate([value_ref[c, comp : comp + 1, :] for c in range(C)], axis=1)
            values.append(jnp.where(mine, jnp.broadcast_to(v, (8, total)), 0.0))
        left = [
            jnp.where(rows8 == r * T + t, values[comp], 0.0)
            for t in range(T)
            for comp in range(D)
            for r in range(R1)
        ]
        out[...] = lax.dot_general(
            jnp.concatenate(left, axis=0),
            hot,
            (((1,), (1,)), ((), ())),
            precision=lax.Precision.HIGHEST,
            preferred_element_type=F32,
        )

    n_loads = load_nodes.shape[1]
    (points,) = call(
        points_body,
        [(T * D * R1 * 8, W)],
        [load_nodes, jnp.swapaxes(load_values, 1, 2)],
        flops=10**6,
    )

    def loads_body(p_ref, b_ref, z_ref, *refs):
        ys, out = refs[:halos], refs[halos]
        core = lax.axis_index("gz")
        for half in range(2):
            t = core if half == 0 else 1 - core
            for comp in range(D):
                for r in range(R1):
                    if r < 2:
                        v = p.tile(ys[0], t * y_part + y_load, 2, comp, r)
                    elif r < Y + 2:
                        if half == 0:
                            v = p.raw(b_ref, 0, comp, core, r - 2)
                        else:
                            v = p.tile(z_ref, z_load, Y, comp, r - 2)
                    else:
                        v = p.tile(ys[-1], t * y_part + y_load, 2, comp, r - Y - 2)
                    at = t * (D * R1) + comp * R1 + r
                    out[at, 0:C, :] = v + p_ref[pl.ds(pl.multiple_of(at * 8, 8), C), :]

    (loaded,) = call(
        loads_body,
        [(T * D * R1, 8, W)],
        [points, b_near, z_got] + y_got,
        flops=10**6,
    )

    def near_start_body(own_m_ref, par_m_ref, *refs):
        modes_ref, part_ref, other_ref = refs[2 * halos :]
        core, sign = place()
        own, par = halo(own_m_ref, refs[:halos], y_part), halo(par_m_ref, refs[halos : 2 * halos], y_part)
        for refs, out in ((own, modes_ref), (par, other_ref)):
            modes_z(
                p,
                lambda t, k, r, refs=refs: field_at(refs, t, k, r),
                lambda t, r, refs=refs: const_at(refs, 1, t, r),
                R0,
                sign,
                out,
            )

        def modulus(t, e):
            return jnp.where(core == 0, const_at(own, 0, t, e), const_at(par, 0, t, e))

        def emit(t, comp, r, v):
            part_ref[(comp * R1 + r) * T + t, 0:C, :] = v

        layer(p, modes_ref, other_ref, False, modulus, R0, sign, emit)

    def field_shapes(count):
        return (6 * count * T, 8, W)

    modes, part = call(
        near_start_body,
        [field_shapes(R0), (D * R1 * T, 8, W)],
        [own_m, par_m] + y_got + par_y,
        [field_shapes(R0)],
        flops=10**6,
    )

    def far_start_body(far_m_ref, own_m_ref, par_m_ref, modes_ref, part_ref, load_ref, *refs):
        r_ref, d_ref, st_ref, other_ref = refs[3 * halos :]
        core, sign = place()
        own, par = halo(own_m_ref, refs[:halos], y_part), halo(par_m_ref, refs[halos : 2 * halos], y_part)
        far = halo(far_m_ref, refs[2 * halos : 3 * halos], d_part)
        column = lax.axis_index("gx")
        inside = jnp.where(core == 0, column > 0, column < p.ngx - 1)
        valid = jnp.where(inside, 1.0, 0.0)
        lane_rows = lax.broadcasted_iota(jnp.int32, (R1, W), 1)
        pad = up8(R0)
        sums = []
        for t in range(T):
            spans = ((0, 3), (3, Y), (Y + 3, 3))
            own_e, par_e, far_e = (const_parts(x, 0, t) for x in (own, par, far))
            own_m, par_m, far_m = (const_parts(x, 1, t) for x in (own, par, far))
            for n, (first, count) in enumerate(spans):
                for kind, v in (
                    (OWN, own_m[n]),
                    (PARTNER, par_m[n]),
                    (RECEIVED, far_m[n] * valid),
                    (NEAR, jnp.where(core == 0, own_e[n], par_e[n])),
                    (FAR, jnp.where(core == 0, far_e[n] * valid, own_e[n])),
                ):
                    to = (kind * T + t) * pad + first
                    st_ref[to : to + count, :] = v
            near, rest = (NEAR * T + t) * pad, (FAR * T + t) * pad
            sums.append(
                (st_ref[near : near + R1, :] + st_ref[rest : rest + R1, :])
                + (st_ref[near + 1 : near + 1 + R1, :] + st_ref[rest + 1 : rest + 1 + R1, :])
            )
        back = p.behind(sums, lane_rows)
        for t in range(T):
            around = sums[t] + back[t]
            at = (OWN * T + t) * pad + 1
            mov = st_ref[at : at + R1, :]
            guarded = jnp.where(mov > 0, around, 1.0)
            to = (SCALE * T + t) * pad + 1
            st_ref[to : to + R1, :] = mov / (CORNER * guarded) + (1.0 - mov)
        modes_z(
            p,
            lambda t, k, r: field_at(far, t, k, r),
            lambda t, r: static(p, st_ref, RECEIVED, t, r),
            R0,
            -sign,
            other_ref,
        )

        def emit(t, comp, r, v):
            force = v + part_ref[(comp * R1 + r) * T + t, 0:C, :]
            mov = p.wide(static(p, st_ref, OWN, t, r + 1))
            here = field_at(own, t, comp, r + 1)
            load = load_ref[t * (D * R1) + comp * R1 + r, 0:C, :]
            res = mov * (load - force) - (1.0 - mov) * here
            p.put(d_ref, t * N1, R1, comp, r, p.wide(static(p, st_ref, SCALE, t, r + 1)) * res)
            if 2 <= r < Y + 2:
                p.put(r_ref, t * N3, Y, comp, r - 2, res)

        layer(p, modes_ref, other_ref, True, lambda t, e: static(p, st_ref, FAR, t, e), R0, -sign, emit)

    res0, dir0, consts = call(
        far_start_body,
        [(T * N3, W), (T * N1, W), (6 * T * up8(R0), W)],
        [far_m, own_m, par_m, modes, part, loaded] + y_got + par_y + far_y,
        [field_shapes(R0)],
        flops=10**6,
    )

    def near_apply(own_ref, par_ref, st_ref, part_ref, modes_ref, other_ref, per, count, shift):
        _, sign = place()
        modes_z(p, lambda t, k, r: p.tile(own_ref, t * per, count, k, r), lambda t, r: static(p, st_ref, OWN, t, r + shift), count, sign, modes_ref)
        modes_z(p, lambda t, k, r: p.tile(par_ref, t * per, count, k, r), lambda t, r: static(p, st_ref, PARTNER, t, r + shift), count, sign, other_ref)

        def emit(t, comp, r, v):
            part_ref[(comp * (count - 2) + r) * T + t, 0:C, :] = v

        def more(t, comp, r, v):
            at = (comp * (count - 2) + r) * T + t
            part_ref[at, 0:C, :] = part_ref[at, 0:C, :] + v

        layer(p, modes_ref, other_ref, False, lambda t, e: static(p, st_ref, NEAR, t, e + shift), count, sign, emit)
        single(p, modes_ref, lambda t, e: static(p, st_ref, FAR, t, e + shift), count, -sign, -1, more)

    def far_apply(far_ref, own_ref, st_ref, part_ref, other_ref, per, count, shift, emit):
        _, sign = place()
        modes_z(p, lambda t, k, r: p.tile(far_ref, t * per, count, k, r), lambda t, r: static(p, st_ref, RECEIVED, t, r + shift), count, -sign, other_ref)

        def finish(t, comp, r, v):
            force = v + part_ref[(comp * (count - 2) + r) * T + t, 0:C, :]
            mov = p.wide(static(p, st_ref, OWN, t, r + 1 + shift))
            here = p.tile(own_ref, t * per, count, comp, r + 1)
            emit(t, comp, r, mov * force + (1.0 - mov) * here, here)

        single(p, other_ref, lambda t, e: static(p, st_ref, FAR, t, e + shift), count, -sign, 1, finish)

    far_d = planes_along(dir0)
    par_d = cores(dir0)

    def near_one_body(own_ref, par_ref, st_ref, part_ref, modes_ref, other_ref):
        near_apply(own_ref, par_ref, st_ref, part_ref, modes_ref, other_ref, N1, R1, 1)

    (part1,) = call(
        near_one_body, [(D * R2 * T, 8, W)], [dir0, par_d, consts], [field_shapes(R1)] * 2, flops=10**6
    )

    def far_one_body(far_ref, own_ref, st_ref, part_ref, q_ref, w_ref, other_ref):
        if N2 > FL * R2:
            for t in range(T):
                w_ref[t * N2 + FL * R2 : (t + 1) * N2, :] = jnp.zeros((N2 - FL * R2, W), F32)

        def emit(t, comp, r, image, here):
            scale = p.wide(static(p, st_ref, SCALE, t, r + 2))
            p.put(w_ref, t * N2, R2, comp, r, scale * image - here)
            if 1 <= r < Y + 1:
                p.put(q_ref, t * N3, Y, comp, r - 1, image)

        far_apply(far_ref, own_ref, st_ref, part_ref, other_ref, N1, R1, 1, emit)

    image0, second = call(
        far_one_body,
        [(T * N3, W), (T * N2, W)],
        [far_d, dir0, consts, part1],
        [field_shapes(R1)],
        flops=10**6,
    )

    far_w = planes_along(second)
    par_w = cores(second)

    def columns(number, sums, lane):
        table = jnp.zeros((C, W), F32)
        for j in range(C):
            column = jnp.sum(sums[j], axis=1, keepdims=True)
            table = jnp.where(lane == number * C + j, column, table)
        return table

    def gram_body(d_ref, q_ref, r_ref, w_ref, g_ref, mine_ref, send_ref):
        core = lax.axis_index("gz")
        lane = p.lanes()
        sums = [[jnp.zeros((C, W), F32) for _ in range(C)] for _ in range(3)]
        for t in range(T):
            for comp in range(D):
                for r in range(Y):
                    d = p.tile(d_ref, t * N1, R1, comp, r + 2)
                    w = p.tile(w_ref, t * N2, R2, comp, r + 1)
                    for j in range(C):
                        at = t * N3 + (j * D + comp) * Y + r
                        q = q_ref[at : at + 1, :]
                        sums[0][j] = sums[0][j] + d * q
                        sums[1][j] = sums[1][j] + d * r_ref[at : at + 1, :]
                        sums[2][j] = sums[2][j] + w * q
        table = columns(0, sums[0], lane) + columns(1, sums[1], lane) + columns(2, sums[2], lane)
        g_ref[...] = jnp.zeros((8, W), F32)
        g_ref[0:C, :] = table
        for out, t in ((mine_ref, core), (send_ref, 1 - core)):
            for number, src in enumerate((r_ref, q_ref)):
                out[number * N3 : (number + 1) * N3, :] = src[pl.ds(pl.multiple_of(t * N3, 8), N3), :]
            for comp in range(D):
                for r in range(Y):
                    p.put(out, 2 * N3, Y, comp, r, p.tile(d_ref, t * N1, R1, comp, r + 2))
                    p.put(out, 3 * N3, Y, comp, r, p.tile(w_ref, t * N2, R2, comp, r + 1))

    gram3, mine, send = call(gram_body, [(8, W), (4 * N3, W), (4 * N3, W)], [dir0, image0, res0, second], flops=10**6)

    def near_two_body(own_ref, par_ref, st_ref, part_ref, modes_ref, other_ref):
        near_apply(own_ref, par_ref, st_ref, part_ref, modes_ref, other_ref, N2, R2, 2)

    (part2,) = call(
        near_two_body, [(D * Y * T, 8, W)], [second, par_w, consts], [field_shapes(R2)] * 2, flops=10**6
    )
    kept = cores(send)

    def far_two_body(far_ref, own_ref, st_ref, part_ref, gram_ref, mine_ref, send_ref, other_ref, u_ref):
        core = lax.axis_index("gz")

        def emit(t, comp, r, image, here):
            p.put(u_ref, t * N3, Y, comp, r, image)
            sums_in.append((image, t, comp, r))

        sums_in = []
        far_apply(far_ref, own_ref, st_ref, part_ref, other_ref, N2, R2, 2, emit)
        sums = [jnp.zeros((C, W), F32) for _ in range(C)]
        for _, t, comp, r in sums_in:
            u = p.tile(u_ref, t * N3, Y, comp, r)
            for j in range(C):
                at = t * N2 + (j * D + comp) * R2 + r + 1
                sums[j] = sums[j] + u * own_ref[at : at + 1, :]
        table = gram_ref[0:C, :] + columns(3, sums, p.lanes())
        for out, t in ((mine_ref, core), (send_ref, 1 - core)):
            out[0:N3, :] = u_ref[pl.ds(pl.multiple_of(t * N3, 8), N3), :]
            out[N3 : N3 + 8, :] = jnp.zeros((8, W), F32)
            out[N3 : N3 + C, :] = table

    mine_u, send_u = call(
        far_two_body,
        [(N3 + 8, W), (N3 + 8, W)],
        [far_w, second, consts, part2, gram3],
        [field_shapes(R2), (T * N3, W)],
        flops=10**6,
    )
    kept_u = cores(send_u)

    table = mine_u[N3 : N3 + 8, :] + kept_u[N3 : N3 + 8, :]

    def crossed(x, axis, size, step):
        pairs = [(i * T + k, (i ^ step) * T + 1 - k) for i in range(size) for k in range(T)]
        return lax.ppermute(x, (axis, "gz"), pairs)

    for axis, size in (("gy", p.ngy), ("gx", p.ngx)):
        if size & (size - 1):
            table = lax.psum(table, axis)
            continue
        step = 1
        while step < size:
            if step * 2 < size:
                one, two, three = (crossed(table, axis, size, step * k) for k in (1, 2, 3))
                table = (table + one) + (two + three)
                step *= 4
            else:
                table = table + crossed(table, axis, size, step)
                step *= 2

    def final_body(
        g_ref, x_ref, mine_ref, mine_u_ref, kept_ref, kept_u_ref, out_hbm, res_hbm, a_ref, out_ref, res_ref, sems
    ):
        core = lax.axis_index("gz")
        lane = lax.broadcasted_iota(jnp.int32, (1, W), 1)

        def splat(row, at):
            return jnp.broadcast_to(row[:, at : at + 1], (1, W))

        def factor(rows, first):
            a = {(i, j): splat(rows[i], first + j) for i in range(C) for j in range(i + 1)}
            low, inv = {}, []
            for k in range(C):
                inv.append(1.0 / a[k, k])
                for i in range(k + 1, C):
                    low[i, k] = a[i, k] * inv[k]
                for i in range(k + 1, C):
                    for j in range(k + 1, i + 1):
                        a[i, j] = a[i, j] - low[i, k] * a[j, k]
            return low, inv

        def solve(factors, right):
            low, inv = factors
            y = []
            for i in range(C):
                v = right[i]
                for k in range(i):
                    v = v - low[i, k] * y[k]
                y.append(v)
            x = [None] * C
            for i in reversed(range(C)):
                v = y[i] * inv[i]
                for k in range(i + 1, C):
                    v = v - low[k, i] * x[k]
                x[i] = v
            return x

        rows = [g_ref[i : i + 1, :] for i in range(C)]
        first = solve(factor(rows, 0), rows)
        reduced = []
        for i in range(C):
            v = jnp.where(
                lane < 2 * C, pltpu.roll(rows[i], C, 1) - rows[i], pltpu.roll(rows[i], W - C, 1)
            )
            for k in range(C):
                v = v - splat(rows[i], 2 * C + k) * first[k]
            reduced.append(v)
        on_second = solve(factor(reduced, 2 * C), reduced)
        for i in range(C):
            v = first[i]
            for k in range(C):
                v = v - splat(first[i], 2 * C + k) * on_second[k]
            for k in range(C):
                a_ref[i * C + k] = jnp.broadcast_to(v[:, C + k : C + k + 1], (Y, W))
                a_ref[C * C + i * C + k] = jnp.broadcast_to(on_second[i][:, C + k : C + k + 1], (Y, W))
        halves = ((mine_ref, mine_u_ref, core), (kept_ref, kept_u_ref, 1 - core))
        moves = []
        for number in range(2):
            target = (out_ref, res_ref)[number]
            for src, src_u, plane in halves:
                for comp in range(D):
                    fs = [(j * D + comp) * Y for j in range(C)]
                    at = N3 if number else 2 * N3
                    v = [src[at + f : at + f + Y, :] for f in fs]
                    u = [src_u[f : f + Y, :] if number else src[3 * N3 + f : 3 * N3 + f + Y, :] for f in fs]
                    for i in range(C):
                        at = pl.ds(pl.multiple_of(((i * D + comp) * Q + plane) * Y, 8), Y)
                        total = a_ref[i] * v[0] + a_ref[C * C + i] * u[0]
                        for j in range(1, C):
                            total = total + (a_ref[j * C + i] * v[j] + a_ref[C * C + j * C + i] * u[j])
                        if number:
                            target[at, :] = src[fs[i] : fs[i] + Y, :] - total
                        else:
                            target[at, :] = x_ref[at, :] + total
            moves.append(pltpu.make_async_copy(target, (out_hbm, res_hbm)[number], sems.at[number]))
            moves[-1].start()
        for move in moves:
            move.wait()

    out, res = call(
        final_body,
        [(n_raw, W)] * 2,
        [table, z_msg, mine, mine_u, kept, kept_u],
        [(2 * C * C, Y, W), (n_raw, W), (n_raw, W), pltpu.SemaphoreType.DMA((2,))],
        flops=10**5,
        far_out=True,
    )
    return out.reshape(start.shape), res.reshape(start.shape)


def solution(mesh):
    in_specs = (
        P(("grp", "gx"), "gy", "gz"),
        P(("grp", "gx"), "gy", "gz"),
        P("grp", None, "gx", "gy", "gz"),
        P("grp", None, "gx", "gy", "gz"),
        P("grp", None),
        P("grp", None, None),
    )
    out_specs = (P("grp", None, "gx", "gy", "gz"), P("grp", None, "gx", "gy", "gz"))

    def body(*args):
        return shards(dict(mesh.shape), *args)

    return jax.shard_map(body, mesh=mesh, in_specs=in_specs, out_specs=out_specs, check_vma=False)
```

```python
import jax
import jax.numpy as jnp
from jax import lax
from jax.experimental import pallas as pl
from jax.experimental.pallas import tpu as pltpu
from jax.sharding import PartitionSpec as P


LEVELS = 16

soft_modulus = 0.05
poisson_ratio = 0.3
lame = poisson_ratio / ((1.0 + poisson_ratio) * (1.0 - 2.0 * poisson_ratio))
shear = 1.0 / (2.0 * (1.0 + poisson_ratio))
THREE, TWO, ONE = 1.0 / 16.0, 1.0 / 48.0, 1.0 / 144.0
CORNER = THREE * (lame + 4.0 * shear) + 2.0 * TWO * (lame + 4.0 * shear) + ONE * (lame + 4.0 * shear)

VMEM, SMEM = pltpu.VMEM, pltpu.SMEM
F32 = jnp.float32


def up8(n):
    return -(-n // 8) * 8


def call(body, outs, ins, scratch=(), flops=0, smem=(), hbm=(), far_out=False):
    kinds = [SMEM if i in smem else pltpu.HBM if i in hbm else VMEM for i in range(len(ins))]
    ins = [x if k is SMEM else pltpu.with_memory_space_constraint(x, k) for x, k in zip(ins, kinds)]
    return pl.pallas_call(
        body,
        out_shape=[jax.ShapeDtypeStruct(s, F32) if far_out else VMEM(s, F32) for s in outs],
        in_specs=[pl.BlockSpec(memory_space=k) for k in kinds],
        out_specs=[pl.BlockSpec(memory_space=pl.ANY if far_out else VMEM)] * len(outs),
        scratch_shapes=[VMEM(s, F32) if isinstance(s, tuple) else s for s in scratch],
        compiler_params=pltpu.CompilerParams(vmem_limit_bytes=16 * 2**20),
        cost_estimate=pl.CostEstimate(flops=flops, bytes_accessed=0, transcendentals=0),
    )(*ins)


class Plan:
    def __init__(self, block, mesh):
        self.cases, self.comps, self.planes, self.rows, self.width = block
        self.fields = self.cases * self.comps
        self.ngx, self.ngy, self.tiles = mesh["gx"], mesh["gy"], mesh["gz"]
        if not (self.planes == self.tiles == 2 and self.rows % 8 == 0 and self.comps == 3):
            raise ValueError("block shape")
        self.depth = (self.tiles * self.width, self.ngy * self.rows)
        self.r0 = self.rows + 6
        self.main = up8((self.fields + 4) * self.rows)

    def per(self, count):
        return up8(self.fields * count)

    def tile(self, ref, base, count, comp, row):
        return ref[pl.ds(base + comp * count + row, self.cases, stride=self.comps * count), :]

    def put(self, ref, base, count, comp, row, value):
        ref[pl.ds(base + comp * count + row, self.cases, stride=self.comps * count), :] = value

    def raw(self, ref, base, comp, plane, row):
        start = base + (comp * self.planes + plane) * self.rows + row
        return ref[pl.ds(start, self.cases, stride=self.comps * self.planes * self.rows), :]

    def lanes(self, count=None):
        return lax.broadcasted_iota(jnp.int32, (count or self.cases, self.width), 1)

    def ahead(self, tiles, lane):
        moved = [pltpu.roll(v, self.width - 1, 1) for v in tiles]
        moved.append(jnp.zeros_like(tiles[0]))
        return [jnp.where(lane == self.width - 1, moved[t + 1], moved[t]) for t in range(self.tiles)]

    def behind(self, tiles, lane):
        moved = [pltpu.roll(v, 1, 1) for v in tiles]
        moved = [jnp.zeros_like(tiles[0])] + moved
        return [jnp.where(lane == 0, moved[t], moved[t + 1]) for t in range(self.tiles)]

    def wide(self, row):
        return jnp.broadcast_to(row, (self.cases, self.width))


def modes_z(p, load, mask, count, sign, out):
    lane = p.lanes()
    for r in range(count):
        m = [p.wide(mask(t, r)) for t in range(p.tiles)]
        ms = [x * sign for x in m]
        for comp in range(3):
            v = [load(t, comp, r) * (ms[t] if comp == 0 else m[t]) for t in range(p.tiles)]
            n = p.ahead(v, lane)
            for t in range(p.tiles):
                out[((comp * 2) * count + r) * p.tiles + t, 0 : p.cases, :] = v[t] + n[t]
                out[((comp * 2 + 1) * count + r) * p.tiles + t, 0 : p.cases, :] = n[t] - v[t]


def layer(p, own, other, flip, modulus, count, sign, emit):
    lane = p.lanes()

    def modes_y(ref, e, t):
        found = {}
        for comp in range(3):
            for c in (0, 1):
                at = ((comp * 2 + c) * count + e) * p.tiles + t
                a = ref[at, 0 : p.cases, :]
                b = ref[at + p.tiles, 0 : p.cases, :]
                found[comp, 0, c] = a + b
                found[comp, 1, c] = b - a
        return found

    carry = {}
    for e in range(count - 1):
        done = {}
        for t in range(p.tiles):
            near, far = modes_y(own, e, t), modes_y(other, e, t)
            u = [{}, {}, {}]
            for (comp, b, c), x in near.items():
                y = far[comp, b, c]
                plus, minus = (y - x, y + x) if flip and comp == 0 else (y + x, y - x)
                u[comp][0, b, c], u[comp][1, b, c] = plus, minus
            ux, uy, uz = u
            mod = p.wide(modulus(t, e))
            ea, eb, es = mod * (THREE * lame), mod * (2.0 * THREE * shear), mod * (THREE * shear)
            ed, ee, ef = mod * (TWO * (lame + 3.0 * shear)), mod * (TWO * lame), mod * (TWO * shear)
            eg = mod * (ONE * (lame + 4.0 * shear))
            q = ea * (ux[1, 0, 0] + uy[0, 1, 0] + uz[0, 0, 1])
            sxy = es * (uy[1, 0, 0] + ux[0, 1, 0])
            syz = es * (uz[0, 1, 0] + uy[0, 0, 1])
            sxz = es * (uz[1, 0, 0] + ux[0, 0, 1])
            s = ux[0, 1, 1] + uy[1, 0, 1] + uz[1, 1, 0]
            gx = {
                (1, 0, 0): q + eb * ux[1, 0, 0],
                (0, 1, 0): sxy,
                (0, 0, 1): sxz,
                (1, 0, 1): ed * ux[1, 0, 1] + ee * uy[0, 1, 1],
                (1, 1, 0): ed * ux[1, 1, 0] + ee * uz[0, 1, 1],
                (0, 1, 1): ef * (s + ux[0, 1, 1]),
                (1, 1, 1): eg * ux[1, 1, 1],
            }
            gy = {
                (0, 1, 0): q + eb * uy[0, 1, 0],
                (1, 0, 0): sxy,
                (0, 0, 1): syz,
                (0, 1, 1): ed * uy[0, 1, 1] + ee * ux[1, 0, 1],
                (1, 1, 0): ed * uy[1, 1, 0] + ee * uz[1, 0, 1],
                (1, 0, 1): ef * (s + uy[1, 0, 1]),
                (1, 1, 1): eg * uy[1, 1, 1],
            }
            gz = {
                (0, 0, 1): q + eb * uz[0, 0, 1],
                (1, 0, 0): sxz,
                (0, 1, 0): syz,
                (0, 1, 1): ed * uz[0, 1, 1] + ee * ux[1, 1, 0],
                (1, 0, 1): ed * uz[1, 0, 1] + ee * uy[1, 1, 0],
                (1, 1, 0): ef * (s + uz[1, 1, 0]),
                (1, 1, 1): eg * uz[1, 1, 1],
            }
            for comp, g in enumerate((gx, gy, gz)):
                h = {bc: g[(0,) + bc] - g[(1,) + bc] for bc in ((0, 1), (1, 0), (1, 1))}
                h[0, 0] = -g[1, 0, 0]
                for c in (0, 1):
                    if e:
                        done[comp, c, t] = carry[comp, c, t] + (h[0, c] - h[1, c])
                    carry[comp, c, t] = h[0, c] + h[1, c]
        if e:
            for comp in range(3):
                low = [done[comp, 0, t] - done[comp, 1, t] for t in range(p.tiles)]
                high = [done[comp, 0, t] + done[comp, 1, t] for t in range(p.tiles)]
                back = p.behind(high, lane)
                for t in range(p.tiles):
                    total = low[t] + back[t]
                    emit(t, comp, e - 1, total * sign if comp == 0 else total)


def single(p, ref, modulus, count, sign, way, emit, flip=False):
    lane = p.lanes()
    cq, cb, cs = THREE * lame, 2.0 * THREE * shear, THREE * shear
    cd, ce, cf = TWO * (lame + 3.0 * shear), TWO * lame, TWO * shear
    cg = ONE * (lame + 4.0 * shear)
    carry = {}
    for e in range(count - 1):
        done = {}
        for t in range(p.tiles):
            m = [{}, {}, {}]
            for comp in range(3):
                for c in (0, 1):
                    at = ((comp * 2 + c) * count + e) * p.tiles + t
                    a = ref[at, 0 : p.cases, :]
                    b = ref[at + p.tiles, 0 : p.cases, :]
                    if flip and comp == 0:
                        m[comp][0, c], m[comp][1, c] = -a - b, a - b
                    else:
                        m[comp][0, c], m[comp][1, c] = a + b, b - a
            x, y, z = m
            mod = p.wide(modulus(t, e))
            q = cq * (x[0, 0] + y[1, 0] + z[0, 1])
            sxy = cs * (y[0, 0] + x[1, 0])
            sxz = cs * (z[0, 0] + x[0, 1])
            pair = z[1, 0] + y[0, 1]
            syz = cs * pair
            s = x[1, 1] + pair
            if way > 0:
                sh = {
                    (0, 1, 0): sxy - (cd * x[1, 0] + ce * z[1, 1]),
                    (0, 0, 1): sxz - (cd * x[0, 1] + ce * y[1, 1]),
                    (0, 1, 1): (2.0 * cf - cg) * x[1, 1] + cf * pair,
                    (1, 0, 0): -sxy,
                    (1, 1, 0): q + ((cb - cd) * y[1, 0] - ce * z[0, 1]),
                    (1, 0, 1): syz - cf * (s + y[0, 1]),
                    (1, 1, 1): (cd - cg) * y[1, 1] + ce * x[0, 1],
                    (2, 0, 0): -sxz,
                    (2, 0, 1): q + ((cb - cd) * z[0, 1] - ce * y[1, 0]),
                    (2, 1, 0): syz - cf * (s + z[1, 0]),
                    (2, 1, 1): (cd - cg) * z[1, 1] + ce * x[1, 0],
                }
            else:
                sh = {
                    (0, 1, 0): -sxy - (cd * x[1, 0] + ce * z[1, 1]),
                    (0, 0, 1): -sxz - (cd * x[0, 1] + ce * y[1, 1]),
                    (0, 1, 1): (-2.0 * cf - cg) * x[1, 1] - cf * pair,
                    (1, 0, 0): sxy,
                    (1, 1, 0): q + ((cb + cd) * y[1, 0] + ce * z[0, 1]),
                    (1, 0, 1): syz + cf * (s + y[0, 1]),
                    (1, 1, 1): (cd + cg) * y[1, 1] + ce * x[0, 1],
                    (2, 0, 0): sxz,
                    (2, 0, 1): q + ((cb + cd) * z[0, 1] + ce * y[1, 0]),
                    (2, 1, 0): syz + cf * (s + z[1, 0]),
                    (2, 1, 1): (cd + cg) * z[1, 1] + ce * x[1, 0],
                }
            sh[0, 0, 0] = -(q + cb * x[0, 0])
            for comp in range(3):
                h = {bc: mod * sh[(comp,) + bc] for bc in ((0, 0), (0, 1), (1, 0), (1, 1))}
                for c in (0, 1):
                    if e:
                        done[comp, c, t] = carry[comp, c, t] + (h[0, c] - h[1, c])
                    carry[comp, c, t] = h[0, c] + h[1, c]
        if e:
            for comp in range(3):
                low = [done[comp, 0, t] - done[comp, 1, t] for t in range(p.tiles)]
                high = [done[comp, 0, t] + done[comp, 1, t] for t in range(p.tiles)]
                back = p.behind(high, lane)
                for t in range(p.tiles):
                    total = low[t] + back[t]
                    emit(t, comp, e - 1, total * sign if comp == 0 else total)


OWN, PARTNER, RECEIVED, NEAR, FAR, SCALE, BEYOND, PAST, SCALE_FAR = range(9)


def static(p, ref, kind, t, row):
    at = (kind * p.tiles + t) * up8(p.r0) + row
    return ref[at : at + 1, :]


def place():
    core = lax.axis_index("gz")
    return core, 1.0 - 2.0 * core.astype(F32)


def shards(mesh, design, supports, body_load, start, load_nodes, load_values):
    p = Plan(body_load.shape, mesh)
    C, D, Y, W, T, FL = p.cases, p.comps, p.rows, p.width, p.tiles, p.fields
    Q = p.planes
    n_raw = FL * Q * Y
    z_load = n_raw
    z_stat = z_load + FL * Y
    z_rows = z_stat + 2 * Q * Y
    y_stat = FL * 3
    y_load = y_stat + 6
    y_part = up8(y_load + FL * 2)
    d_part = up8(y_stat + 12)
    R0, R1, R2 = Y + 6, Y + 4, Y + 2
    N1, N2, N3 = p.per(R1), p.per(R2), p.per(Y)
    M = p.main
    both = p.ngy == 2

    x0 = start.reshape(n_raw, W)
    bl = body_load.reshape(n_raw, W)
    de = design.reshape(Q * Y, W)
    su = supports.reshape(Q * Y, W)

    def gather_body(x_hbm, b_hbm, d_hbm, s_hbm, z_ref, b_ref, *refs):
        d_ref, s_ref, sems = refs
        core = lax.axis_index("gz")
        moves = [
            pltpu.make_async_copy(src, dst, sems.at[i])
            for i, (src, dst) in enumerate(
                ((x_hbm, z_ref.at[pl.ds(0, n_raw)]), (b_hbm, b_ref), (d_hbm, d_ref), (s_hbm, s_ref))
            )
        ]
        for move in moves:
            move.start()
        moves[2].wait()
        density = (d_ref[...].astype(F32) + 1.0) / LEVELS
        z_ref[z_stat : z_stat + Q * Y, :] = (
            soft_modulus + (1.0 - soft_modulus) * density * density * density
        )
        moves[3].wait()
        z_ref[z_stat + Q * Y : z_rows, :] = 1.0 - s_ref[...].astype(F32)
        moves[1].wait()
        for f in range(FL):
            z_ref[z_load + f * Y : z_load + (f + 1) * Y, :] = b_ref[
                pl.ds(pl.multiple_of((f * Q + 1 - core) * Y, 8), Y), :
            ]
        moves[0].wait()

    z_msg, b_near = call(
        gather_body,
        [(z_rows, W), (n_raw, W)],
        [x0, bl, de, su],
        [VMEM((Q * Y, W), jnp.int32), VMEM((Q * Y, W), jnp.int32), pltpu.SemaphoreType.DMA((4,))],
        flops=10**5,
        hbm=(0, 1, 2, 3),
    )

    def cores(x):
        return lax.ppermute(x, "gz", [(i, 1 - i) for i in range(T)])

    def rows_along(x, step):
        return lax.ppermute(x, "gy", [(i, (i + step) % p.ngy) for i in range(p.ngy)])

    def planes_along(x, step=0):
        pairs = []
        for i in range(p.ngx):
            for j in range(p.ngy):
                for k in range(T):
                    to = i + 2 * k - 1
                    mine = (i * p.ngy + j) * T + k
                    row = (j + step) % p.ngy
                    if 0 <= to < p.ngx:
                        pairs.append((mine, (to * p.ngy + row) * T + 1 - k))
                    elif step:
                        pairs.append((mine, (i * p.ngy + row) * T + k))
                    elif p.ngy % 2 == 0:
                        pairs.append((mine, (i * p.ngy + (j ^ 1)) * T + k))
                    else:
                        pairs.append((mine, mine))
        return lax.ppermute(x, ("gx", "gy", "gz"), pairs)

    z_got = cores(z_msg)

    def main_body(s_ref, z_ref, b_ref, own_ref, par_ref, *y_refs):
        core = lax.axis_index("gz")
        if both:
            first = lax.axis_index("gy") == 0
            froms = [(jnp.where(first, Y - 3, 0), jnp.where(first, Y - 2, 0))]
        else:
            froms = [(Y - 3, Y - 2), (0, 0)]
        count = len(froms)
        for y_ref, d_ref, (three, two) in zip(y_refs[:count], y_refs[count:], froms):
            for src, half in ((s_ref, core), (z_ref, 1 - core)):
                at, to = half * y_part, half * d_part
                for comp in range(D):
                    for r in range(3):
                        v = p.raw(src, 0, comp, core, three + r)
                        p.put(y_ref, at, 3, comp, r, v)
                        p.put(d_ref, to, 3, comp, r, v)
                    for r in range(2):
                        if src is s_ref:
                            v = p.raw(b_ref, 0, comp, core, two + r)
                        else:
                            v = p.tile(src, z_load, Y, comp, two + r)
                        p.put(y_ref, at + y_load, 2, comp, r, v)
                for kind in range(2):
                    for r in range(3):
                        v = src[pl.ds(z_stat + (kind * Q + core) * Y + three + r, 1), :]
                        y_ref[pl.ds(at + y_stat + kind * 3 + r, 1), :] = v
                        d_ref[pl.ds(to + y_stat + kind * 3 + r, 1), :] = v
                        d_ref[pl.ds(to + y_stat + 6 + kind * 3 + r, 1), :] = src[
                            pl.ds(z_stat + (kind * Q + 1 - core) * Y + three + r, 1), :
                        ]
            for t in range(T):
                for ref, part, used in ((y_ref, y_part, y_load + FL * 2), (d_ref, d_part, y_stat + 12)):
                    if part > used:
                        ref[t * part + used : (t + 1) * part, :] = jnp.zeros((part - used, W), F32)
        for out, plane in ((own_ref, core), (par_ref, 1 - core)):
            for src, half in ((s_ref, core), (z_ref, 1 - core)):
                base = half * M
                for comp in range(D):
                    for r in range(Y):
                        p.put(out, base, Y, comp, r, p.raw(src, 0, comp, plane, r))
                for kind in range(4):
                    of = plane if kind < 2 else 1 - plane
                    out[pl.ds(pl.multiple_of(base + (FL + kind) * Y, 8), Y), :] = src[
                        pl.ds(pl.multiple_of(z_stat + (kind % 2 * Q + of) * Y, 8), Y), :
                    ]

    ways = (1,) if both else (1, -1)
    halos = len(ways)
    own_m, par_m, *sent = call(
        main_body,
        [(T * M, W)] * 2 + [(T * y_part, W)] * halos + [(T * d_part, W)] * halos,
        [z_msg, z_got, b_near],
        flops=10**5,
    )
    y_got = [rows_along(x, step) for x, step in zip(sent, ways)]
    far_m = planes_along(own_m)
    far_y = [planes_along(x, step) for x, step in zip(sent[halos:], ways)]
    par_y = [cores(x) for x in y_got]

    def halo(main, refs, part):
        row = lax.axis_index("gy")
        below = jnp.where(row > 0, 1.0, 0.0)
        above = jnp.where(row < p.ngy - 1, 1.0, 0.0)
        return main, refs[0], refs[-1], part, below, above

    def field_at(refs, t, comp, r):
        main, low, high, part, _, _ = refs
        if 3 <= r < Y + 3:
            return p.tile(main, t * M, Y, comp, r - 3)
        if r < 3:
            return p.tile(low, t * part, 3, comp, r)
        return p.tile(high, t * part, 3, comp, r - Y - 3)

    def const_at(refs, kind, t, r):
        main, low, high, part, below, above = refs
        if 3 <= r < Y + 3:
            at = t * M + (FL + kind) * Y + r - 3
            return main[at : at + 1, :]
        at = t * part + y_stat + kind * 3
        if r < 3:
            return low[at + r : at + r + 1, :] * below
        at += r - Y - 3
        return high[at : at + 1, :] * above

    def const_parts(refs, kind, t):
        main, low, high, part, below, above = refs
        at = t * part + y_stat + kind * 3
        to = t * M + (FL + kind) * Y
        return low[at : at + 3, :] * below, main[to : to + Y, :], high[at : at + 3, :] * above

    def points_body(node_ref, value_ref, out):
        core = lax.axis_index("gz")
        deep, across = p.depth
        base = ((lax.axis_index("gx") * Q + core) * across + lax.axis_index("gy") * Y - 2) * deep
        spots = jnp.concatenate([node_ref[c : c + 1, :] for c in range(C)], axis=1) - base
        total = C * n_loads
        if W & (W - 1):
            row = spots // W
            lane = spots - row * W
        else:
            row, lane = spots >> (W.bit_length() - 1), spots & (W - 1)
        hot = jnp.where(lax.broadcasted_iota(jnp.int32, (W, total), 0) == lane, 1.0, 0.0)
        rows8 = jnp.broadcast_to(row, (8, total))
        mine = lax.broadcasted_iota(jnp.int32, (8, total), 0)
        column = lax.broadcasted_iota(jnp.int32, (8, total), 1)
        mine = (column >= mine * n_loads) & (column < (mine + 1) * n_loads)
        values = []
        for comp in range(D):
            v = jnp.concatenate([value_ref[c, comp : comp + 1, :] for c in range(C)], axis=1)
            values.append(jnp.where(mine, jnp.broadcast_to(v, (8, total)), 0.0))
        left = [
            jnp.where(rows8 == r * T + t, values[comp], 0.0)
            for t in range(T)
            for comp in range(D)
            for r in range(R1)
        ]
        out[...] = lax.dot_general(
            jnp.concatenate(left, axis=0),
            hot,
            (((1,), (1,)), ((), ())),
            precision=lax.Precision.HIGHEST,
            preferred_element_type=F32,
        )

    n_loads = load_nodes.shape[1]
    (points,) = call(
        points_body,
        [(T * D * R1 * 8, W)],
        [load_nodes, jnp.swapaxes(load_values, 1, 2)],
        flops=10**6,
    )

    def loads_body(p_ref, b_ref, z_ref, *refs):
        ys, out = refs[:halos], refs[halos]
        core = lax.axis_index("gz")
        for half in range(2):
            t = core if half == 0 else 1 - core
            for comp in range(D):
                for r in range(R1):
                    if r < 2:
                        v = p.tile(ys[0], t * y_part + y_load, 2, comp, r)
                    elif r < Y + 2:
                        if half == 0:
                            v = p.raw(b_ref, 0, comp, core, r - 2)
                        else:
                            v = p.tile(z_ref, z_load, Y, comp, r - 2)
                    else:
                        v = p.tile(ys[-1], t * y_part + y_load, 2, comp, r - Y - 2)
                    at = t * (D * R1) + comp * R1 + r
                    out[at, 0:C, :] = v + p_ref[pl.ds(pl.multiple_of(at * 8, 8), C), :]

    (loaded,) = call(
        loads_body,
        [(T * D * R1, 8, W)],
        [points, b_near, z_got] + y_got,
        flops=10**6,
    )

    def near_start_body(own_m_ref, par_m_ref, *refs):
        modes_ref, part_ref, other_ref = refs[2 * halos :]
        core, sign = place()
        own, par = halo(own_m_ref, refs[:halos], y_part), halo(par_m_ref, refs[halos : 2 * halos], y_part)
        for refs, out in ((own, modes_ref), (par, other_ref)):
            modes_z(
                p,
                lambda t, k, r, refs=refs: field_at(refs, t, k, r),
                lambda t, r, refs=refs: const_at(refs, 1, t, r),
                R0,
                sign,
                out,
            )

        def modulus(t, e):
            return jnp.where(core == 0, const_at(own, 0, t, e), const_at(par, 0, t, e))

        def emit(t, comp, r, v):
            part_ref[(comp * R1 + r) * T + t, 0:C, :] = v

        layer(p, modes_ref, other_ref, False, modulus, R0, sign, emit)

    def field_shapes(count):
        return (6 * count * T, 8, W)

    modes, part = call(
        near_start_body,
        [field_shapes(R0), (D * R1 * T, 8, W)],
        [own_m, par_m] + y_got + par_y,
        [field_shapes(R0)],
        flops=10**6,
    )

    def far_start_body(far_m_ref, own_m_ref, par_m_ref, modes_ref, part_ref, load_ref, *refs):
        r_ref, d_ref, st_ref, other_ref = refs[3 * halos :]
        core, sign = place()
        own, par = halo(own_m_ref, refs[:halos], y_part), halo(par_m_ref, refs[halos : 2 * halos], y_part)
        far = halo(far_m_ref, refs[2 * halos : 3 * halos], d_part)
        column = lax.axis_index("gx")
        inside = jnp.where(core == 0, column > 0, column < p.ngx - 1)
        valid = jnp.where(inside, 1.0, 0.0)
        lane_rows = lax.broadcasted_iota(jnp.int32, (R1, W), 1)
        pad = up8(R0)
        for t in range(T):
            spans = ((0, 3), (3, Y), (Y + 3, 3))
            own_e, par_e, far_e = (const_parts(x, 0, t) for x in (own, par, far))
            own_m, par_m, far_m = (const_parts(x, 1, t) for x in (own, par, far))
            next_e, next_m = const_parts(far, 2, t), const_parts(far, 3, t)
            for n, (first, count) in enumerate(spans):
                for kind, v in (
                    (OWN, own_m[n]),
                    (PARTNER, par_m[n]),
                    (RECEIVED, far_m[n] * valid),
                    (NEAR, jnp.where(core == 0, own_e[n], par_e[n])),
                    (FAR, jnp.where(core == 0, far_e[n] * valid, own_e[n])),
                    (BEYOND, next_m[n] * valid),
                    (PAST, jnp.where(core == 0, next_e[n], far_e[n]) * valid),
                ):
                    to = (kind * T + t) * pad + first
                    st_ref[to : to + count, :] = v
        for one, other, moved, scaled in ((NEAR, FAR, OWN, SCALE), (FAR, PAST, RECEIVED, SCALE_FAR)):
            sums = []
            for t in range(T):
                near, rest = (one * T + t) * pad, (other * T + t) * pad
                sums.append(
                    (st_ref[near : near + R1, :] + st_ref[rest : rest + R1, :])
                    + (st_ref[near + 1 : near + 1 + R1, :] + st_ref[rest + 1 : rest + 1 + R1, :])
                )
            back = p.behind(sums, lane_rows)
            for t in range(T):
                around = sums[t] + back[t]
                at = (moved * T + t) * pad + 1
                mov = st_ref[at : at + R1, :]
                guarded = jnp.where(mov > 0, around, 1.0)
                to = (scaled * T + t) * pad + 1
                st_ref[to : to + R1, :] = mov / (CORNER * guarded) + (1.0 - mov)
        modes_z(
            p,
            lambda t, k, r: field_at(far, t, k, r),
            lambda t, r: static(p, st_ref, RECEIVED, t, r),
            R0,
            -sign,
            other_ref,
        )

        def emit(t, comp, r, v):
            force = v + part_ref[(comp * R1 + r) * T + t, 0:C, :]
            mov = p.wide(static(p, st_ref, OWN, t, r + 1))
            here = field_at(own, t, comp, r + 1)
            load = load_ref[t * (D * R1) + comp * R1 + r, 0:C, :]
            res = mov * (load - force) - (1.0 - mov) * here
            p.put(d_ref, t * N1, R1, comp, r, p.wide(static(p, st_ref, SCALE, t, r + 1)) * res)
            if 2 <= r < Y + 2:
                p.put(r_ref, t * N3, Y, comp, r - 2, res)

        layer(p, modes_ref, other_ref, True, lambda t, e: static(p, st_ref, FAR, t, e), R0, -sign, emit)

    res0, dir0, consts = call(
        far_start_body,
        [(T * N3, W), (T * N1, W), (9 * T * up8(R0), W)],
        [far_m, own_m, par_m, modes, part, loaded] + y_got + par_y + far_y,
        [field_shapes(R0)],
        flops=10**6,
    )

    def near_apply(own_ref, par_ref, st_ref, part_ref, modes_ref, other_ref, per, count, shift):
        _, sign = place()
        modes_z(p, lambda t, k, r: p.tile(own_ref, t * per, count, k, r), lambda t, r: static(p, st_ref, OWN, t, r + shift), count, sign, modes_ref)
        modes_z(p, lambda t, k, r: p.tile(par_ref, t * per, count, k, r), lambda t, r: static(p, st_ref, PARTNER, t, r + shift), count, sign, other_ref)

        def emit(t, comp, r, v):
            part_ref[(comp * (count - 2) + r) * T + t, 0:C, :] = v

        def more(t, comp, r, v):
            at = (comp * (count - 2) + r) * T + t
            part_ref[at, 0:C, :] = part_ref[at, 0:C, :] + v

        layer(p, modes_ref, other_ref, False, lambda t, e: static(p, st_ref, NEAR, t, e + shift), count, sign, emit)
        single(p, modes_ref, lambda t, e: static(p, st_ref, FAR, t, e + shift), count, -sign, -1, more)

    def far_apply(load, own_ref, st_ref, part_ref, other_ref, per, count, shift, emit):
        _, sign = place()
        modes_z(p, load, lambda t, r: static(p, st_ref, RECEIVED, t, r + shift), count, -sign, other_ref)

        def finish(t, comp, r, v):
            force = v + part_ref[(comp * (count - 2) + r) * T + t, 0:C, :]
            mov = p.wide(static(p, st_ref, OWN, t, r + 1 + shift))
            here = p.tile(own_ref, t * per, count, comp, r + 1)
            emit(t, comp, r, mov * force + (1.0 - mov) * here, here)

        single(p, other_ref, lambda t, e: static(p, st_ref, FAR, t, e + shift), count, -sign, 1, finish)

    far_d = planes_along(dir0)
    par_d = cores(dir0)
    next_d = planes_along(par_d)

    def near_one_body(own_ref, par_ref, st_ref, part_ref, modes_ref, other_ref):
        near_apply(own_ref, par_ref, st_ref, part_ref, modes_ref, other_ref, N1, R1, 1)

    part1, modes1 = call(
        near_one_body,
        [(D * R2 * T, 8, W), field_shapes(R1)],
        [dir0, par_d, consts],
        [field_shapes(R1)],
        flops=10**6,
    )

    def far_one_body(far_ref, own_ref, st_ref, part_ref, q_ref, w_ref, other_ref):
        if N2 > FL * R2:
            for t in range(T):
                w_ref[t * N2 + FL * R2 : (t + 1) * N2, :] = jnp.zeros((N2 - FL * R2, W), F32)

        def emit(t, comp, r, image, here):
            scale = p.wide(static(p, st_ref, SCALE, t, r + 2))
            p.put(w_ref, t * N2, R2, comp, r, scale * image - here)
            if 1 <= r < Y + 1:
                p.put(q_ref, t * N3, Y, comp, r - 1, image)

        load = lambda t, k, r: p.tile(far_ref, t * N1, R1, k, r)
        far_apply(load, own_ref, st_ref, part_ref, other_ref, N1, R1, 1, emit)

    image0, second, modes_far = call(
        far_one_body,
        [(T * N3, W), (T * N2, W), field_shapes(R1)],
        [far_d, dir0, consts, part1],
        flops=10**6,
    )
    par_w = cores(second)

    def across_body(far_ref, own_ref, st_ref, part_ref):
        _, sign = place()

        def emit(t, comp, r, v):
            part_ref[(comp * R2 + r) * T + t, 0:C, :] = v

        def more(t, comp, r, v):
            at = (comp * R2 + r) * T + t
            part_ref[at, 0:C, :] = part_ref[at, 0:C, :] + v

        layer(p, far_ref, own_ref, True, lambda t, e: static(p, st_ref, FAR, t, e + 1), R1, sign, emit)
        single(p, far_ref, lambda t, e: static(p, st_ref, PAST, t, e + 1), R1, -sign, -1, more, True)

    (part_far,) = call(across_body, [(D * R2 * T, 8, W)], [modes_far, modes1, consts], flops=10**6)

    def columns(number, sums, lane):
        table = jnp.zeros((C, W), F32)
        for j in range(C):
            column = jnp.sum(sums[j], axis=1, keepdims=True)
            table = jnp.where(lane == number * C + j, column, table)
        return table

    def gram_body(d_ref, q_ref, r_ref, w_ref, g_ref, mine_ref, send_ref):
        core = lax.axis_index("gz")
        lane = p.lanes()
        sums = [[jnp.zeros((C, W), F32) for _ in range(C)] for _ in range(3)]
        for t in range(T):
            for comp in range(D):
                for r in range(Y):
                    d = p.tile(d_ref, t * N1, R1, comp, r + 2)
                    w = p.tile(w_ref, t * N2, R2, comp, r + 1)
                    for j in range(C):
                        at = t * N3 + (j * D + comp) * Y + r
                        q = q_ref[at : at + 1, :]
                        sums[0][j] = sums[0][j] + d * q
                        sums[1][j] = sums[1][j] + d * r_ref[at : at + 1, :]
                        sums[2][j] = sums[2][j] + w * q
        table = columns(0, sums[0], lane) + columns(1, sums[1], lane) + columns(2, sums[2], lane)
        g_ref[...] = jnp.zeros((8, W), F32)
        g_ref[0:C, :] = table
        for out, t in ((mine_ref, core), (send_ref, 1 - core)):
            for number, src in enumerate((r_ref, q_ref)):
                out[number * N3 : (number + 1) * N3, :] = src[pl.ds(pl.multiple_of(t * N3, 8), N3), :]
            for comp in range(D):
                for r in range(Y):
                    p.put(out, 2 * N3, Y, comp, r, p.tile(d_ref, t * N1, R1, comp, r + 2))
                    p.put(out, 3 * N3, Y, comp, r, p.tile(w_ref, t * N2, R2, comp, r + 1))

    gram3, mine, send = call(gram_body, [(8, W), (4 * N3, W), (4 * N3, W)], [dir0, image0, res0, second], flops=10**6)

    def near_two_body(own_ref, par_ref, st_ref, part_ref, modes_ref, other_ref):
        near_apply(own_ref, par_ref, st_ref, part_ref, modes_ref, other_ref, N2, R2, 2)

    (part2,) = call(near_two_body, [(D * Y * T, 8, W)], [second, par_w, consts], [field_shapes(R2)] * 2, flops=10**6)
    kept = cores(send)

    def far_two_body(
        next_ref, far_ref, own_ref, st_ref, part_far_ref, part_ref, gram_ref,
        mine_ref, send_ref, next_modes_ref, w_ref, other_ref, u_ref,
    ):
        core, sign = place()
        modes_z(
            p,
            lambda t, k, r: p.tile(next_ref, t * N1, R1, k, r),
            lambda t, r: static(p, st_ref, BEYOND, t, r + 1),
            R1,
            -sign,
            next_modes_ref,
        )

        def found(t, comp, r, v):
            force = v + part_far_ref[(comp * R2 + r) * T + t, 0:C, :]
            mov = p.wide(static(p, st_ref, RECEIVED, t, r + 2))
            here = p.tile(far_ref, t * N1, R1, comp, r + 1)
            image = mov * force + (1.0 - mov) * here
            scale = p.wide(static(p, st_ref, SCALE_FAR, t, r + 2))
            w_ref[(comp * R2 + r) * T + t, 0:C, :] = scale * image - here

        single(p, next_modes_ref, lambda t, e: static(p, st_ref, PAST, t, e + 1), R1, -sign, 1, found)

        def emit(t, comp, r, image, here):
            p.put(u_ref, t * N3, Y, comp, r, image)
            sums_in.append((image, t, comp, r))

        sums_in = []
        load = lambda t, k, r: w_ref[(k * R2 + r) * T + t, 0:C, :]
        far_apply(load, own_ref, st_ref, part_ref, other_ref, N2, R2, 2, emit)
        sums = [jnp.zeros((C, W), F32) for _ in range(C)]
        for _, t, comp, r in sums_in:
            u = p.tile(u_ref, t * N3, Y, comp, r)
            for j in range(C):
                at = t * N2 + (j * D + comp) * R2 + r + 1
                sums[j] = sums[j] + u * own_ref[at : at + 1, :]
        table = gram_ref[0:C, :] + columns(3, sums, p.lanes())
        for out, t in ((mine_ref, core), (send_ref, 1 - core)):
            out[0:N3, :] = u_ref[pl.ds(pl.multiple_of(t * N3, 8), N3), :]
            out[N3 : N3 + 8, :] = jnp.zeros((8, W), F32)
            out[N3 : N3 + C, :] = table

    mine_u, send_u = call(
        far_two_body,
        [(N3 + 8, W), (N3 + 8, W)],
        [next_d, far_d, second, consts, part_far, part2, gram3],
        [field_shapes(R1), (D * R2 * T, 8, W), field_shapes(R2), (T * N3, W)],
        flops=10**6,
    )
    kept_u = cores(send_u)

    table = mine_u[N3 : N3 + 8, :] + kept_u[N3 : N3 + 8, :]

    def crossed(x, axis, size, step):
        pairs = [(i * T + k, (i ^ step) * T + 1 - k) for i in range(size) for k in range(T)]
        return lax.ppermute(x, (axis, "gz"), pairs)

    for axis, size in (("gy", p.ngy), ("gx", p.ngx)):
        if size & (size - 1):
            table = lax.psum(table, axis)
            continue
        step = 1
        while step < size:
            if step * 2 < size:
                one, two, three = (crossed(table, axis, size, step * k) for k in (1, 2, 3))
                table = (table + one) + (two + three)
                step *= 4
            else:
                table = table + crossed(table, axis, size, step)
                step *= 2

    def final_body(
        g_ref, x_ref, mine_ref, mine_u_ref, kept_ref, kept_u_ref, out_hbm, res_hbm, a_ref, out_ref, res_ref, sems
    ):
        core = lax.axis_index("gz")
        lane = lax.broadcasted_iota(jnp.int32, (1, W), 1)

        def splat(row, at):
            return jnp.broadcast_to(row[:, at : at + 1], (1, W))

        def factor(rows, first):
            a = {(i, j): splat(rows[i], first + j) for i in range(C) for j in range(i + 1)}
            low, inv = {}, []
            for k in range(C):
                inv.append(1.0 / a[k, k])
                for i in range(k + 1, C):
                    low[i, k] = a[i, k] * inv[k]
                for i in range(k + 1, C):
                    for j in range(k + 1, i + 1):
                        a[i, j] = a[i, j] - low[i, k] * a[j, k]
            return low, inv

        def solve(factors, right):
            low, inv = factors
            y = []
            for i in range(C):
                v = right[i]
                for k in range(i):
                    v = v - low[i, k] * y[k]
                y.append(v)
            x = [None] * C
            for i in reversed(range(C)):
                v = y[i] * inv[i]
                for k in range(i + 1, C):
                    v = v - low[k, i] * x[k]
                x[i] = v
            return x

        rows = [g_ref[i : i + 1, :] for i in range(C)]
        first = solve(factor(rows, 0), rows)
        reduced = []
        for i in range(C):
            v = jnp.where(
                lane < 2 * C, pltpu.roll(rows[i], C, 1) - rows[i], pltpu.roll(rows[i], W - C, 1)
            )
            for k in range(C):
                v = v - splat(rows[i], 2 * C + k) * first[k]
            reduced.append(v)
        on_second = solve(factor(reduced, 2 * C), reduced)
        for i in range(C):
            v = first[i]
            for k in range(C):
                v = v - splat(first[i], 2 * C + k) * on_second[k]
            for k in range(C):
                a_ref[i * C + k] = jnp.broadcast_to(v[:, C + k : C + k + 1], (Y, W))
                a_ref[C * C + i * C + k] = jnp.broadcast_to(on_second[i][:, C + k : C + k + 1], (Y, W))
        halves = ((mine_ref, mine_u_ref, core), (kept_ref, kept_u_ref, 1 - core))
        moves = []
        for number in range(2):
            target = (out_ref, res_ref)[number]
            for src, src_u, plane in halves:
                for comp in range(D):
                    fs = [(j * D + comp) * Y for j in range(C)]
                    at = N3 if number else 2 * N3
                    v = [src[at + f : at + f + Y, :] for f in fs]
                    u = [src_u[f : f + Y, :] if number else src[3 * N3 + f : 3 * N3 + f + Y, :] for f in fs]
                    for i in range(C):
                        at = pl.ds(pl.multiple_of(((i * D + comp) * Q + plane) * Y, 8), Y)
                        total = a_ref[i] * v[0] + a_ref[C * C + i] * u[0]
                        for j in range(1, C):
                            total = total + (a_ref[j * C + i] * v[j] + a_ref[C * C + j * C + i] * u[j])
                        if number:
                            target[at, :] = src[fs[i] : fs[i] + Y, :] - total
                        else:
                            target[at, :] = x_ref[at, :] + total
            moves.append(pltpu.make_async_copy(target, (out_hbm, res_hbm)[number], sems.at[number]))
            moves[-1].start()
        for move in moves:
            move.wait()

    out, res = call(
        final_body,
        [(n_raw, W)] * 2,
        [table, z_msg, mine, mine_u, kept, kept_u],
        [(2 * C * C, Y, W), (n_raw, W), (n_raw, W), pltpu.SemaphoreType.DMA((2,))],
        flops=10**5,
        far_out=True,
    )
    return out.reshape(start.shape), res.reshape(start.shape)


def solution(mesh):
    in_specs = (
        P(("grp", "gx"), "gy", "gz"),
        P(("grp", "gx"), "gy", "gz"),
        P("grp", None, "gx", "gy", "gz"),
        P("grp", None, "gx", "gy", "gz"),
        P("grp", None),
        P("grp", None, None),
    )
    out_specs = (P("grp", None, "gx", "gy", "gz"), P("grp", None, "gx", "gy", "gz"))

    def body(*args):
        return shards(dict(mesh.shape), *args)

    return jax.shard_map(body, mesh=mesh, in_specs=in_specs, out_specs=out_specs, check_vma=False)
```

```python
import jax
import jax.numpy as jnp
from jax import lax
from jax.experimental import pallas as pl
from jax.experimental.pallas import tpu as pltpu
from jax.sharding import PartitionSpec as P


LEVELS = 16

soft_modulus = 0.05
poisson_ratio = 0.3
lame = poisson_ratio / ((1.0 + poisson_ratio) * (1.0 - 2.0 * poisson_ratio))
shear = 1.0 / (2.0 * (1.0 + poisson_ratio))
THREE, TWO, ONE = 1.0 / 16.0, 1.0 / 48.0, 1.0 / 144.0
CORNER = THREE * (lame + 4.0 * shear) + 2.0 * TWO * (lame + 4.0 * shear) + ONE * (lame + 4.0 * shear)

VMEM, SMEM = pltpu.VMEM, pltpu.SMEM
F32 = jnp.float32


def up8(n):
    return -(-n // 8) * 8


def call(body, outs, ins, scratch=(), flops=0, smem=(), hbm=(), far_out=False):
    kinds = [SMEM if i in smem else pltpu.HBM if i in hbm else VMEM for i in range(len(ins))]
    ins = [x if k is SMEM else pltpu.with_memory_space_constraint(x, k) for x, k in zip(ins, kinds)]
    return pl.pallas_call(
        body,
        out_shape=[jax.ShapeDtypeStruct(s, F32) if far_out else VMEM(s, F32) for s in outs],
        in_specs=[pl.BlockSpec(memory_space=k) for k in kinds],
        out_specs=[pl.BlockSpec(memory_space=pl.ANY if far_out else VMEM)] * len(outs),
        scratch_shapes=[VMEM(s, F32) if isinstance(s, tuple) else s for s in scratch],
        compiler_params=pltpu.CompilerParams(vmem_limit_bytes=16 * 2**20),
        cost_estimate=pl.CostEstimate(flops=flops, bytes_accessed=0, transcendentals=0),
    )(*ins)


class Plan:
    def __init__(self, block, mesh):
        self.cases, self.comps, self.planes, self.rows, self.width = block
        self.fields = self.cases * self.comps
        self.ngx, self.ngy, self.tiles = mesh["gx"], mesh["gy"], mesh["gz"]
        if not (self.planes == self.tiles == 2 and self.rows % 8 == 0 and self.comps == 3):
            raise ValueError("block shape")
        self.depth = (self.tiles * self.width, self.ngy * self.rows)
        self.r0 = self.rows + 6
        self.main = up8((self.fields + 4) * self.rows)

    def per(self, count):
        return up8(self.fields * count)

    def tile(self, ref, base, count, comp, row):
        return ref[pl.ds(base + comp * count + row, self.cases, stride=self.comps * count), :]

    def put(self, ref, base, count, comp, row, value):
        ref[pl.ds(base + comp * count + row, self.cases, stride=self.comps * count), :] = value

    def raw(self, ref, base, comp, plane, row):
        start = base + (comp * self.planes + plane) * self.rows + row
        return ref[pl.ds(start, self.cases, stride=self.comps * self.planes * self.rows), :]

    def lanes(self, count=None):
        return lax.broadcasted_iota(jnp.int32, (count or self.cases, self.width), 1)

    def ahead(self, tiles, lane):
        moved = [pltpu.roll(v, self.width - 1, 1) for v in tiles]
        moved.append(jnp.zeros_like(tiles[0]))
        return [jnp.where(lane == self.width - 1, moved[t + 1], moved[t]) for t in range(self.tiles)]

    def behind(self, tiles, lane):
        moved = [pltpu.roll(v, 1, 1) for v in tiles]
        moved = [jnp.zeros_like(tiles[0])] + moved
        return [jnp.where(lane == 0, moved[t], moved[t + 1]) for t in range(self.tiles)]

    def wide(self, row):
        return jnp.broadcast_to(row, (self.cases, self.width))


def modes_z(p, load, mask, count, sign, out):
    lane = p.lanes()
    for r in range(count):
        m = [p.wide(mask(t, r)) for t in range(p.tiles)]
        ms = [x * sign for x in m]
        for comp in range(3):
            v = [load(t, comp, r) * (ms[t] if comp == 0 else m[t]) for t in range(p.tiles)]
            n = p.ahead(v, lane)
            for t in range(p.tiles):
                out[((comp * 2) * count + r) * p.tiles + t, 0 : p.cases, :] = v[t] + n[t]
                out[((comp * 2 + 1) * count + r) * p.tiles + t, 0 : p.cases, :] = n[t] - v[t]


CQ, CB, CS = THREE * lame, 2.0 * THREE * shear, THREE * shear
CD, CE, CF = TWO * (lame + 3.0 * shear), TWO * lame, TWO * shear
CG = ONE * (lame + 4.0 * shear)


def modes_y(p, ref, count, e, t, flip):
    found = [{}, {}, {}]
    for comp in range(3):
        for c in (0, 1):
            at = ((comp * 2 + c) * count + e) * p.tiles + t
            a = ref[at, 0 : p.cases, :]
            b = ref[at + p.tiles, 0 : p.cases, :]
            if flip and comp == 0:
                found[comp][0, c], found[comp][1, c] = -a - b, a - b
            else:
                found[comp][0, c], found[comp][1, c] = a + b, b - a
    return found


def between(total, change):
    (x, y, z), (dx, dy, dz) = total, change
    q = CQ * (dx[0, 0] + y[1, 0] + z[0, 1])
    sxy = CS * (dy[0, 0] + x[1, 0])
    sxz = CS * (dz[0, 0] + x[0, 1])
    syz = CS * (z[1, 0] + y[0, 1])
    s = x[1, 1] + dy[0, 1] + dz[1, 0]
    return {
        (0, 0, 0): -(q + CB * dx[0, 0]),
        (0, 1, 0): sxy - (CD * dx[1, 0] + CE * z[1, 1]),
        (0, 0, 1): sxz - (CD * dx[0, 1] + CE * y[1, 1]),
        (0, 1, 1): CF * (s + x[1, 1]) - CG * dx[1, 1],
        (1, 0, 0): -sxy,
        (1, 1, 0): (q + CB * y[1, 0]) - (CD * dy[1, 0] + CE * dz[0, 1]),
        (1, 0, 1): syz - CF * (s + dy[0, 1]),
        (1, 1, 1): (CD * y[1, 1] + CE * dx[0, 1]) - CG * dy[1, 1],
        (2, 0, 0): -sxz,
        (2, 0, 1): (q + CB * z[0, 1]) - (CD * dz[0, 1] + CE * dy[1, 0]),
        (2, 1, 0): syz - CF * (s + dz[1, 0]),
        (2, 1, 1): (CD * z[1, 1] + CE * dx[1, 0]) - CG * dz[1, 1],
    }


def share(m, way):
    x, y, z = m
    q = CQ * (x[0, 0] + y[1, 0] + z[0, 1])
    sxy = CS * (y[0, 0] + x[1, 0])
    sxz = CS * (z[0, 0] + x[0, 1])
    pair = z[1, 0] + y[0, 1]
    syz = CS * pair
    s = x[1, 1] + pair
    found = {
        (0, 0, 0): -(q + CB * x[0, 0]),
        (1, 1, 1): (CD - way * CG) * y[1, 1] + CE * x[0, 1],
        (2, 1, 1): (CD - way * CG) * z[1, 1] + CE * x[1, 0],
        (0, 1, 1): (way * 2.0 * CF - CG) * x[1, 1] + (way * CF) * pair,
    }
    low, high = CD * x[1, 0] + CE * z[1, 1], CD * x[0, 1] + CE * y[1, 1]
    if way > 0:
        found[0, 1, 0], found[0, 0, 1] = sxy - low, sxz - high
        found[1, 0, 0], found[2, 0, 0] = -sxy, -sxz
        found[1, 1, 0] = q + ((CB - CD) * y[1, 0] - CE * z[0, 1])
        found[2, 0, 1] = q + ((CB - CD) * z[0, 1] - CE * y[1, 0])
        found[1, 0, 1] = syz - CF * (s + y[0, 1])
        found[2, 1, 0] = syz - CF * (s + z[1, 0])
    else:
        found[0, 1, 0], found[0, 0, 1] = -sxy - low, -sxz - high
        found[1, 0, 0], found[2, 0, 0] = sxy, sxz
        found[1, 1, 0] = q + ((CB + CD) * y[1, 0] + CE * z[0, 1])
        found[2, 0, 1] = q + ((CB + CD) * z[0, 1] + CE * y[1, 0])
        found[1, 0, 1] = syz + CF * (s + y[0, 1])
        found[2, 1, 0] = syz + CF * (s + z[1, 0])
    return found


def spread(p, forces, count, sign, emit):
    lane = p.lanes()
    carry = {}
    for e in range(count - 1):
        done = {}
        for t in range(p.tiles):
            h = forces(e, t)
            for comp in range(3):
                for c in (0, 1):
                    if e:
                        done[comp, c, t] = carry[comp, c, t] + (h[comp, 0, c] - h[comp, 1, c])
                    carry[comp, c, t] = h[comp, 0, c] + h[comp, 1, c]
        if e:
            for comp in range(3):
                low = [done[comp, 0, t] - done[comp, 1, t] for t in range(p.tiles)]
                high = [done[comp, 0, t] + done[comp, 1, t] for t in range(p.tiles)]
                back = p.behind(high, lane)
                for t in range(p.tiles):
                    total = low[t] + back[t]
                    emit(t, comp, e - 1, total * sign if comp == 0 else total)


def layer(p, own, other, flip, modulus, count, sign, emit, outer=None):
    def forces(e, t):
        near, far = modes_y(p, own, count, e, t, flip), modes_y(p, other, count, e, t, False)
        total = [{k: far[c][k] + v for k, v in near[c].items()} for c in range(3)]
        change = [{k: far[c][k] - v for k, v in near[c].items()} for c in range(3)]
        mod = p.wide(modulus(t, e))
        h = {k: mod * v for k, v in between(total, change).items()}
        if outer is not None:
            rest = p.wide(outer(t, e))
            for k, v in share(near, -1).items():
                h[k] = h[k] - rest * v if k[0] == 0 else h[k] + rest * v
        return h

    spread(p, forces, count, sign, emit)


def single(p, ref, modulus, count, sign, emit):
    def forces(e, t):
        mod = p.wide(modulus(t, e))
        return {k: mod * v for k, v in share(modes_y(p, ref, count, e, t, False), 1).items()}

    spread(p, forces, count, sign, emit)


OWN, PARTNER, RECEIVED, NEAR, FAR, SCALE, BEYOND, PAST, SCALE_FAR = range(9)


def static(p, ref, kind, t, row):
    at = (kind * p.tiles + t) * up8(p.r0) + row
    return ref[at : at + 1, :]


def place():
    core = lax.axis_index("gz")
    return core, 1.0 - 2.0 * core.astype(F32)


def shards(mesh, design, supports, body_load, start, load_nodes, load_values):
    p = Plan(body_load.shape, mesh)
    C, D, Y, W, T, FL = p.cases, p.comps, p.rows, p.width, p.tiles, p.fields
    Q = p.planes
    n_raw = FL * Q * Y
    z_load = n_raw
    z_stat = z_load + FL * Y
    z_rows = z_stat + 2 * Q * Y
    y_stat = FL * 3
    y_load = y_stat + 6
    y_part = up8(y_load + FL * 2)
    d_part = up8(y_stat + 12)
    R0, R1, R2 = Y + 6, Y + 4, Y + 2
    N1, N2, N3 = p.per(R1), p.per(R2), p.per(Y)
    M = p.main
    both = p.ngy == 2

    x0 = start.reshape(n_raw, W)
    bl = body_load.reshape(n_raw, W)
    de = design.reshape(Q * Y, W)
    su = supports.reshape(Q * Y, W)

    def gather_body(x_hbm, b_hbm, d_hbm, s_hbm, z_ref, b_ref, *refs):
        d_ref, s_ref, sems = refs
        core = lax.axis_index("gz")
        moves = [
            pltpu.make_async_copy(src, dst, sems.at[i])
            for i, (src, dst) in enumerate(
                ((x_hbm, z_ref.at[pl.ds(0, n_raw)]), (b_hbm, b_ref), (d_hbm, d_ref), (s_hbm, s_ref))
            )
        ]
        for move in moves:
            move.start()
        moves[2].wait()
        density = (d_ref[...].astype(F32) + 1.0) / LEVELS
        z_ref[z_stat : z_stat + Q * Y, :] = (
            soft_modulus + (1.0 - soft_modulus) * density * density * density
        )
        moves[3].wait()
        z_ref[z_stat + Q * Y : z_rows, :] = 1.0 - s_ref[...].astype(F32)
        moves[1].wait()
        for f in range(FL):
            z_ref[z_load + f * Y : z_load + (f + 1) * Y, :] = b_ref[
                pl.ds(pl.multiple_of((f * Q + 1 - core) * Y, 8), Y), :
            ]
        moves[0].wait()

    z_msg, b_near = call(
        gather_body,
        [(z_rows, W), (n_raw, W)],
        [x0, bl, de, su],
        [VMEM((Q * Y, W), jnp.int32), VMEM((Q * Y, W), jnp.int32), pltpu.SemaphoreType.DMA((4,))],
        flops=10**5,
        hbm=(0, 1, 2, 3),
    )

    def cores(x):
        return lax.ppermute(x, "gz", [(i, 1 - i) for i in range(T)])

    def rows_along(x, step):
        return lax.ppermute(x, "gy", [(i, (i + step) % p.ngy) for i in range(p.ngy)])

    def planes_along(x, step=0):
        pairs = []
        for i in range(p.ngx):
            for j in range(p.ngy):
                for k in range(T):
                    to = i + 2 * k - 1
                    mine = (i * p.ngy + j) * T + k
                    row = (j + step) % p.ngy
                    if 0 <= to < p.ngx:
                        pairs.append((mine, (to * p.ngy + row) * T + 1 - k))
                    elif step:
                        pairs.append((mine, (i * p.ngy + row) * T + k))
                    elif p.ngy % 2 == 0:
                        pairs.append((mine, (i * p.ngy + (j ^ 1)) * T + k))
                    else:
                        pairs.append((mine, mine))
        return lax.ppermute(x, ("gx", "gy", "gz"), pairs)

    z_got = cores(z_msg)

    def main_body(s_ref, z_ref, b_ref, own_ref, par_ref, *y_refs):
        core = lax.axis_index("gz")
        if both:
            first = lax.axis_index("gy") == 0
            froms = [(jnp.where(first, Y - 3, 0), jnp.where(first, Y - 2, 0))]
        else:
            froms = [(Y - 3, Y - 2), (0, 0)]
        count = len(froms)
        for y_ref, d_ref, (three, two) in zip(y_refs[:count], y_refs[count:], froms):
            for src, half in ((s_ref, core), (z_ref, 1 - core)):
                at, to = half * y_part, half * d_part
                for comp in range(D):
                    for r in range(3):
                        v = p.raw(src, 0, comp, core, three + r)
                        p.put(y_ref, at, 3, comp, r, v)
                        p.put(d_ref, to, 3, comp, r, v)
                    for r in range(2):
                        if src is s_ref:
                            v = p.raw(b_ref, 0, comp, core, two + r)
                        else:
                            v = p.tile(src, z_load, Y, comp, two + r)
                        p.put(y_ref, at + y_load, 2, comp, r, v)
                for kind in range(2):
                    for r in range(3):
                        v = src[pl.ds(z_stat + (kind * Q + core) * Y + three + r, 1), :]
                        y_ref[pl.ds(at + y_stat + kind * 3 + r, 1), :] = v
                        d_ref[pl.ds(to + y_stat + kind * 3 + r, 1), :] = v
                        d_ref[pl.ds(to + y_stat + 6 + kind * 3 + r, 1), :] = src[
                            pl.ds(z_stat + (kind * Q + 1 - core) * Y + three + r, 1), :
                        ]
            for t in range(T):
                for ref, part, used in ((y_ref, y_part, y_load + FL * 2), (d_ref, d_part, y_stat + 12)):
                    if part > used:
                        ref[t * part + used : (t + 1) * part, :] = jnp.zeros((part - used, W), F32)
        for out, plane in ((own_ref, core), (par_ref, 1 - core)):
            for src, half in ((s_ref, core), (z_ref, 1 - core)):
                base = half * M
                for comp in range(D):
                    for r in range(Y):
                        p.put(out, base, Y, comp, r, p.raw(src, 0, comp, plane, r))
                for kind in range(4):
                    of = plane if kind < 2 else 1 - plane
                    out[pl.ds(pl.multiple_of(base + (FL + kind) * Y, 8), Y), :] = src[
                        pl.ds(pl.multiple_of(z_stat + (kind % 2 * Q + of) * Y, 8), Y), :
                    ]

    ways = (1,) if both else (1, -1)
    halos = len(ways)
    own_m, par_m, *sent = call(
        main_body,
        [(T * M, W)] * 2 + [(T * y_part, W)] * halos + [(T * d_part, W)] * halos,
        [z_msg, z_got, b_near],
        flops=10**5,
    )
    y_got = [rows_along(x, step) for x, step in zip(sent, ways)]
    far_m = planes_along(own_m)
    far_y = [planes_along(x, step) for x, step in zip(sent[halos:], ways)]
    par_y = [cores(x) for x in y_got]

    def halo(main, refs, part):
        row = lax.axis_index("gy")
        below = jnp.where(row > 0, 1.0, 0.0)
        above = jnp.where(row < p.ngy - 1, 1.0, 0.0)
        return main, refs[0], refs[-1], part, below, above

    def field_at(refs, t, comp, r):
        main, low, high, part, _, _ = refs
        if 3 <= r < Y + 3:
            return p.tile(main, t * M, Y, comp, r - 3)
        if r < 3:
            return p.tile(low, t * part, 3, comp, r)
        return p.tile(high, t * part, 3, comp, r - Y - 3)

    def const_at(refs, kind, t, r):
        main, low, high, part, below, above = refs
        if 3 <= r < Y + 3:
            at = t * M + (FL + kind) * Y + r - 3
            return main[at : at + 1, :]
        at = t * part + y_stat + kind * 3
        if r < 3:
            return low[at + r : at + r + 1, :] * below
        at += r - Y - 3
        return high[at : at + 1, :] * above

    def const_parts(refs, kind, t):
        main, low, high, part, below, above = refs
        at = t * part + y_stat + kind * 3
        to = t * M + (FL + kind) * Y
        return low[at : at + 3, :] * below, main[to : to + Y, :], high[at : at + 3, :] * above

    def points_body(node_ref, value_ref, out):
        core = lax.axis_index("gz")
        deep, across = p.depth
        base = ((lax.axis_index("gx") * Q + core) * across + lax.axis_index("gy") * Y - 2) * deep
        spots = jnp.concatenate([node_ref[c : c + 1, :] for c in range(C)], axis=1) - base
        total = C * n_loads
        if W & (W - 1):
            row = spots // W
            lane = spots - row * W
        else:
            row, lane = spots >> (W.bit_length() - 1), spots & (W - 1)
        hot = jnp.where(lax.broadcasted_iota(jnp.int32, (W, total), 0) == lane, 1.0, 0.0)
        rows8 = jnp.broadcast_to(row, (8, total))
        mine = lax.broadcasted_iota(jnp.int32, (8, total), 0)
        column = lax.broadcasted_iota(jnp.int32, (8, total), 1)
        mine = (column >= mine * n_loads) & (column < (mine + 1) * n_loads)
        values = []
        for comp in range(D):
            v = jnp.concatenate([value_ref[c, comp : comp + 1, :] for c in range(C)], axis=1)
            values.append(jnp.where(mine, jnp.broadcast_to(v, (8, total)), 0.0))
        left = [
            jnp.where(rows8 == r * T + t, values[comp], 0.0)
            for t in range(T)
            for comp in range(D)
            for r in range(R1)
        ]
        out[...] = lax.dot_general(
            jnp.concatenate(left, axis=0),
            hot,
            (((1,), (1,)), ((), ())),
            precision=lax.Precision.HIGHEST,
            preferred_element_type=F32,
        )

    n_loads = load_nodes.shape[1]
    (points,) = call(
        points_body,
        [(T * D * R1 * 8, W)],
        [load_nodes, jnp.swapaxes(load_values, 1, 2)],
        flops=10**6,
    )

    def loads_body(p_ref, b_ref, z_ref, *refs):
        ys, out = refs[:halos], refs[halos]
        core = lax.axis_index("gz")
        for half in range(2):
            t = core if half == 0 else 1 - core
            for comp in range(D):
                for r in range(R1):
                    if r < 2:
                        v = p.tile(ys[0], t * y_part + y_load, 2, comp, r)
                    elif r < Y + 2:
                        if half == 0:
                            v = p.raw(b_ref, 0, comp, core, r - 2)
                        else:
                            v = p.tile(z_ref, z_load, Y, comp, r - 2)
                    else:
                        v = p.tile(ys[-1], t * y_part + y_load, 2, comp, r - Y - 2)
                    at = t * (D * R1) + comp * R1 + r
                    out[at, 0:C, :] = v + p_ref[pl.ds(pl.multiple_of(at * 8, 8), C), :]

    (loaded,) = call(
        loads_body,
        [(T * D * R1, 8, W)],
        [points, b_near, z_got] + y_got,
        flops=10**6,
    )

    def near_start_body(own_m_ref, par_m_ref, *refs):
        modes_ref, part_ref, other_ref = refs[2 * halos :]
        core, sign = place()
        own, par = halo(own_m_ref, refs[:halos], y_part), halo(par_m_ref, refs[halos : 2 * halos], y_part)
        for refs, out in ((own, modes_ref), (par, other_ref)):
            modes_z(
                p,
                lambda t, k, r, refs=refs: field_at(refs, t, k, r),
                lambda t, r, refs=refs: const_at(refs, 1, t, r),
                R0,
                sign,
                out,
            )

        def modulus(t, e):
            return jnp.where(core == 0, const_at(own, 0, t, e), const_at(par, 0, t, e))

        def emit(t, comp, r, v):
            part_ref[(comp * R1 + r) * T + t, 0:C, :] = v

        layer(p, modes_ref, other_ref, False, modulus, R0, sign, emit)

    def field_shapes(count):
        return (6 * count * T, 8, W)

    modes, part = call(
        near_start_body,
        [field_shapes(R0), (D * R1 * T, 8, W)],
        [own_m, par_m] + y_got + par_y,
        [field_shapes(R0)],
        flops=10**6,
    )

    def far_start_body(far_m_ref, own_m_ref, par_m_ref, modes_ref, part_ref, load_ref, *refs):
        r_ref, d_ref, st_ref, other_ref = refs[3 * halos :]
        core, sign = place()
        own, par = halo(own_m_ref, refs[:halos], y_part), halo(par_m_ref, refs[halos : 2 * halos], y_part)
        far = halo(far_m_ref, refs[2 * halos : 3 * halos], d_part)
        column = lax.axis_index("gx")
        inside = jnp.where(core == 0, column > 0, column < p.ngx - 1)
        valid = jnp.where(inside, 1.0, 0.0)
        lane_rows = lax.broadcasted_iota(jnp.int32, (R1, W), 1)
        pad = up8(R0)
        for t in range(T):
            spans = ((0, 3), (3, Y), (Y + 3, 3))
            own_e, par_e, far_e = (const_parts(x, 0, t) for x in (own, par, far))
            own_m, par_m, far_m = (const_parts(x, 1, t) for x in (own, par, far))
            next_e, next_m = const_parts(far, 2, t), const_parts(far, 3, t)
            for n, (first, count) in enumerate(spans):
                for kind, v in (
                    (OWN, own_m[n]),
                    (PARTNER, par_m[n]),
                    (RECEIVED, far_m[n] * valid),
                    (NEAR, jnp.where(core == 0, own_e[n], par_e[n])),
                    (FAR, jnp.where(core == 0, far_e[n] * valid, own_e[n])),
                    (BEYOND, next_m[n] * valid),
                    (PAST, jnp.where(core == 0, next_e[n], far_e[n]) * valid),
                ):
                    to = (kind * T + t) * pad + first
                    st_ref[to : to + count, :] = v
        for one, other, moved, scaled in ((NEAR, FAR, OWN, SCALE), (FAR, PAST, RECEIVED, SCALE_FAR)):
            sums = []
            for t in range(T):
                near, rest = (one * T + t) * pad, (other * T + t) * pad
                sums.append(
                    (st_ref[near : near + R1, :] + st_ref[rest : rest + R1, :])
                    + (st_ref[near + 1 : near + 1 + R1, :] + st_ref[rest + 1 : rest + 1 + R1, :])
                )
            back = p.behind(sums, lane_rows)
            for t in range(T):
                around = sums[t] + back[t]
                at = (moved * T + t) * pad + 1
                mov = st_ref[at : at + R1, :]
                guarded = jnp.where(mov > 0, around, 1.0)
                to = (scaled * T + t) * pad + 1
                st_ref[to : to + R1, :] = mov / (CORNER * guarded) + (1.0 - mov)
        modes_z(
            p,
            lambda t, k, r: field_at(far, t, k, r),
            lambda t, r: static(p, st_ref, RECEIVED, t, r),
            R0,
            -sign,
            other_ref,
        )

        def emit(t, comp, r, v):
            force = v + part_ref[(comp * R1 + r) * T + t, 0:C, :]
            mov = p.wide(static(p, st_ref, OWN, t, r + 1))
            here = field_at(own, t, comp, r + 1)
            load = load_ref[t * (D * R1) + comp * R1 + r, 0:C, :]
            res = mov * (load - force) - (1.0 - mov) * here
            p.put(d_ref, t * N1, R1, comp, r, p.wide(static(p, st_ref, SCALE, t, r + 1)) * res)
            if 2 <= r < Y + 2:
                p.put(r_ref, t * N3, Y, comp, r - 2, res)

        layer(p, modes_ref, other_ref, True, lambda t, e: static(p, st_ref, FAR, t, e), R0, -sign, emit)

    res0, dir0, consts = call(
        far_start_body,
        [(T * N3, W), (T * N1, W), (9 * T * up8(R0), W)],
        [far_m, own_m, par_m, modes, part, loaded] + y_got + par_y + far_y,
        [field_shapes(R0)],
        flops=10**6,
    )

    def near_apply(own_ref, par_ref, st_ref, part_ref, modes_ref, other_ref, per, count, shift):
        _, sign = place()
        modes_z(p, lambda t, k, r: p.tile(own_ref, t * per, count, k, r), lambda t, r: static(p, st_ref, OWN, t, r + shift), count, sign, modes_ref)
        modes_z(p, lambda t, k, r: p.tile(par_ref, t * per, count, k, r), lambda t, r: static(p, st_ref, PARTNER, t, r + shift), count, sign, other_ref)

        def emit(t, comp, r, v):
            part_ref[(comp * (count - 2) + r) * T + t, 0:C, :] = v

        near, far = (lambda t, e, kind=kind: static(p, st_ref, kind, t, e + shift) for kind in (NEAR, FAR))
        layer(p, modes_ref, other_ref, False, near, count, sign, emit, far)

    def far_apply(load, own_ref, st_ref, part_ref, other_ref, per, count, shift, emit):
        _, sign = place()
        modes_z(p, load, lambda t, r: static(p, st_ref, RECEIVED, t, r + shift), count, -sign, other_ref)

        def finish(t, comp, r, v):
            force = v + part_ref[(comp * (count - 2) + r) * T + t, 0:C, :]
            mov = p.wide(static(p, st_ref, OWN, t, r + 1 + shift))
            here = p.tile(own_ref, t * per, count, comp, r + 1)
            emit(t, comp, r, mov * force + (1.0 - mov) * here, here)

        single(p, other_ref, lambda t, e: static(p, st_ref, FAR, t, e + shift), count, -sign, finish)

    far_d = planes_along(dir0)
    par_d = cores(dir0)
    next_d = planes_along(par_d)

    def near_one_body(own_ref, par_ref, st_ref, part_ref, modes_ref, other_ref):
        near_apply(own_ref, par_ref, st_ref, part_ref, modes_ref, other_ref, N1, R1, 1)

    part1, modes1 = call(
        near_one_body,
        [(D * R2 * T, 8, W), field_shapes(R1)],
        [dir0, par_d, consts],
        [field_shapes(R1)],
        flops=10**6,
    )

    def far_one_body(far_ref, own_ref, st_ref, part_ref, q_ref, w_ref, other_ref):
        if N2 > FL * R2:
            for t in range(T):
                w_ref[t * N2 + FL * R2 : (t + 1) * N2, :] = jnp.zeros((N2 - FL * R2, W), F32)

        def emit(t, comp, r, image, here):
            scale = p.wide(static(p, st_ref, SCALE, t, r + 2))
            p.put(w_ref, t * N2, R2, comp, r, scale * image - here)
            if 1 <= r < Y + 1:
                p.put(q_ref, t * N3, Y, comp, r - 1, image)

        load = lambda t, k, r: p.tile(far_ref, t * N1, R1, k, r)
        far_apply(load, own_ref, st_ref, part_ref, other_ref, N1, R1, 1, emit)

    image0, second, modes_far = call(
        far_one_body,
        [(T * N3, W), (T * N2, W), field_shapes(R1)],
        [far_d, dir0, consts, part1],
        flops=10**6,
    )
    par_w = cores(second)

    def across_body(far_ref, own_ref, st_ref, part_ref):
        _, sign = place()

        def emit(t, comp, r, v):
            part_ref[(comp * R2 + r) * T + t, 0:C, :] = v

        far, past = (lambda t, e, kind=kind: static(p, st_ref, kind, t, e + 1) for kind in (FAR, PAST))
        layer(p, far_ref, own_ref, True, far, R1, sign, emit, past)

    (part_far,) = call(across_body, [(D * R2 * T, 8, W)], [modes_far, modes1, consts], flops=10**6)

    def columns(number, sums, lane):
        table = jnp.zeros((C, W), F32)
        for j in range(C):
            column = jnp.sum(sums[j], axis=1, keepdims=True)
            table = jnp.where(lane == number * C + j, column, table)
        return table

    def gram_body(d_ref, q_ref, r_ref, w_ref, g_ref):
        lane = p.lanes()
        sums = [[jnp.zeros((C, W), F32) for _ in range(C)] for _ in range(3)]
        for t in range(T):
            for comp in range(D):
                for r in range(Y):
                    d = p.tile(d_ref, t * N1, R1, comp, r + 2)
                    w = p.tile(w_ref, t * N2, R2, comp, r + 1)
                    for j in range(C):
                        at = t * N3 + (j * D + comp) * Y + r
                        q = q_ref[at : at + 1, :]
                        sums[0][j] = sums[0][j] + d * q
                        sums[1][j] = sums[1][j] + d * r_ref[at : at + 1, :]
                        sums[2][j] = sums[2][j] + w * q
        table = columns(0, sums[0], lane) + columns(1, sums[1], lane) + columns(2, sums[2], lane)
        g_ref[...] = jnp.zeros((8, W), F32)
        g_ref[0:C, :] = table

    (gram3,) = call(gram_body, [(8, W)], [dir0, image0, res0, second], flops=10**6)

    def near_two_body(own_ref, par_ref, st_ref, part_ref, modes_ref, other_ref):
        near_apply(own_ref, par_ref, st_ref, part_ref, modes_ref, other_ref, N2, R2, 2)

    (part2,) = call(near_two_body, [(D * Y * T, 8, W)], [second, par_w, consts], [field_shapes(R2)] * 2, flops=10**6)

    def far_two_body(
        next_ref, far_ref, own_ref, st_ref, part_far_ref, part_ref, gram_ref,
        g_ref, u_ref, next_modes_ref, w_ref, other_ref,
    ):
        _, sign = place()
        modes_z(
            p,
            lambda t, k, r: p.tile(next_ref, t * N1, R1, k, r),
            lambda t, r: static(p, st_ref, BEYOND, t, r + 1),
            R1,
            -sign,
            next_modes_ref,
        )

        def found(t, comp, r, v):
            force = v + part_far_ref[(comp * R2 + r) * T + t, 0:C, :]
            mov = p.wide(static(p, st_ref, RECEIVED, t, r + 2))
            here = p.tile(far_ref, t * N1, R1, comp, r + 1)
            image = mov * force + (1.0 - mov) * here
            scale = p.wide(static(p, st_ref, SCALE_FAR, t, r + 2))
            w_ref[(comp * R2 + r) * T + t, 0:C, :] = scale * image - here

        single(p, next_modes_ref, lambda t, e: static(p, st_ref, PAST, t, e + 1), R1, -sign, found)

        def emit(t, comp, r, image, here):
            p.put(u_ref, t * N3, Y, comp, r, image)
            sums_in.append((image, t, comp, r))

        sums_in = []
        load = lambda t, k, r: w_ref[(k * R2 + r) * T + t, 0:C, :]
        far_apply(load, own_ref, st_ref, part_ref, other_ref, N2, R2, 2, emit)
        sums = [jnp.zeros((C, W), F32) for _ in range(C)]
        for _, t, comp, r in sums_in:
            u = p.tile(u_ref, t * N3, Y, comp, r)
            for j in range(C):
                at = t * N2 + (j * D + comp) * R2 + r + 1
                sums[j] = sums[j] + u * own_ref[at : at + 1, :]
        g_ref[...] = jnp.zeros((8, W), F32)
        g_ref[0:C, :] = gram_ref[0:C, :] + columns(3, sums, p.lanes())

    table, image2 = call(
        far_two_body,
        [(8, W), (T * N3, W)],
        [next_d, far_d, second, consts, part_far, part2, gram3],
        [field_shapes(R1), (D * R2 * T, 8, W), field_shapes(R2)],
        flops=10**6,
    )

    def pack_body(r_ref, q_ref, d_ref, w_ref, u_ref, mine_ref, send_ref):
        core = lax.axis_index("gz")
        for out, t in ((mine_ref, core), (send_ref, 1 - core)):
            for number, src in enumerate((r_ref, q_ref)):
                out[number * N3 : (number + 1) * N3, :] = src[pl.ds(pl.multiple_of(t * N3, 8), N3), :]
            out[4 * N3 : 5 * N3, :] = u_ref[pl.ds(pl.multiple_of(t * N3, 8), N3), :]
            for comp in range(D):
                for r in range(Y):
                    p.put(out, 2 * N3, Y, comp, r, p.tile(d_ref, t * N1, R1, comp, r + 2))
                    p.put(out, 3 * N3, Y, comp, r, p.tile(w_ref, t * N2, R2, comp, r + 1))

    mine, send = call(
        pack_body, [(5 * N3, W)] * 2, [res0, image0, dir0, second, image2], flops=10**6
    )
    kept = cores(send)

    table = table + cores(table)

    def crossed(x, axis, size, step):
        pairs = [(i * T + k, (i ^ step) * T + 1 - k) for i in range(size) for k in range(T)]
        return lax.ppermute(x, (axis, "gz"), pairs)

    for axis, size in (("gy", p.ngy), ("gx", p.ngx)):
        if size & (size - 1):
            table = lax.psum(table, axis)
            continue
        step = 1
        while step < size:
            if step * 2 < size:
                one, two, three = (crossed(table, axis, size, step * k) for k in (1, 2, 3))
                table = (table + one) + (two + three)
                step *= 4
            else:
                table = table + crossed(table, axis, size, step)
                step *= 2

    def final_body(
        g_ref, x_ref, mine_ref, kept_ref, out_hbm, res_hbm, a_ref, out_ref, res_ref, sems
    ):
        core = lax.axis_index("gz")
        lane = lax.broadcasted_iota(jnp.int32, (1, W), 1)

        def splat(row, at):
            return jnp.broadcast_to(row[:, at : at + 1], (1, W))

        def factor(rows, first):
            a = {(i, j): splat(rows[i], first + j) for i in range(C) for j in range(i + 1)}
            low, inv = {}, []
            for k in range(C):
                inv.append(1.0 / a[k, k])
                for i in range(k + 1, C):
                    low[i, k] = a[i, k] * inv[k]
                for i in range(k + 1, C):
                    for j in range(k + 1, i + 1):
                        a[i, j] = a[i, j] - low[i, k] * a[j, k]
            return low, inv

        def solve(factors, right):
            low, inv = factors
            y = []
            for i in range(C):
                v = right[i]
                for k in range(i):
                    v = v - low[i, k] * y[k]
                y.append(v)
            x = [None] * C
            for i in reversed(range(C)):
                v = y[i] * inv[i]
                for k in range(i + 1, C):
                    v = v - low[k, i] * x[k]
                x[i] = v
            return x

        rows = [g_ref[i : i + 1, :] for i in range(C)]
        first = solve(factor(rows, 0), rows)
        reduced = []
        for i in range(C):
            v = jnp.where(
                lane < 2 * C, pltpu.roll(rows[i], C, 1) - rows[i], pltpu.roll(rows[i], W - C, 1)
            )
            for k in range(C):
                v = v - splat(rows[i], 2 * C + k) * first[k]
            reduced.append(v)
        on_second = solve(factor(reduced, 2 * C), reduced)
        for i in range(C):
            v = first[i]
            for k in range(C):
                v = v - splat(first[i], 2 * C + k) * on_second[k]
            for k in range(C):
                a_ref[i * C + k] = jnp.broadcast_to(v[:, C + k : C + k + 1], (Y, W))
                a_ref[C * C + i * C + k] = jnp.broadcast_to(on_second[i][:, C + k : C + k + 1], (Y, W))
        moves = []
        span = D * Q * Y
        for number in range(2):
            target, to = ((out_ref, out_hbm), (res_ref, res_hbm))[number]
            for i in range(C):
                a = [a_ref[j * C + i] for j in range(C)]
                b = [a_ref[C * C + j * C + i] for j in range(C)]
                for src, plane in ((mine_ref, core), (kept_ref, 1 - core)):
                    for comp in range(D):
                        at = [(j * D + comp) * Y for j in range(C)]
                        one, two = (1, 4) if number else (2, 3)
                        terms = [
                            a[j] * src[one * N3 + at[j] : one * N3 + at[j] + Y, :]
                            + b[j] * src[two * N3 + at[j] : two * N3 + at[j] + Y, :]
                            for j in range(C)
                        ]
                        total = sum(terms[1:], terms[0])
                        rows = pl.ds(pl.multiple_of(((i * D + comp) * Q + plane) * Y, 8), Y)
                        if number:
                            target[rows, :] = src[at[i] : at[i] + Y, :] - total
                        else:
                            target[rows, :] = x_ref[rows, :] + total
                rows = pl.ds(i * span, span)
                moves.append(pltpu.make_async_copy(target.at[rows], to.at[rows], sems.at[number * C + i]))
                moves[-1].start()
        for move in moves:
            move.wait()

    out, res = call(
        final_body,
        [(n_raw, W)] * 2,
        [table, z_msg, mine, kept],
        [(2 * C * C, Y, W), (n_raw, W), (n_raw, W), pltpu.SemaphoreType.DMA((2 * C,))],
        flops=10**5,
        far_out=True,
    )
    return out.reshape(start.shape), res.reshape(start.shape)


def solution(mesh):
    in_specs = (
        P(("grp", "gx"), "gy", "gz"),
        P(("grp", "gx"), "gy", "gz"),
        P("grp", None, "gx", "gy", "gz"),
        P("grp", None, "gx", "gy", "gz"),
        P("grp", None),
        P("grp", None, None),
    )
    out_specs = (P("grp", None, "gx", "gy", "gz"), P("grp", None, "gx", "gy", "gz"))

    def body(*args):
        return shards(dict(mesh.shape), *args)

    return jax.shard_map(body, mesh=mesh, in_specs=in_specs, out_specs=out_specs, check_vma=False)
```

```python
import jax
import jax.numpy as jnp
from jax import lax
from jax.experimental import pallas as pl
from jax.experimental.pallas import tpu as pltpu
from jax.sharding import PartitionSpec as P


LEVELS = 16

soft_modulus = 0.05
poisson_ratio = 0.3
lame = poisson_ratio / ((1.0 + poisson_ratio) * (1.0 - 2.0 * poisson_ratio))
shear = 1.0 / (2.0 * (1.0 + poisson_ratio))
THREE, TWO, ONE = 1.0 / 16.0, 1.0 / 48.0, 1.0 / 144.0
CORNER = THREE * (lame + 4.0 * shear) + 2.0 * TWO * (lame + 4.0 * shear) + ONE * (lame + 4.0 * shear)

VMEM, SMEM = pltpu.VMEM, pltpu.SMEM
F32 = jnp.float32


def up8(n):
    return -(-n // 8) * 8


def call(body, outs, ins, scratch=(), flops=0, smem=(), hbm=(), far_out=False):
    kinds = [SMEM if i in smem else pltpu.HBM if i in hbm else VMEM for i in range(len(ins))]
    ins = [x if k is SMEM else pltpu.with_memory_space_constraint(x, k) for x, k in zip(ins, kinds)]
    return pl.pallas_call(
        body,
        out_shape=[jax.ShapeDtypeStruct(s, F32) if far_out else VMEM(s, F32) for s in outs],
        in_specs=[pl.BlockSpec(memory_space=k) for k in kinds],
        out_specs=[pl.BlockSpec(memory_space=pl.ANY if far_out else VMEM)] * len(outs),
        scratch_shapes=[VMEM(s, F32) if isinstance(s, tuple) else s for s in scratch],
        compiler_params=pltpu.CompilerParams(vmem_limit_bytes=16 * 2**20),
        cost_estimate=pl.CostEstimate(flops=flops, bytes_accessed=0, transcendentals=0),
    )(*ins)


class Plan:
    def __init__(self, block, mesh):
        self.cases, self.comps, self.planes, self.rows, self.width = block
        self.fields = self.cases * self.comps
        self.ngx, self.ngy, self.tiles = mesh["gx"], mesh["gy"], mesh["gz"]
        if not (self.planes == self.tiles == 2 and self.rows % 8 == 0 and self.comps == 3):
            raise ValueError("block shape")
        self.depth = (self.tiles * self.width, self.ngy * self.rows)
        self.r0 = self.rows + 6
        self.main = up8((self.fields + 4) * self.rows)

    def per(self, count):
        return up8(self.fields * count)

    def tile(self, ref, base, count, comp, row):
        return ref[pl.ds(base + comp * count + row, self.cases, stride=self.comps * count), :]

    def put(self, ref, base, count, comp, row, value):
        ref[pl.ds(base + comp * count + row, self.cases, stride=self.comps * count), :] = value

    def raw(self, ref, base, comp, plane, row):
        start = base + (comp * self.planes + plane) * self.rows + row
        return ref[pl.ds(start, self.cases, stride=self.comps * self.planes * self.rows), :]

    def lanes(self, count=None):
        return lax.broadcasted_iota(jnp.int32, (count or self.cases, self.width), 1)

    def ahead(self, tiles, lane):
        moved = [pltpu.roll(v, self.width - 1, 1) for v in tiles]
        moved.append(jnp.zeros_like(tiles[0]))
        return [jnp.where(lane == self.width - 1, moved[t + 1], moved[t]) for t in range(self.tiles)]

    def behind(self, tiles, lane):
        moved = [pltpu.roll(v, 1, 1) for v in tiles]
        moved = [jnp.zeros_like(tiles[0])] + moved
        return [jnp.where(lane == 0, moved[t], moved[t + 1]) for t in range(self.tiles)]

    def wide(self, row):
        return jnp.broadcast_to(row, (self.cases, self.width))


def modes_z(p, load, mask, count, sign, out):
    lane = p.lanes()
    for r in range(count):
        m = [p.wide(mask(t, r)) for t in range(p.tiles)]
        ms = [x * sign for x in m]
        for comp in range(3):
            v = [load(t, comp, r) * (ms[t] if comp == 0 else m[t]) for t in range(p.tiles)]
            n = p.ahead(v, lane)
            for t in range(p.tiles):
                out[((comp * 2) * count + r) * p.tiles + t, 0 : p.cases, :] = v[t] + n[t]
                out[((comp * 2 + 1) * count + r) * p.tiles + t, 0 : p.cases, :] = n[t] - v[t]


CQ, CB, CS = THREE * lame, 2.0 * THREE * shear, THREE * shear
CD, CE, CF = TWO * (lame + 3.0 * shear), TWO * lame, TWO * shear
CG = ONE * (lame + 4.0 * shear)


def modes_y(p, ref, count, e, t, flip):
    found = [{}, {}, {}]
    for comp in range(3):
        for c in (0, 1):
            at = ((comp * 2 + c) * count + e) * p.tiles + t
            a = ref[at, 0 : p.cases, :]
            b = ref[at + p.tiles, 0 : p.cases, :]
            if flip and comp == 0:
                found[comp][0, c], found[comp][1, c] = -a - b, a - b
            else:
                found[comp][0, c], found[comp][1, c] = a + b, b - a
    return found


def between(total, change):
    (x, y, z), (dx, dy, dz) = total, change
    q = CQ * (dx[0, 0] + y[1, 0] + z[0, 1])
    sxy = CS * (dy[0, 0] + x[1, 0])
    sxz = CS * (dz[0, 0] + x[0, 1])
    syz = CS * (z[1, 0] + y[0, 1])
    s = x[1, 1] + dy[0, 1] + dz[1, 0]
    return {
        (0, 0, 0): -(q + CB * dx[0, 0]),
        (0, 1, 0): sxy - (CD * dx[1, 0] + CE * z[1, 1]),
        (0, 0, 1): sxz - (CD * dx[0, 1] + CE * y[1, 1]),
        (0, 1, 1): CF * (s + x[1, 1]) - CG * dx[1, 1],
        (1, 0, 0): -sxy,
        (1, 1, 0): (q + CB * y[1, 0]) - (CD * dy[1, 0] + CE * dz[0, 1]),
        (1, 0, 1): syz - CF * (s + dy[0, 1]),
        (1, 1, 1): (CD * y[1, 1] + CE * dx[0, 1]) - CG * dy[1, 1],
        (2, 0, 0): -sxz,
        (2, 0, 1): (q + CB * z[0, 1]) - (CD * dz[0, 1] + CE * dy[1, 0]),
        (2, 1, 0): syz - CF * (s + dz[1, 0]),
        (2, 1, 1): (CD * z[1, 1] + CE * dx[1, 0]) - CG * dz[1, 1],
    }


def share(m, way):
    x, y, z = m
    q = CQ * (x[0, 0] + y[1, 0] + z[0, 1])
    sxy = CS * (y[0, 0] + x[1, 0])
    sxz = CS * (z[0, 0] + x[0, 1])
    pair = z[1, 0] + y[0, 1]
    syz = CS * pair
    s = x[1, 1] + pair
    found = {
        (0, 0, 0): -(q + CB * x[0, 0]),
        (1, 1, 1): (CD - way * CG) * y[1, 1] + CE * x[0, 1],
        (2, 1, 1): (CD - way * CG) * z[1, 1] + CE * x[1, 0],
        (0, 1, 1): (way * 2.0 * CF - CG) * x[1, 1] + (way * CF) * pair,
    }
    low, high = CD * x[1, 0] + CE * z[1, 1], CD * x[0, 1] + CE * y[1, 1]
    if way > 0:
        found[0, 1, 0], found[0, 0, 1] = sxy - low, sxz - high
        found[1, 0, 0], found[2, 0, 0] = -sxy, -sxz
        found[1, 1, 0] = q + ((CB - CD) * y[1, 0] - CE * z[0, 1])
        found[2, 0, 1] = q + ((CB - CD) * z[0, 1] - CE * y[1, 0])
        found[1, 0, 1] = syz - CF * (s + y[0, 1])
        found[2, 1, 0] = syz - CF * (s + z[1, 0])
    else:
        found[0, 1, 0], found[0, 0, 1] = -sxy - low, -sxz - high
        found[1, 0, 0], found[2, 0, 0] = sxy, sxz
        found[1, 1, 0] = q + ((CB + CD) * y[1, 0] + CE * z[0, 1])
        found[2, 0, 1] = q + ((CB + CD) * z[0, 1] + CE * y[1, 0])
        found[1, 0, 1] = syz + CF * (s + y[0, 1])
        found[2, 1, 0] = syz + CF * (s + z[1, 0])
    return found


def both_shares(m, inner, outer):
    x, y, z = m
    volume = CQ * (y[1, 0] + z[0, 1])
    pair = z[1, 0] + y[0, 1]
    sy, sz, sp = CS * y[0, 0], CS * z[0, 0], CS * pair
    even = {
        (0, 0, 0): volume,
        (0, 1, 0): sy + CE * z[1, 1],
        (0, 0, 1): sz + CE * y[1, 1],
        (0, 1, 1): CF * pair,
        (1, 0, 0): sy,
        (1, 1, 0): volume + ((CB + CD) * y[1, 0] + CE * z[0, 1]),
        (1, 0, 1): sp + CF * (pair + y[0, 1]),
        (1, 1, 1): (CD + CG) * y[1, 1],
        (2, 0, 0): sz,
        (2, 0, 1): volume + ((CB + CD) * z[0, 1] + CE * y[1, 0]),
        (2, 1, 0): sp + CF * (pair + z[1, 0]),
        (2, 1, 1): (CD + CG) * z[1, 1],
    }
    q, f = CQ * x[0, 0], CF * x[1, 1]
    odd = {
        (0, 0, 0): (CQ + CB) * x[0, 0],
        (0, 1, 0): (CS + CD) * x[1, 0],
        (0, 0, 1): (CS + CD) * x[0, 1],
        (0, 1, 1): (2.0 * CF + CG) * x[1, 1],
        (1, 0, 0): CS * x[1, 0],
        (1, 1, 0): q,
        (1, 0, 1): f,
        (1, 1, 1): CE * x[0, 1],
        (2, 0, 0): CS * x[0, 1],
        (2, 0, 1): q,
        (2, 1, 0): f,
        (2, 1, 1): CE * x[1, 0],
    }
    total, gap = inner + outer, outer - inner
    return {k: (gap * v + total * odd[k]) if k[0] == 0 else (total * v + gap * odd[k]) for k, v in even.items()}


def twice(p, ref, flip, inner, outer, count, sign, emit):
    def forces(e, t):
        return both_shares(
            modes_y(p, ref, count, e, t, flip), p.wide(inner(t, e)), p.wide(outer(t, e))
        )

    spread(p, forces, count, sign, emit)


def spread(p, forces, count, sign, emit):
    lane = p.lanes()
    carry = {}
    for e in range(count - 1):
        done = {}
        for t in range(p.tiles):
            h = forces(e, t)
            for comp in range(3):
                for c in (0, 1):
                    if e:
                        done[comp, c, t] = carry[comp, c, t] + (h[comp, 0, c] - h[comp, 1, c])
                    carry[comp, c, t] = h[comp, 0, c] + h[comp, 1, c]
        if e:
            for comp in range(3):
                low = [done[comp, 0, t] - done[comp, 1, t] for t in range(p.tiles)]
                high = [done[comp, 0, t] + done[comp, 1, t] for t in range(p.tiles)]
                back = p.behind(high, lane)
                for t in range(p.tiles):
                    total = low[t] + back[t]
                    emit(t, comp, e - 1, total * sign if comp == 0 else total)


def layer(p, own, other, flip, modulus, count, sign, emit, outer=None):
    def forces(e, t):
        near, far = modes_y(p, own, count, e, t, flip), modes_y(p, other, count, e, t, False)
        total = [{k: far[c][k] + v for k, v in near[c].items()} for c in range(3)]
        change = [{k: far[c][k] - v for k, v in near[c].items()} for c in range(3)]
        mod = p.wide(modulus(t, e))
        h = {k: mod * v for k, v in between(total, change).items()}
        if outer is not None:
            rest = p.wide(outer(t, e))
            for k, v in share(near, -1).items():
                h[k] = h[k] - rest * v if k[0] == 0 else h[k] + rest * v
        return h

    spread(p, forces, count, sign, emit)


def single(p, ref, modulus, count, sign, emit):
    def forces(e, t):
        mod = p.wide(modulus(t, e))
        return {k: mod * v for k, v in share(modes_y(p, ref, count, e, t, False), 1).items()}

    spread(p, forces, count, sign, emit)


OWN, PARTNER, RECEIVED, NEAR, FAR, SCALE, BEYOND, PAST, SCALE_FAR = range(9)


def static(p, ref, kind, t, row):
    at = (kind * p.tiles + t) * up8(p.r0) + row
    return ref[at : at + 1, :]


def place():
    core = lax.axis_index("gz")
    return core, 1.0 - 2.0 * core.astype(F32)


def shards(mesh, design, supports, body_load, start, load_nodes, load_values):
    p = Plan(body_load.shape, mesh)
    C, D, Y, W, T, FL = p.cases, p.comps, p.rows, p.width, p.tiles, p.fields
    Q = p.planes
    n_raw = FL * Q * Y
    z_load = n_raw
    z_stat = z_load + FL * Y
    z_rows = z_stat + 2 * Q * Y
    y_stat = FL * 3
    y_load = y_stat + 6
    y_part = up8(y_load + FL * 2)
    d_part = up8(y_stat + 12)
    raw_load = Q * FL * 3
    raw_stat = raw_load + Q * FL * 2
    raw_rows = up8(raw_stat + Q * 6)
    R0, R1, R2 = Y + 6, Y + 4, Y + 2
    N1, N2, N3 = p.per(R1), p.per(R2), p.per(Y)
    M = p.main
    both = p.ngy == 2

    x0 = start.reshape(n_raw, W)
    bl = body_load.reshape(n_raw, W)
    de = design.reshape(Q * Y, W)
    su = supports.reshape(Q * Y, W)

    def edges():
        if both:
            first = lax.axis_index("gy") == 0
            return [(jnp.where(first, Y - 3, 0), jnp.where(first, Y - 2, 0))]
        return [(Y - 3, Y - 2), (0, 0)]

    ways = (1,) if both else (1, -1)
    halos = len(ways)

    def gather_body(x_hbm, b_hbm, d_hbm, s_hbm, z_ref, b_ref, *refs):
        y_refs, (d_ref, s_ref, sems) = refs[:halos], refs[halos:]
        core = lax.axis_index("gz")
        moves = [
            pltpu.make_async_copy(src, dst, sems.at[i])
            for i, (src, dst) in enumerate(
                ((x_hbm, z_ref.at[pl.ds(0, n_raw)]), (b_hbm, b_ref), (d_hbm, d_ref), (s_hbm, s_ref))
            )
        ]
        for move in moves:
            move.start()
        moves[2].wait()
        density = (d_ref[...].astype(F32) + 1.0) / LEVELS
        z_ref[z_stat : z_stat + Q * Y, :] = (
            soft_modulus + (1.0 - soft_modulus) * density * density * density
        )
        moves[3].wait()
        z_ref[z_stat + Q * Y : z_rows, :] = 1.0 - s_ref[...].astype(F32)
        for y_ref, (three, _) in zip(y_refs, edges()):
            if raw_rows > raw_stat + Q * 6:
                y_ref[raw_stat + Q * 6 : raw_rows, :] = jnp.zeros((raw_rows - raw_stat - Q * 6, W), F32)
            for q in range(Q):
                for kind in range(2):
                    for r in range(3):
                        at = raw_stat + q * 6 + kind * 3 + r
                        y_ref[at : at + 1, :] = z_ref[pl.ds(z_stat + (kind * Q + q) * Y + three + r, 1), :]
        moves[0].wait()
        for y_ref, (three, _) in zip(y_refs, edges()):
            for q in range(Q):
                for comp in range(D):
                    for r in range(3):
                        p.put(y_ref, q * FL * 3, 3, comp, r, p.raw(z_ref, 0, comp, q, three + r))
        moves[1].wait()
        for y_ref, (_, two) in zip(y_refs, edges()):
            for q in range(Q):
                for comp in range(D):
                    for r in range(2):
                        p.put(y_ref, raw_load + q * FL * 2, 2, comp, r, p.raw(b_ref, 0, comp, q, two + r))
        for f in range(FL):
            z_ref[z_load + f * Y : z_load + (f + 1) * Y, :] = b_ref[
                pl.ds(pl.multiple_of((f * Q + 1 - core) * Y, 8), Y), :
            ]

    z_msg, b_near, *y_sent = call(
        gather_body,
        [(z_rows, W), (n_raw, W)] + [(raw_rows, W)] * halos,
        [x0, bl, de, su],
        [VMEM((Q * Y, W), jnp.int32), VMEM((Q * Y, W), jnp.int32), pltpu.SemaphoreType.DMA((4,))],
        flops=10**5,
        hbm=(0, 1, 2, 3),
    )

    def cores(x):
        return lax.ppermute(x, "gz", [(i, 1 - i) for i in range(T)])

    def rows_along(x, step):
        return lax.ppermute(x, "gy", [(i, (i + step) % p.ngy) for i in range(p.ngy)])

    def planes_along(x, step=0):
        pairs = []
        for i in range(p.ngx):
            for j in range(p.ngy):
                for k in range(T):
                    to = i + 2 * k - 1
                    mine = (i * p.ngy + j) * T + k
                    row = (j + step) % p.ngy
                    if 0 <= to < p.ngx:
                        pairs.append((mine, (to * p.ngy + row) * T + 1 - k))
                    elif step:
                        pairs.append((mine, (i * p.ngy + row) * T + k))
                    elif p.ngy % 2 == 0:
                        pairs.append((mine, (i * p.ngy + (j ^ 1)) * T + k))
                    else:
                        pairs.append((mine, mine))
        return lax.ppermute(x, ("gx", "gy", "gz"), pairs)

    y_raw = [rows_along(x, step) for x, step in zip(y_sent, ways)]
    z_got = cores(z_msg)
    zy_raw = [cores(x) for x in y_raw]

    def main_body(s_ref, z_ref, own_ref, par_ref, *d_refs):
        core = lax.axis_index("gz")
        for d_ref, (three, _) in zip(d_refs, edges()):
            for src, half in ((s_ref, core), (z_ref, 1 - core)):
                to = half * d_part
                for comp in range(D):
                    for r in range(3):
                        p.put(d_ref, to, 3, comp, r, p.raw(src, 0, comp, core, three + r))
                for kind in range(4):
                    of = core if kind < 2 else 1 - core
                    for r in range(3):
                        d_ref[pl.ds(to + y_stat + kind * 3 + r, 1), :] = src[
                            pl.ds(z_stat + (kind % 2 * Q + of) * Y + three + r, 1), :
                        ]
            for t in range(T):
                if d_part > y_stat + 12:
                    d_ref[t * d_part + y_stat + 12 : (t + 1) * d_part, :] = jnp.zeros(
                        (d_part - y_stat - 12, W), F32
                    )
        for out, plane in ((own_ref, core), (par_ref, 1 - core)):
            for src, half in ((s_ref, core), (z_ref, 1 - core)):
                base = half * M
                for comp in range(D):
                    for r in range(Y):
                        p.put(out, base, Y, comp, r, p.raw(src, 0, comp, plane, r))
                for kind in range(4):
                    of = plane if kind < 2 else 1 - plane
                    out[pl.ds(pl.multiple_of(base + (FL + kind) * Y, 8), Y), :] = src[
                        pl.ds(pl.multiple_of(z_stat + (kind % 2 * Q + of) * Y, 8), Y), :
                    ]

    own_m, par_m, *sent = call(
        main_body, [(T * M, W)] * 2 + [(T * d_part, W)] * halos, [z_msg, z_got], flops=10**5
    )
    far_y = [planes_along(x, step) for x, step in zip(sent, ways)]
    far_m = planes_along(own_m)

    def rows_body(*refs):
        core = lax.axis_index("gz")
        outs = refs[2 * halos :]
        for n in range(halos):
            for out, plane in ((outs[n], core), (outs[halos + n], 1 - core)):
                for src, half in ((refs[n], core), (refs[halos + n], 1 - core)):
                    to = half * y_part
                    for comp in range(D):
                        for r in range(3):
                            p.put(out, to, 3, comp, r, p.tile(src, plane * (FL * 3), 3, comp, r))
                        for r in range(2):
                            v = p.tile(src, raw_load + plane * (FL * 2), 2, comp, r)
                            p.put(out, to + y_load, 2, comp, r, v)
                    for r in range(6):
                        out[pl.ds(to + y_stat + r, 1), :] = src[pl.ds(raw_stat + plane * 6 + r, 1), :]

    got = call(rows_body, [(T * y_part, W)] * (2 * halos), y_raw + zy_raw, flops=10**5)
    y_got, par_y = list(got[:halos]), list(got[halos:])

    def halo(main, refs, part):
        row = lax.axis_index("gy")
        below = jnp.where(row > 0, 1.0, 0.0)
        above = jnp.where(row < p.ngy - 1, 1.0, 0.0)
        return main, refs[0], refs[-1], part, below, above

    def field_at(refs, t, comp, r):
        main, low, high, part, _, _ = refs
        if 3 <= r < Y + 3:
            return p.tile(main, t * M, Y, comp, r - 3)
        if r < 3:
            return p.tile(low, t * part, 3, comp, r)
        return p.tile(high, t * part, 3, comp, r - Y - 3)

    def const_at(refs, kind, t, r):
        main, low, high, part, below, above = refs
        if 3 <= r < Y + 3:
            at = t * M + (FL + kind) * Y + r - 3
            return main[at : at + 1, :]
        at = t * part + y_stat + kind * 3
        if r < 3:
            return low[at + r : at + r + 1, :] * below
        at += r - Y - 3
        return high[at : at + 1, :] * above

    def const_parts(refs, kind, t):
        main, low, high, part, below, above = refs
        at = t * part + y_stat + kind * 3
        to = t * M + (FL + kind) * Y
        return low[at : at + 3, :] * below, main[to : to + Y, :], high[at : at + 3, :] * above

    def points_body(node_ref, value_ref, out):
        core = lax.axis_index("gz")
        deep, across = p.depth
        base = ((lax.axis_index("gx") * Q + core) * across + lax.axis_index("gy") * Y - 2) * deep
        spots = jnp.concatenate([node_ref[c : c + 1, :] for c in range(C)], axis=1) - base
        total = C * n_loads
        if W & (W - 1):
            row = spots // W
            lane = spots - row * W
        else:
            row, lane = spots >> (W.bit_length() - 1), spots & (W - 1)
        hot = jnp.where(lax.broadcasted_iota(jnp.int32, (W, total), 0) == lane, 1.0, 0.0)
        rows8 = jnp.broadcast_to(row, (8, total))
        mine = lax.broadcasted_iota(jnp.int32, (8, total), 0)
        column = lax.broadcasted_iota(jnp.int32, (8, total), 1)
        mine = (column >= mine * n_loads) & (column < (mine + 1) * n_loads)
        values = []
        for comp in range(D):
            v = jnp.concatenate([value_ref[c, comp : comp + 1, :] for c in range(C)], axis=1)
            values.append(jnp.where(mine, jnp.broadcast_to(v, (8, total)), 0.0))
        left = [
            jnp.where(rows8 == r * T + t, values[comp], 0.0)
            for t in range(T)
            for comp in range(D)
            for r in range(R1)
        ]
        out[...] = lax.dot_general(
            jnp.concatenate(left, axis=0),
            hot,
            (((1,), (1,)), ((), ())),
            precision=lax.Precision.HIGHEST,
            preferred_element_type=F32,
        )

    n_loads = load_nodes.shape[1]
    (points,) = call(
        points_body,
        [(T * D * R1 * 8, W)],
        [load_nodes, jnp.swapaxes(load_values, 1, 2)],
        flops=10**6,
    )

    def loads_body(p_ref, b_ref, z_ref, *refs):
        ys, out = refs[:halos], refs[halos]
        core = lax.axis_index("gz")
        for half in range(2):
            t = core if half == 0 else 1 - core
            for comp in range(D):
                for r in range(R1):
                    if r < 2:
                        v = p.tile(ys[0], t * y_part + y_load, 2, comp, r)
                    elif r < Y + 2:
                        if half == 0:
                            v = p.raw(b_ref, 0, comp, core, r - 2)
                        else:
                            v = p.tile(z_ref, z_load, Y, comp, r - 2)
                    else:
                        v = p.tile(ys[-1], t * y_part + y_load, 2, comp, r - Y - 2)
                    at = t * (D * R1) + comp * R1 + r
                    out[at, 0:C, :] = v + p_ref[pl.ds(pl.multiple_of(at * 8, 8), C), :]

    (loaded,) = call(
        loads_body,
        [(T * D * R1, 8, W)],
        [points, b_near, z_got] + y_got,
        flops=10**6,
    )

    def near_start_body(own_m_ref, par_m_ref, *refs):
        modes_ref, part_ref, other_ref = refs[2 * halos :]
        core, sign = place()
        own, par = halo(own_m_ref, refs[:halos], y_part), halo(par_m_ref, refs[halos : 2 * halos], y_part)
        for refs, out in ((own, modes_ref), (par, other_ref)):
            modes_z(
                p,
                lambda t, k, r, refs=refs: field_at(refs, t, k, r),
                lambda t, r, refs=refs: const_at(refs, 1, t, r),
                R0,
                sign,
                out,
            )

        def modulus(t, e):
            return jnp.where(core == 0, const_at(own, 0, t, e), const_at(par, 0, t, e))

        def emit(t, comp, r, v):
            part_ref[(comp * R1 + r) * T + t, 0:C, :] = v

        layer(p, modes_ref, other_ref, False, modulus, R0, sign, emit)

    def field_shapes(count):
        return (6 * count * T, 8, W)

    modes, part = call(
        near_start_body,
        [field_shapes(R0), (D * R1 * T, 8, W)],
        [own_m, par_m] + y_got + par_y,
        [field_shapes(R0)],
        flops=10**6,
    )

    def far_start_body(far_m_ref, own_m_ref, par_m_ref, modes_ref, part_ref, load_ref, *refs):
        r_ref, d_ref, st_ref, other_ref = refs[3 * halos :]
        core, sign = place()
        own, par = halo(own_m_ref, refs[:halos], y_part), halo(par_m_ref, refs[halos : 2 * halos], y_part)
        far = halo(far_m_ref, refs[2 * halos : 3 * halos], d_part)
        column = lax.axis_index("gx")
        inside = jnp.where(core == 0, column > 0, column < p.ngx - 1)
        valid = jnp.where(inside, 1.0, 0.0)
        lane_rows = lax.broadcasted_iota(jnp.int32, (R1, W), 1)
        pad = up8(R0)
        for t in range(T):
            spans = ((0, 3), (3, Y), (Y + 3, 3))
            own_e, par_e, far_e = (const_parts(x, 0, t) for x in (own, par, far))
            own_m, par_m, far_m = (const_parts(x, 1, t) for x in (own, par, far))
            next_e, next_m = const_parts(far, 2, t), const_parts(far, 3, t)
            for n, (first, count) in enumerate(spans):
                for kind, v in (
                    (OWN, own_m[n]),
                    (PARTNER, par_m[n]),
                    (RECEIVED, far_m[n] * valid),
                    (NEAR, jnp.where(core == 0, own_e[n], par_e[n])),
                    (FAR, jnp.where(core == 0, far_e[n] * valid, own_e[n])),
                    (BEYOND, next_m[n] * valid),
                    (PAST, jnp.where(core == 0, next_e[n], far_e[n]) * valid),
                ):
                    to = (kind * T + t) * pad + first
                    st_ref[to : to + count, :] = v
        for one, other, moved, scaled in ((NEAR, FAR, OWN, SCALE), (FAR, PAST, RECEIVED, SCALE_FAR)):
            sums = []
            for t in range(T):
                near, rest = (one * T + t) * pad, (other * T + t) * pad
                sums.append(
                    (st_ref[near : near + R1, :] + st_ref[rest : rest + R1, :])
                    + (st_ref[near + 1 : near + 1 + R1, :] + st_ref[rest + 1 : rest + 1 + R1, :])
                )
            back = p.behind(sums, lane_rows)
            for t in range(T):
                around = sums[t] + back[t]
                at = (moved * T + t) * pad + 1
                mov = st_ref[at : at + R1, :]
                guarded = jnp.where(mov > 0, around, 1.0)
                to = (scaled * T + t) * pad + 1
                st_ref[to : to + R1, :] = mov / (CORNER * guarded) + (1.0 - mov)
        modes_z(
            p,
            lambda t, k, r: field_at(far, t, k, r),
            lambda t, r: static(p, st_ref, RECEIVED, t, r),
            R0,
            -sign,
            other_ref,
        )

        def emit(t, comp, r, v):
            force = v + part_ref[(comp * R1 + r) * T + t, 0:C, :]
            mov = p.wide(static(p, st_ref, OWN, t, r + 1))
            here = field_at(own, t, comp, r + 1)
            load = load_ref[t * (D * R1) + comp * R1 + r, 0:C, :]
            res = mov * (load - force) - (1.0 - mov) * here
            p.put(d_ref, t * N1, R1, comp, r, p.wide(static(p, st_ref, SCALE, t, r + 1)) * res)
            if 2 <= r < Y + 2:
                p.put(r_ref, t * N3, Y, comp, r - 2, res)

        layer(p, modes_ref, other_ref, True, lambda t, e: static(p, st_ref, FAR, t, e), R0, -sign, emit)

    res0, dir0, consts = call(
        far_start_body,
        [(T * N3, W), (T * N1, W), (9 * T * up8(R0), W)],
        [far_m, own_m, par_m, modes, part, loaded] + y_got + par_y + far_y,
        [field_shapes(R0)],
        flops=10**6,
    )

    def near_apply(own_ref, par_ref, st_ref, part_ref, modes_ref, other_ref, per, count, shift):
        _, sign = place()
        modes_z(p, lambda t, k, r: p.tile(own_ref, t * per, count, k, r), lambda t, r: static(p, st_ref, OWN, t, r + shift), count, sign, modes_ref)
        modes_z(p, lambda t, k, r: p.tile(par_ref, t * per, count, k, r), lambda t, r: static(p, st_ref, PARTNER, t, r + shift), count, sign, other_ref)

        def emit(t, comp, r, v):
            part_ref[(comp * (count - 2) + r) * T + t, 0:C, :] = v

        near, far = (lambda t, e, kind=kind: static(p, st_ref, kind, t, e + shift) for kind in (NEAR, FAR))
        layer(p, modes_ref, other_ref, False, near, count, sign, emit, far)

    def far_apply(load, own_ref, st_ref, part_ref, other_ref, per, count, shift, emit):
        _, sign = place()
        modes_z(p, load, lambda t, r: static(p, st_ref, RECEIVED, t, r + shift), count, -sign, other_ref)

        def finish(t, comp, r, v):
            force = v + part_ref[(comp * (count - 2) + r) * T + t, 0:C, :]
            mov = p.wide(static(p, st_ref, OWN, t, r + 1 + shift))
            here = p.tile(own_ref, t * per, count, comp, r + 1)
            emit(t, comp, r, mov * force + (1.0 - mov) * here, here)

        single(p, other_ref, lambda t, e: static(p, st_ref, FAR, t, e + shift), count, -sign, finish)

    far_d = planes_along(dir0)
    par_d = cores(dir0)
    next_d = planes_along(par_d)

    def near_one_body(own_ref, par_ref, st_ref, part_ref, modes_ref, other_ref):
        near_apply(own_ref, par_ref, st_ref, part_ref, modes_ref, other_ref, N1, R1, 1)

    part1, modes1 = call(
        near_one_body,
        [(D * R2 * T, 8, W), field_shapes(R1)],
        [dir0, par_d, consts],
        [field_shapes(R1)],
        flops=10**6,
    )

    def far_one_body(far_ref, own_ref, st_ref, part_ref, q_ref, w_ref, other_ref):
        if N2 > FL * R2:
            for t in range(T):
                w_ref[t * N2 + FL * R2 : (t + 1) * N2, :] = jnp.zeros((N2 - FL * R2, W), F32)

        def emit(t, comp, r, image, here):
            scale = p.wide(static(p, st_ref, SCALE, t, r + 2))
            p.put(w_ref, t * N2, R2, comp, r, scale * image - here)
            if 1 <= r < Y + 1:
                p.put(q_ref, t * N3, Y, comp, r - 1, image)

        load = lambda t, k, r: p.tile(far_ref, t * N1, R1, k, r)
        far_apply(load, own_ref, st_ref, part_ref, other_ref, N1, R1, 1, emit)

    image0, second, modes_far = call(
        far_one_body,
        [(T * N3, W), (T * N2, W), field_shapes(R1)],
        [far_d, dir0, consts, part1],
        flops=10**6,
    )
    par_w = cores(second)

    def beside_body(own_ref, st_ref, part_ref):
        _, sign = place()

        def emit(t, comp, r, v):
            part_ref[(comp * R2 + r) * T + t, 0:C, :] = v

        single(p, own_ref, lambda t, e: static(p, st_ref, FAR, t, e + 1), R1, sign, emit)

    (part_beside,) = call(beside_body, [(D * R2 * T, 8, W)], [modes1, consts], flops=10**6)

    def across_body(far_ref, beside_ref, st_ref, part_ref):
        _, sign = place()

        def emit(t, comp, r, v):
            at = (comp * R2 + r) * T + t
            part_ref[at, 0:C, :] = beside_ref[at, 0:C, :] + v

        far, past = (lambda t, e, kind=kind: static(p, st_ref, kind, t, e + 1) for kind in (FAR, PAST))
        twice(p, far_ref, True, far, past, R1, sign, emit)

    (part_far,) = call(
        across_body, [(D * R2 * T, 8, W)], [modes_far, part_beside, consts], flops=10**6
    )

    def columns(number, sums, lane):
        table = jnp.zeros((C, W), F32)
        for j in range(C):
            column = jnp.sum(sums[j], axis=1, keepdims=True)
            table = jnp.where(lane == number * C + j, column, table)
        return table

    def first_gram_body(d_ref, r_ref, g_ref):
        sums = [jnp.zeros((C, W), F32) for _ in range(C)]
        for t in range(T):
            for comp in range(D):
                for r in range(Y):
                    d = p.tile(d_ref, t * N1, R1, comp, r + 2)
                    for j in range(C):
                        at = t * N3 + (j * D + comp) * Y + r
                        sums[j] = sums[j] + d * r_ref[at : at + 1, :]
        g_ref[...] = jnp.zeros((8, W), F32)
        g_ref[0:C, :] = columns(1, sums, p.lanes())

    (gram1,) = call(first_gram_body, [(8, W)], [dir0, res0], flops=10**6)

    def gram_body(d_ref, q_ref, w_ref, first_ref, g_ref):
        lane = p.lanes()
        sums = [[jnp.zeros((C, W), F32) for _ in range(C)] for _ in range(2)]
        for t in range(T):
            for comp in range(D):
                for r in range(Y):
                    d = p.tile(d_ref, t * N1, R1, comp, r + 2)
                    w = p.tile(w_ref, t * N2, R2, comp, r + 1)
                    for j in range(C):
                        at = t * N3 + (j * D + comp) * Y + r
                        q = q_ref[at : at + 1, :]
                        sums[0][j] = sums[0][j] + d * q
                        sums[1][j] = sums[1][j] + w * q
        g_ref[...] = first_ref[...]
        g_ref[0:C, :] = first_ref[0:C, :] + columns(0, sums[0], lane) + columns(2, sums[1], lane)

    (gram3,) = call(gram_body, [(8, W)], [dir0, image0, second, gram1], flops=10**6)

    def own_two_body(own_ref, st_ref, part_ref, modes_ref):
        _, sign = place()
        modes_z(
            p,
            lambda t, k, r: p.tile(own_ref, t * N2, R2, k, r),
            lambda t, r: static(p, st_ref, OWN, t, r + 2),
            R2,
            sign,
            modes_ref,
        )

        def emit(t, comp, r, v):
            part_ref[(comp * Y + r) * T + t, 0:C, :] = v

        near, far = (lambda t, e, kind=kind: static(p, st_ref, kind, t, e + 2) for kind in (NEAR, FAR))
        twice(p, modes_ref, False, near, far, R2, sign, emit)

    (part_own,) = call(
        own_two_body, [(D * Y * T, 8, W)], [second, consts], [field_shapes(R2)], flops=10**6
    )

    def near_two_body(par_ref, st_ref, own_part_ref, part_ref, modes_ref):
        _, sign = place()
        modes_z(
            p,
            lambda t, k, r: p.tile(par_ref, t * N2, R2, k, r),
            lambda t, r: static(p, st_ref, PARTNER, t, r + 2),
            R2,
            sign,
            modes_ref,
        )

        def emit(t, comp, r, v):
            at = (comp * Y + r) * T + t
            part_ref[at, 0:C, :] = own_part_ref[at, 0:C, :] + v

        single(p, modes_ref, lambda t, e: static(p, st_ref, NEAR, t, e + 2), R2, sign, emit)

    (part2,) = call(
        near_two_body, [(D * Y * T, 8, W)], [par_w, consts, part_own], [field_shapes(R2)], flops=10**6
    )

    def far_two_body(
        next_ref, far_ref, own_ref, st_ref, part_far_ref, part_ref, gram_ref,
        g_ref, u_ref, next_modes_ref, w_ref, other_ref,
    ):
        _, sign = place()
        modes_z(
            p,
            lambda t, k, r: p.tile(next_ref, t * N1, R1, k, r),
            lambda t, r: static(p, st_ref, BEYOND, t, r + 1),
            R1,
            -sign,
            next_modes_ref,
        )

        def found(t, comp, r, v):
            force = v + part_far_ref[(comp * R2 + r) * T + t, 0:C, :]
            mov = p.wide(static(p, st_ref, RECEIVED, t, r + 2))
            here = p.tile(far_ref, t * N1, R1, comp, r + 1)
            image = mov * force + (1.0 - mov) * here
            scale = p.wide(static(p, st_ref, SCALE_FAR, t, r + 2))
            w_ref[(comp * R2 + r) * T + t, 0:C, :] = scale * image - here

        single(p, next_modes_ref, lambda t, e: static(p, st_ref, PAST, t, e + 1), R1, -sign, found)

        def emit(t, comp, r, image, here):
            p.put(u_ref, t * N3, Y, comp, r, image)
            sums_in.append((image, t, comp, r))

        sums_in = []
        load = lambda t, k, r: w_ref[(k * R2 + r) * T + t, 0:C, :]
        far_apply(load, own_ref, st_ref, part_ref, other_ref, N2, R2, 2, emit)
        sums = [jnp.zeros((C, W), F32) for _ in range(C)]
        for _, t, comp, r in sums_in:
            u = p.tile(u_ref, t * N3, Y, comp, r)
            for j in range(C):
                at = t * N2 + (j * D + comp) * R2 + r + 1
                sums[j] = sums[j] + u * own_ref[at : at + 1, :]
        g_ref[...] = jnp.zeros((8, W), F32)
        g_ref[0:C, :] = gram_ref[0:C, :] + columns(3, sums, p.lanes())

    table, image2 = call(
        far_two_body,
        [(8, W), (T * N3, W)],
        [next_d, far_d, second, consts, part_far, part2, gram3],
        [field_shapes(R1), (D * R2 * T, 8, W), field_shapes(R2)],
        flops=10**6,
    )

    def pack_body(r_ref, q_ref, d_ref, w_ref, u_ref, mine_ref, send_ref):
        core = lax.axis_index("gz")
        for out, t in ((mine_ref, core), (send_ref, 1 - core)):
            for number, src in enumerate((r_ref, q_ref)):
                out[number * N3 : (number + 1) * N3, :] = src[pl.ds(pl.multiple_of(t * N3, 8), N3), :]
            out[4 * N3 : 5 * N3, :] = u_ref[pl.ds(pl.multiple_of(t * N3, 8), N3), :]
            for comp in range(D):
                for r in range(Y):
                    p.put(out, 2 * N3, Y, comp, r, p.tile(d_ref, t * N1, R1, comp, r + 2))
                    p.put(out, 3 * N3, Y, comp, r, p.tile(w_ref, t * N2, R2, comp, r + 1))

    mine, send = call(
        pack_body, [(5 * N3, W)] * 2, [res0, image0, dir0, second, image2], flops=10**6
    )
    kept = cores(send)

    table = table + cores(table)

    def crossed(x, axis, size, step):
        pairs = [(i * T + k, (i ^ step) * T + 1 - k) for i in range(size) for k in range(T)]
        return lax.ppermute(x, (axis, "gz"), pairs)

    for axis, size in (("gy", p.ngy), ("gx", p.ngx)):
        if size & (size - 1):
            table = lax.psum(table, axis)
            continue
        step = 1
        while step < size:
            if step * 2 < size:
                one, two, three = (crossed(table, axis, size, step * k) for k in (1, 2, 3))
                table = (table + one) + (two + three)
                step *= 4
            else:
                table = table + crossed(table, axis, size, step)
                step *= 2

    def final_body(
        g_ref, x_ref, mine_ref, kept_ref, out_hbm, res_hbm, a_ref, out_ref, res_ref, sems
    ):
        core = lax.axis_index("gz")
        lane = lax.broadcasted_iota(jnp.int32, (1, W), 1)

        def splat(row, at):
            return jnp.broadcast_to(row[:, at : at + 1], (1, W))

        def factor(rows, first):
            a = {(i, j): splat(rows[i], first + j) for i in range(C) for j in range(i + 1)}
            low, inv = {}, []
            for k in range(C):
                inv.append(1.0 / a[k, k])
                for i in range(k + 1, C):
                    low[i, k] = a[i, k] * inv[k]
                for i in range(k + 1, C):
                    for j in range(k + 1, i + 1):
                        a[i, j] = a[i, j] - low[i, k] * a[j, k]
            return low, inv

        def solve(factors, right):
            low, inv = factors
            y = []
            for i in range(C):
                v = right[i]
                for k in range(i):
                    v = v - low[i, k] * y[k]
                y.append(v)
            x = [None] * C
            for i in reversed(range(C)):
                v = y[i] * inv[i]
                for k in range(i + 1, C):
                    v = v - low[k, i] * x[k]
                x[i] = v
            return x

        rows = [g_ref[i : i + 1, :] for i in range(C)]
        first = solve(factor(rows, 0), rows)
        reduced = []
        for i in range(C):
            v = jnp.where(
                lane < 2 * C, pltpu.roll(rows[i], C, 1) - rows[i], pltpu.roll(rows[i], W - C, 1)
            )
            for k in range(C):
                v = v - splat(rows[i], 2 * C + k) * first[k]
            reduced.append(v)
        on_second = solve(factor(reduced, 2 * C), reduced)
        for i in range(C):
            v = first[i]
            for k in range(C):
                v = v - splat(first[i], 2 * C + k) * on_second[k]
            for k in range(C):
                a_ref[i * C + k] = jnp.broadcast_to(v[:, C + k : C + k + 1], (Y, W))
                a_ref[C * C + i * C + k] = jnp.broadcast_to(on_second[i][:, C + k : C + k + 1], (Y, W))
        moves = []
        span = D * Q * Y
        for number in range(2):
            target, to = ((out_ref, out_hbm), (res_ref, res_hbm))[number]
            for i in range(C):
                a = [a_ref[j * C + i] for j in range(C)]
                b = [a_ref[C * C + j * C + i] for j in range(C)]
                for src, plane in ((mine_ref, core), (kept_ref, 1 - core)):
                    for comp in range(D):
                        at = [(j * D + comp) * Y for j in range(C)]
                        one, two = (1, 4) if number else (2, 3)
                        terms = [
                            a[j] * src[one * N3 + at[j] : one * N3 + at[j] + Y, :]
                            + b[j] * src[two * N3 + at[j] : two * N3 + at[j] + Y, :]
                            for j in range(C)
                        ]
                        total = sum(terms[1:], terms[0])
                        rows = pl.ds(pl.multiple_of(((i * D + comp) * Q + plane) * Y, 8), Y)
                        if number:
                            target[rows, :] = src[at[i] : at[i] + Y, :] - total
                        else:
                            target[rows, :] = x_ref[rows, :] + total
                rows = pl.ds(i * span, span)
                moves.append(pltpu.make_async_copy(target.at[rows], to.at[rows], sems.at[number * C + i]))
                moves[-1].start()
        for move in moves:
            move.wait()

    out, res = call(
        final_body,
        [(n_raw, W)] * 2,
        [table, z_msg, mine, kept],
        [(2 * C * C, Y, W), (n_raw, W), (n_raw, W), pltpu.SemaphoreType.DMA((2 * C,))],
        flops=10**5,
        far_out=True,
    )
    return out.reshape(start.shape), res.reshape(start.shape)


def solution(mesh):
    in_specs = (
        P(("grp", "gx"), "gy", "gz"),
        P(("grp", "gx"), "gy", "gz"),
        P("grp", None, "gx", "gy", "gz"),
        P("grp", None, "gx", "gy", "gz"),
        P("grp", None),
        P("grp", None, None),
    )
    out_specs = (P("grp", None, "gx", "gy", "gz"), P("grp", None, "gx", "gy", "gz"))

    def body(*args):
        return shards(dict(mesh.shape), *args)

    return jax.shard_map(body, mesh=mesh, in_specs=in_specs, out_specs=out_specs, check_vma=False)
```
